32 devices in a mesh: band: 8 (over y, x, core), lev: 4 (over z).
Axes of the slice: x: 2, y: 2, z: 4, core: 2. Of those that a mesh axis runs over, the one named last changes fastest.
Arguments:
- increment: bfloat16 [32, 768, 1536], P('lev', 'band'), may hold values from -6 to 6
- background: float32 [384, 2, 32, 769], P(('band', 'lev')), may hold values from -6 to 6
- legendre: bfloat16 [384, 768, 769], P(('band', 'lev')), may hold values from -6 to 6, as said below
- coupling: float32 [4, 32, 32], replicated, may hold values from -1 to 1
- damping: float32 [4], replicated, may hold values from 0.5 to 4
- target_mass: float32 [1], replicated, may hold values from 1 to 4
- numerators: int32 [4], replicated, may hold values from 8 to 32
- pair_low: int32 [384], replicated, may hold values from 0 to 383, as said below
- lat_map: int32 [768], replicated, may hold values from 0 to 767, each once
Outputs:
- analysis: bfloat16 [32, 768, 1536], P('lev', 'band')
- corrections: float32 [4], replicated
The draws below stay inside these ranges and needn't reach their ends.
Inputs may be any that keep to these rules, and one draw needn't show every extreme that they name: Slot p holds the wavenumbers pair_low[p] and 767 - pair_low[p]; every value appears once. For the slot p with pair_low[p] = 0, legendre[p, j, 0] = 1 at every latitude j. Stored grid row r lies on latitude lat_map[r]; every latitude appears once.
All inputs are finite; a program needn't handle non-finite values.
Results may differ from the reference program's by a relative error of at most 0.0078.
Values may be sent and summed in bfloat16 or wider, within the bound.
A program may use at most 128 MiB of HBM per device.

```python
import math
import jax
import jax.numpy as jnp
from jax import lax

NT = 767
NLAT = 768
NLON = 1536
LEV = 32
STEPS = 4
DEN = 64
NPAIR = 384


def pair_order(key):
    return jax.random.permutation(jax.random.fold_in(key, 7001), NPAIR).astype(jnp.int32)


def draw_pair_low(key, part):
    return pair_order(key)


def draw_legendre(key, part):
    pairs = pair_order(key)
    sub = jax.random.fold_in(key, 7002)
    scale_key = jax.random.fold_in(key, 7003)
    values = jax.random.truncated_normal(sub, -3.0, 3.0, (NPAIR, NLAT, NT + 2), jnp.float32)
    log_scale = jax.random.uniform(scale_key, (NLAT,), jnp.float32, jnp.log(0.5), jnp.log(2.0))
    values = values * jnp.exp(log_scale)[None, :, None]
    column = jnp.where(pairs[:, None] == 0, jnp.ones_like(values[:, :, 0]), values[:, :, 0])
    values = values.at[:, :, 0].set(column)
    return values.astype(jnp.bfloat16)


def place_ends(drawn, rng, smallest, high):
    longest = drawn.shape.index(max(drawn.shape))
    spots = []
    for shift in (0, 1):
        where = [jax.random.randint(jax.random.fold_in(rng, axis), (), 0, length) for axis, length in enumerate(drawn.shape)]
        where[longest] = (where[longest] + shift) % drawn.shape[longest]
        spots.append(tuple(where))
    return drawn.at[spots[0]].set(smallest).at[spots[1]].set(high)


def shard_levels(stream_key, dims, cuts, low, top_value):
    def one(dim, blocks):
        draws = jax.random.uniform(jax.random.fold_in(jax.random.fold_in(stream_key, 6), dim), (blocks,), jnp.float32, low / len(cuts), top_value / len(cuts))
        return jnp.repeat(jnp.exp(draws), dims[dim] // blocks).reshape((-1,) + (1,) * (len(dims) - dim - 1))

    level = one(*cuts[0])
    for cut in cuts[1:]:
        level = level * one(*cut)
    return level


def centred(rng, extent, width, reach, split=(), held_as=jnp.bfloat16):
    array = width * jax.random.normal(rng, extent, jnp.float32)
    if split:
        array = array * shard_levels(rng, extent, split, -0.22, 0.18)
    return jnp.clip(array, -reach, reach).astype(held_as)


def setup_inputs(seed: int = 0) -> dict:
    streams_of = jax.random.split(jax.random.key(seed), 10)
    return {
        "increment": centred(streams_of[0], (LEV, NLAT, NLON), 1.0, 6.0, ((0, 4), (1, 8))),
        "background": centred(streams_of[1], (NPAIR, 2, LEV, NT + 2), 1.0, 6.0, ((0, 32),), jnp.float32),
        "legendre": draw_legendre(jax.random.fold_in(streams_of[9], 71), 0),
        "coupling": centred(streams_of[3], (STEPS, LEV, LEV), LEV ** -0.5, 1.0, (), jnp.float32),
        "damping": jnp.clip(jnp.exp(jax.random.uniform(streams_of[4], (STEPS,), jnp.float32, math.log(0.5), math.log(4.0))), 0.5, 4.0),
        "target_mass": jnp.clip(jnp.exp(jax.random.uniform(streams_of[5], (1,), jnp.float32, math.log(1.0), math.log(4.0))), 1.0, 4.0),
        "numerators": place_ends(jax.random.randint(streams_of[6], (STEPS,), 8, 33), jax.random.fold_in(streams_of[6], 1), 8, 32).astype(jnp.int32),
        "pair_low": draw_pair_low(jax.random.fold_in(streams_of[9], 71), 0),
        "lat_map": jax.random.permutation(streams_of[8], NLAT).astype(jnp.int32),
    }


def wave_table(pair_low):
    member = jnp.arange(4, dtype=jnp.int32) // 2
    re_im = jnp.arange(4, dtype=jnp.int32) % 2
    wavenumber = jnp.where(member[None, :] == 0, pair_low[:, None], NT - pair_low[:, None]).reshape(-1)
    part_of = jnp.tile(re_im, pair_low.shape[0])
    points = jnp.arange(NLON, dtype=jnp.int32)
    phase_idx = wavenumber[:, None] * points[None, :] % NLON
    angles = phase_idx.astype(jnp.float32) * (2.0 * math.pi / NLON)
    values = jnp.where(part_of[:, None] == 0, jnp.cos(angles), -jnp.sin(angles)) * math.sqrt(2.0 / NLON)
    return values.astype(jnp.bfloat16)

def lat_weights(lat_rows):
    return jnp.cos(math.pi * ((lat_rows.astype(jnp.float32) + 0.5) / NLAT - 0.5))

def degrees(low_wave):
    columns = jnp.arange(NT + 2, dtype=jnp.int32)
    in_second = columns[None, :] >= NT + 1 - low_wave[:, None]
    degree = jnp.where(in_second, columns[None, :] - 1, low_wave[:, None] + columns[None, :])
    return (degree.astype(jnp.float32), in_second)

def reference(increment, background, legendre, coupling, damping, target_mass, numerators, pair_low, lat_map):
    fourier_tab = wave_table(pair_low)
    row_weight = lat_weights(lat_map)
    fourier = jnp.dot(fourier_tab, increment.reshape(LEV * NLAT, NLON).T, preferred_element_type=jnp.float32)
    fourier = (fourier.reshape(NPAIR, 4, LEV, NLAT) * row_weight).astype(jnp.bfloat16)
    degree, in_second = degrees(pair_low)

    def direct(packed):
        block_in, poly_tab, second = packed
        stored = poly_tab[lat_map]
        coeffs = jnp.dot(block_in.reshape(4 * LEV, NLAT), stored, preferred_element_type=jnp.float32)
        coeffs = coeffs.reshape(2, 2, LEV, NT + 2) * math.sqrt(2.0 / NLAT)
        return jnp.where(second, coeffs[1], coeffs[0])
    smoothing = 1.0 / (1.0 + (degree / NT) ** 4)
    incr_spec = lax.map(direct, (fourier, legendre, in_second)) * smoothing[:, None, None, :]
    shape_term = degree * (degree + 1.0) / (NT * (NT + 1.0))
    holder = (pair_low == 0).astype(jnp.float32)
    level_weight = 1.0 + 2.0 * jnp.arange(LEV, dtype=jnp.float32) / (LEV - 1)
    normaliser = jnp.sum(level_weight) * jnp.sum(lat_weights(jnp.arange(NLAT, dtype=jnp.int32))) * NLON
    fix_scale = math.sqrt(NT * NLON) / 2.0

    def inverse(packed):
        coeffs, poly_tab, second = packed
        stored = poly_tab[lat_map]
        zeros_bf = jnp.zeros_like(coeffs)
        split_rows = jnp.stack([jnp.where(second, zeros_bf, coeffs), jnp.where(second, coeffs, zeros_bf)])
        result = jnp.dot(split_rows.reshape(4 * LEV, NT + 2), stored.T, preferred_element_type=jnp.float32)
        return (result * math.sqrt(2.0 / NT)).astype(jnp.bfloat16).reshape(4, LEV, NLAT)
    spectral = background
    fix_list = []
    grid_now = jnp.zeros((LEV, NLAT, NLON), jnp.float32)
    for step_idx in range(STEPS):
        coupled = 0.7 * spectral + 0.4 * jnp.einsum('lm,prmc->prlc', coupling[step_idx], spectral, precision=lax.Precision.HIGHEST)
        weight_now = numerators[step_idx].astype(jnp.float32) / DEN
        spectral = coupled / (1.0 + damping[step_idx] * shape_term)[:, None, None, :] + weight_now * incr_spec
        waves = lax.map(inverse, (spectral.astype(jnp.bfloat16), legendre, in_second))
        grid_now = jnp.dot(waves.reshape(NPAIR * 4, LEV * NLAT).T, fourier_tab, preferred_element_type=jnp.float32).reshape(LEV, NLAT, NLON)
        total_mass = jnp.sum(jnp.exp(grid_now) * level_weight[:, None, None] * row_weight[None, :, None]) / normaliser
        mass_fix = jnp.log(target_mass[0] / total_mass)
        spectral = spectral.at[:, 0, :, 0].add(holder[:, None] * (mass_fix * fix_scale))
        fix_list.append(mass_fix)
    return (grid_now.astype(jnp.bfloat16), jnp.stack(fix_list))
```

```python
import math

import jax
import jax.numpy as jnp
from jax import lax
from jax.experimental import pallas as pl
from jax.experimental.pallas import tpu as pltpu
from jax.sharding import PartitionSpec as P

NT = 767
NLAT = 768
NLON = 1536
LEV = 32
STEPS = 4
DEN = 64
NPAIR = 384
AXES = ("band", "lev")


def wave_table(pair_low):
    column = jnp.arange(4 * pair_low.shape[0], dtype=jnp.int32)
    low = jnp.repeat(pair_low, 4)
    wavenumber = jnp.where(column // 2 % 2 == 0, low, NT - low)[:, None]
    quarter = (column % 2 * (NLON // 4))[:, None]
    fine = math.gcd(128, NLON)
    unit = 2.0 * math.pi / NLON
    coarse_pts = jnp.arange(NLON // fine, dtype=jnp.int32)[None, :] * fine
    coarse = ((wavenumber * coarse_pts + quarter) % NLON).astype(jnp.float32) * unit
    rest = (wavenumber * jnp.arange(fine, dtype=jnp.int32)[None, :] % NLON).astype(
        jnp.float32
    ) * unit
    norm = math.sqrt(2.0 / NLON)
    cos_a, sin_a, cos_b, sin_b = lax.optimization_barrier(
        (jnp.cos(coarse) * norm, jnp.sin(coarse) * norm, jnp.cos(rest), jnp.sin(rest))
    )
    blocks = [
        cos_a[:, i : i + 1] * cos_b - sin_a[:, i : i + 1] * sin_b for i in range(NLON // fine)
    ]
    return jnp.concatenate(blocks, axis=1).astype(jnp.bfloat16)


def lat_weights(lat_rows):
    return jnp.cos(math.pi * ((lat_rows.astype(jnp.float32) + 0.5) / NLAT - 0.5))


def degrees(low_wave):
    columns = jnp.arange(NT + 2, dtype=jnp.int32)
    in_second = columns[None, :] >= NT + 1 - low_wave[:, None]
    degree = jnp.where(in_second, columns[None, :] - 1, low_wave[:, None] + columns[None, :])
    return (degree.astype(jnp.float32), in_second)


def body_general(
    increment, background, legendre, coupling, damping, target_mass, numerators, pair_low, lat_map
):
    band_count = lax.axis_size("band")
    lev_count = lax.axis_size("lev")
    device_count = band_count * lev_count
    band_id = lax.axis_index("band")
    lev_id = lax.axis_index("lev")
    lev_dev = increment.shape[0]
    lat_dev = increment.shape[1]
    pair_dev = legendre.shape[0]
    points = lev_dev * lat_dev
    fourier_tab = wave_table(pair_low)
    local_lats = lax.dynamic_slice_in_dim(lat_map, band_id * lat_dev, lat_dev)
    row_weight = lat_weights(local_lats)
    all_levels = 1.0 + 2.0 * jnp.arange(LEV, dtype=jnp.float32) / (LEV - 1)
    normaliser = (
        jnp.sum(all_levels) * jnp.sum(lat_weights(jnp.arange(NLAT, dtype=jnp.int32))) * NLON
    )
    fix_scale = math.sqrt(NT * NLON) / 2.0
    own_pairs = lax.dynamic_slice_in_dim(
        pair_low, (band_id * lev_count + lev_id) * pair_dev, pair_dev
    )
    degree, in_second = degrees(own_pairs)
    holder = (own_pairs == 0).astype(jnp.float32)

    fourier = jnp.einsum(
        "ck,xk->cx",
        fourier_tab,
        increment.reshape(points, NLON),
        preferred_element_type=jnp.float32,
    )
    fourier = (fourier * jnp.tile(row_weight, lev_dev)[None, :]).astype(jnp.bfloat16)
    received = lax.all_to_all(
        fourier.reshape(device_count, pair_dev * 4, points), AXES, split_axis=0, concat_axis=0
    )

    pick = (lat_map[:, None] == jnp.arange(NLAT, dtype=jnp.int32)[None, :]).astype(jnp.bfloat16)
    stored = jnp.einsum(
        "jn,pnc->pjc", pick, legendre, preferred_element_type=jnp.float32
    ).astype(jnp.bfloat16)

    received = received.reshape(band_count, lev_count, pair_dev * 4, lev_dev, lat_dev)
    waves_in = received.transpose(2, 1, 3, 0, 4).reshape(pair_dev, 4 * LEV, NLAT)
    coeffs = jnp.einsum("prj,pjc->prc", waves_in, stored, preferred_element_type=jnp.float32)
    coeffs = coeffs.reshape(pair_dev, 2, 2, LEV, NT + 2) * math.sqrt(2.0 / NLAT)
    second_cols = in_second[:, None, None, :]
    smoothing = 1.0 / (1.0 + (degree / NT) ** 4)
    incr_spec = jnp.where(second_cols, coeffs[:, 1], coeffs[:, 0]) * smoothing[:, None, None, :]
    shape_term = degree * (degree + 1.0) / (NT * (NT + 1.0))

    spectral = background
    means = []
    arrived = []
    for step_idx in range(STEPS):
        coupled = 0.7 * spectral + 0.4 * jnp.einsum(
            "lm,prmc->prlc", coupling[step_idx], spectral, precision=lax.Precision.HIGHEST
        )
        weight_now = numerators[step_idx].astype(jnp.float32) / DEN
        spectral = (
            coupled / (1.0 + damping[step_idx] * shape_term)[:, None, None, :]
            + weight_now * incr_spec
        )
        means.append(jnp.sum(spectral[:, 0, :, 0] * holder[:, None], axis=0))
        spec_bf = spectral.astype(jnp.bfloat16)
        zeros_bf = jnp.zeros_like(spec_bf)
        split_rows = jnp.stack(
            [jnp.where(second_cols, zeros_bf, spec_bf), jnp.where(second_cols, spec_bf, zeros_bf)],
            axis=1,
        )
        waves_f = jnp.einsum(
            "prc,pjc->prj",
            split_rows.reshape(pair_dev, 4 * LEV, NT + 2),
            stored,
            preferred_element_type=jnp.float32,
        )
        waves_bf = (waves_f * math.sqrt(2.0 / NT)).astype(jnp.bfloat16)
        outgoing = waves_bf.reshape(pair_dev * 4, lev_count, lev_dev, band_count, lat_dev)
        outgoing = outgoing.transpose(3, 1, 0, 2, 4).reshape(device_count, pair_dev * 4, points)
        spectral, outgoing = lax.optimization_barrier((spectral, outgoing))
        arrived.append(lax.all_to_all(outgoing, AXES, split_axis=0, concat_axis=0))

    tops, sums = [], []
    for step_idx in range(STEPS):
        grid_now = jnp.einsum(
            "cx,ck->xk",
            arrived[step_idx].reshape(NPAIR * 4, points),
            fourier_tab,
            preferred_element_type=jnp.float32,
        ).reshape(lev_dev, lat_dev, NLON)
        top = jnp.max(grid_now, axis=(1, 2))
        tops.append(top)
        sums.append(
            jnp.sum(
                jnp.sum(jnp.exp(grid_now - top[:, None, None]), axis=2) * row_weight[None, :],
                axis=1,
            )
        )

    packed = jnp.concatenate(
        [jnp.stack(tops).reshape(-1), jnp.stack(sums).reshape(-1), jnp.stack(means).reshape(-1)]
    )
    gathered = lax.all_to_all(
        jnp.broadcast_to(packed[None, :], (device_count, packed.shape[0])),
        AXES,
        split_axis=0,
        concat_axis=0,
    )
    count = STEPS * lev_dev
    all_tops = gathered[:, :count].reshape(band_count, lev_count, STEPS, lev_dev)
    all_sums = gathered[:, count : 2 * count].reshape(band_count, lev_count, STEPS, lev_dev)
    all_tops = all_tops.transpose(2, 0, 1, 3).reshape(STEPS, band_count, LEV)
    all_sums = all_sums.transpose(2, 0, 1, 3).reshape(STEPS, band_count, LEV)
    all_means = jnp.sum(gathered[:, 2 * count :], axis=0).reshape(STEPS, LEV)

    table_entry = jnp.full((), math.sqrt(2.0 / NLON), jnp.bfloat16).astype(jnp.float32)
    to_grid = math.sqrt(2.0 / NT) * table_entry
    carried = jnp.zeros((LEV,), jnp.float32)
    shift = jnp.zeros((LEV,), jnp.float32)
    fix_list = []
    for step_idx in range(STEPS):
        carried = 0.7 * carried + 0.4 * jnp.sum(coupling[step_idx] * carried[None, :], axis=1)
        base = all_means[step_idx]
        moved = (base + carried).astype(jnp.bfloat16).astype(jnp.float32) - base.astype(
            jnp.bfloat16
        ).astype(jnp.float32)
        shift = moved * to_grid
        total = jnp.sum(
            jnp.exp(all_tops[step_idx] + shift[None, :]) * all_sums[step_idx] * all_levels[None, :]
        )
        mass_fix = jnp.log(target_mass[0] / (total / normaliser))
        fix_list.append(mass_fix)
        carried = carried + mass_fix * fix_scale
    own_shift = lax.dynamic_slice_in_dim(shift, lev_id * lev_dev, lev_dev)
    analysis = (grid_now + own_shift[:, None, None]).astype(jnp.bfloat16)
    return (analysis, jnp.stack(fix_list))


GROUP = 4
MESH = pl.DeviceIdType.MESH
LAST = (((1,), (1,)), ((), ()))


def flat_dot(a, b):
    return jnp.dot(a, b, preferred_element_type=jnp.float32)


def exchange_kernel(
    sizes,
    weight_ref,
    target_ref,
    inc_ref,
    leg_ref,
    back_ref,
    cos_a_ref,
    sin_a_ref,
    cos_b_ref,
    sin_b_ref,
    cos_at_ref,
    sin_at_ref,
    cos_bt_ref,
    sin_bt_ref,
    rows_ref,
    lat_ref,
    consts_ref,
    mix_ref,
    grid_ref,
    fix_ref,
    shift_ref,
    points_in,
    table,
    table_t,
    pick,
    leg_buf,
    stored,
    back_buf,
    incr,
    spec,
    turn,
    acc,
    send,
    recv,
    means,
    stat_send,
    stat_recv,
    load_sem,
    leg_sem,
    back_sem,
    send_sem,
    recv_sem,
    stat_sem,
    out_sem,
):
    bands, levs, lev_dev, lat_dev, chunks = sizes
    devs = bands * levs
    band_id = lax.axis_index("band")
    lev_id = lax.axis_index("lev")
    me = band_id * levs + lev_id
    piece = 32
    splits = lat_dev // piece
    rows = 4 * GROUP
    cols = devs * rows
    points = lev_dev * lat_dev
    slots = chunks * GROUP
    per_tile = 128 // piece
    halves = lev_dev // per_tile

    barrier = pltpu.get_barrier_semaphore()

    def peer(o):
        return (
            lax.rem(band_id + lax.rem(o, bands), bands),
            lax.rem(lev_id + o // bands, levs),
        )

    def greet(o, _):
        pl.semaphore_signal(barrier, inc=1, device_id=peer(o), device_id_type=MESH)
        return 0

    lax.fori_loop(1, devs, greet, 0)

    def load_piece(i, j):
        return pltpu.make_async_copy(
            inc_ref.at[i, pl.ds(j * piece, piece), :],
            points_in.at[pl.ds((j * lev_dev + i) * piece, piece), :],
            load_sem,
        )

    for j in range(splits):
        for i in range(lev_dev):
            load_piece(i, j).start()

    def leg_copy(slot):
        return pltpu.make_async_copy(
            leg_ref.at[slot], leg_buf.at[lax.rem(slot, 2)], leg_sem.at[lax.rem(slot, 2)]
        )

    def back_copy(slot):
        return pltpu.make_async_copy(
            back_ref.at[slot], back_buf.at[lax.rem(slot, 2)], back_sem.at[lax.rem(slot, 2)]
        )

    for slot in range(2):
        leg_copy(slot).start()
        back_copy(slot).start()

    def message(t, o):
        db, dz = peer(o)
        return pltpu.make_async_remote_copy(
            src_ref=send.at[t, pl.ds((db * levs + dz) * rows, rows), :],
            dst_ref=recv.at[t, pl.ds(me * rows, rows), :],
            send_sem=send_sem.at[t],
            recv_sem=recv_sem.at[t],
            device_id=(db, dz),
            device_id_type=MESH,
        )

    def send_all(t):
        def one(o, _):
            message(t, o).start()
            return 0

        lax.fori_loop(1, devs, one, 0)
        pltpu.make_async_copy(
            send.at[t, pl.ds(me * rows, rows), :],
            recv.at[t, pl.ds(me * rows, rows), :],
            recv_sem.at[t],
        ).start()

    def wait_recv(t):
        pltpu.make_async_copy(recv.at[t], recv.at[t], recv_sem.at[t]).wait()

    row_weight = rows_ref[...]

    def fourier(ch, _):
        def fill(rb, _):
            base = pl.multiple_of(ch * cols + rb * 128, 128)
            out = pl.multiple_of(rb * 128, 128)
            cos_b = cos_b_ref[pl.ds(base, 128), :]
            sin_b = sin_b_ref[pl.ds(base, 128), :]
            cos_a = cos_a_ref[pl.ds(base, 128), :]
            sin_a = sin_a_ref[pl.ds(base, 128), :]
            for kc in range(NLON // 128):
                table[pl.ds(out, 128), kc * 128 : (kc + 1) * 128] = (
                    cos_a[:, kc : kc + 1] * cos_b - sin_a[:, kc : kc + 1] * sin_b
                ).astype(jnp.bfloat16)
            return 0

        lax.fori_loop(0, cols // 128, fill, 0)

        @pl.when(ch == 0)
        def _():
            pltpu.make_async_copy(points_in, points_in, load_sem).wait()

        got = lax.dot_general(
            table[...], points_in[...], LAST, preferred_element_type=jnp.float32
        )
        send[ch] = (got * row_weight).astype(jnp.bfloat16)

        @pl.when(ch == 0)
        def _():
            pl.semaphore_wait(barrier, devs - 1)

        send_all(ch)
        return 0

    lax.fori_loop(0, chunks, fourier, 0)

    def fill_t(kc, _):
        cos_a = cos_at_ref[pl.ds(kc, 1), :]
        sin_a = sin_at_ref[pl.ds(kc, 1), :]
        table_t[pl.ds(pl.multiple_of(kc * 128, 128), 128), :] = (
            cos_a * cos_bt_ref[...] - sin_a * sin_bt_ref[...]
        ).astype(jnp.bfloat16)
        return 0

    lax.fori_loop(0, NLON // 128, fill_t, 0)
    pick[...] = (
        (lat_ref[...] == lax.broadcasted_iota(jnp.int32, (NLAT, NLAT), 1))
        .astype(jnp.float32)
        .astype(jnp.bfloat16)
    )
    means[...] = jnp.zeros_like(means)
    lane_part = lax.broadcasted_iota(jnp.int32, (rows, 128), 1) // piece

    def gather_pieces(parts):
        out = parts[0]
        for n in range(1, per_tile):
            out = jnp.where(lane_part == n, parts[n], out)
        return out

    def rolled(x, amount):
        amount = amount * piece % 128
        return pltpu.roll(x, amount, 1) if amount else x

    def chunk_body(ch, _):
        def prepare(s, _):
            slot = ch * GROUP + s
            leg_copy(slot).wait()
            stored[s] = flat_dot(pick[...], leg_buf[lax.rem(slot, 2)]).astype(jnp.bfloat16)

            @pl.when(slot + 2 < slots)
            def _():
                leg_copy(slot + 2).start()

            return 0

        lax.fori_loop(0, GROUP, prepare, 0)
        wait_recv(ch)

        def arrive(z, _):
            for half in range(halves):
                for t in range(NLAT // 128):
                    tiles = []
                    for n in range(per_tile):
                        g = t * per_tile + n
                        b, j = g // splits, g % splits
                        lane0 = (j * halves + half) * 128
                        tiles.append(
                            recv[
                                ch,
                                pl.ds(pl.multiple_of((b * levs + z) * rows, rows), rows),
                                lane0 : lane0 + 128,
                            ].astype(jnp.float32)
                        )
                    for il in range(per_tile):
                        level = z * lev_dev + half * per_tile + il
                        turn[t, pl.ds(pl.multiple_of(level * rows, rows), rows), :] = gather_pieces([rolled(tiles[n], n - il) for n in range(per_tile)])
            return 0

        lax.fori_loop(0, levs, arrive, 0)

        def direct(s, _):
            slot = ch * GROUP + s
            back_copy(slot).wait()
            waves_in = jnp.concatenate(
                [
                    jnp.concatenate(
                        [
                            turn[t, pl.ds(s * 4 + qr, LEV, stride=rows), :]
                            for t in range(NLAT // 128)
                        ],
                        axis=1,
                    )
                    for qr in range(4)
                ],
                axis=0,
            ).astype(jnp.bfloat16)
            coeffs = flat_dot(waves_in, stored[s]) * math.sqrt(2.0 / NLAT)
            second = consts_ref[slot, 0:1, :] > 0.5
            incr[s] = (
                jnp.where(second, coeffs[2 * LEV :], coeffs[: 2 * LEV]) * consts_ref[slot, 1:2, :]
            )
            spec[s] = back_buf[lax.rem(slot, 2)]

            @pl.when(slot + 2 < slots)
            def _():
                back_copy(slot + 2).start()

            return 0

        lax.fori_loop(0, GROUP, direct, 0)

        def step(k, _):
            def inverse(s, _):
                slot = ch * GROUP + s
                second = consts_ref[slot, 0:1, :] > 0.5
                inv = consts_ref[slot, pl.ds(2 + k, 1), :]
                mix = mix_ref[k][:, :LEV]
                now = [
                    jnp.dot(
                        mix,
                        spec[s, r * LEV : (r + 1) * LEV, :],
                        precision=lax.Precision.HIGHEST,
                        preferred_element_type=jnp.float32,
                    )
                    * inv
                    + weight_ref[k] * incr[s, r * LEV : (r + 1) * LEV, :]
                    for r in range(2)
                ]
                for r in range(2):
                    spec[s, r * LEV : (r + 1) * LEV, :] = now[r]
                means[k] += now[0][:, :128] * consts_ref[slot, 6:7, :128]
                both = jnp.concatenate(now, axis=0)
                split = jnp.concatenate(
                    [jnp.where(second, 0.0, both), jnp.where(second, both, 0.0)], axis=0
                ).astype(jnp.bfloat16)
                waves = lax.dot_general(
                    split, stored[s], LAST, preferred_element_type=jnp.float32
                ) * math.sqrt(2.0 / NT)
                for qr in range(4):
                    for t in range(NLAT // 128):
                        turn[t, pl.ds(s * 4 + qr, LEV, stride=rows), :] = waves[
                            qr * LEV : (qr + 1) * LEV, t * 128 : (t + 1) * 128
                        ]
                return 0

            lax.fori_loop(0, GROUP, inverse, 0)
            t_out = chunks + ch * STEPS + k

            def depart(z, _):
                for half in range(halves):
                    for t in range(NLAT // 128):
                        tiles = []
                        for il in range(per_tile):
                            level = z * lev_dev + half * per_tile + il
                            tiles.append(
                                turn[t, pl.ds(pl.multiple_of(level * rows, rows), rows), :]
                            )
                        for n in range(per_tile):
                            g = t * per_tile + n
                            b, j = g // splits, g % splits
                            lane0 = (j * halves + half) * 128
                            send[
                                t_out,
                                pl.ds(pl.multiple_of((b * levs + z) * rows, rows), rows),
                                lane0 : lane0 + 128,
                            ] = gather_pieces(
                                [rolled(tiles[il], il - n) for il in range(per_tile)]
                            ).astype(jnp.bfloat16)
                return 0

            lax.fori_loop(0, levs, depart, 0)
            send_all(t_out)
            return 0

        lax.fori_loop(0, STEPS, step, 0)
        return 0

    lax.fori_loop(0, chunks, chunk_body, 0)

    wide = 256
    sub = lax.broadcasted_iota(jnp.int32, (lev_dev, points), 0)
    in_level = lax.broadcasted_iota(jnp.int32, (lev_dev, points), 1) // piece % lev_dev == sub
    lane = lax.broadcasted_iota(jnp.int32, (lev_dev, 128), 1)
    own_lane = lev_id * lev_dev + lax.broadcasted_iota(jnp.int32, (lev_dev, 128), 0)
    low = -1e30

    def grid_part(k, lo, hi, add):
        def part(nb, _):
            at = pl.ds(pl.multiple_of(nb * wide, wide), wide)
            total = None
            for ch in range(lo, hi):
                one = flat_dot(
                    table_t[:, ch * cols : (ch + 1) * cols], recv[chunks + ch * STEPS + k, :, at]
                )
                total = one if total is None else total + one
            acc[:, at] = acc[:, at] + total if add else total
            return 0

        lax.fori_loop(0, points // wide, part, 0)

    def mass(k, tops_row, sums_row):
        tops, sums = [], []
        for nb in range(points // wide):
            tile = acc[:, nb * wide : (nb + 1) * wide]
            top = jnp.max(tile, axis=0, keepdims=True)
            tops.append(top)
            sums.append(jnp.sum(jnp.exp(tile - top), axis=0, keepdims=True))
        top = jnp.concatenate(tops, axis=1)
        total = jnp.concatenate(sums, axis=1) * row_weight
        level_top = jnp.max(jnp.where(in_level, top, low), axis=1, keepdims=True)
        level_sum = jnp.sum(
            jnp.where(in_level, total * jnp.exp(jnp.minimum(top - level_top, 0.0)), 0.0),
            axis=1,
            keepdims=True,
        )
        here = lane == own_lane + LEV * k
        tops_row = jnp.where(
            jnp.max(here.astype(jnp.float32), axis=0, keepdims=True) > 0.5,
            jnp.sum(jnp.where(here, level_top, 0.0), axis=0, keepdims=True),
            tops_row,
        )
        sums_row = sums_row + jnp.sum(jnp.where(here, level_sum, 0.0), axis=0, keepdims=True)
        return tops_row, sums_row

    def early(k, carry):
        def take(ch, _):
            wait_recv(chunks + ch * STEPS + k)
            return 0

        lax.fori_loop(0, chunks, take, 0)
        grid_part(k, 0, chunks, False)
        return mass(k, *carry)

    rows_now = (jnp.full((1, 128), low, jnp.float32), jnp.zeros((1, 128), jnp.float32))
    rows_now = lax.fori_loop(0, STEPS - 1, early, rows_now)
    k = STEPS - 1
    if chunks > 1:
        for ch in range(chunks - 1):
            wait_recv(chunks + ch * STEPS + k)
        grid_part(k, 0, chunks - 1, False)
    wait_recv(chunks + (chunks - 1) * STEPS + k)
    grid_part(k, chunks - 1, chunks, chunks > 1)
    grid_out = pltpu.make_async_copy(acc, grid_ref, out_sem)
    grid_out.start()
    tops_row, sums_row = mass(k, *rows_now)

    wide_lane = lax.broadcasted_iota(jnp.int32, (LEV, 128), 1)
    diag = lax.broadcasted_iota(jnp.int32, (LEV, 128), 0)
    means_row = jnp.zeros((1, 128), jnp.float32)
    for n in range(STEPS):
        column = jnp.sum(jnp.where(wide_lane == 0, means[n], 0.0), axis=1, keepdims=True)
        means_row = means_row + jnp.sum(
            jnp.where(wide_lane == diag + LEV * n, column, 0.0), axis=0, keepdims=True
        )
    stat_send[0:1, :] = tops_row
    stat_send[1:2, :] = sums_row
    stat_send[2:3, :] = means_row
    stat_send[3:4, :] = jnp.zeros((1, 128), jnp.float32)

    def stat_one(o, _):
        db, dz = peer(o)
        pltpu.make_async_remote_copy(
            src_ref=stat_send,
            dst_ref=stat_recv.at[me],
            send_sem=stat_sem.at[0],
            recv_sem=stat_sem.at[1],
            device_id=(db, dz),
            device_id_type=MESH,
        ).start()
        return 0

    lax.fori_loop(1, devs, stat_one, 0)
    pltpu.make_async_copy(stat_send, stat_recv.at[me], stat_sem.at[1]).start()

    def finish(t, _):
        left = send.at[t, pl.ds(0, (devs - 1) * rows), :]
        pltpu.make_async_copy(left, left, send_sem.at[t]).wait()
        return 0

    lax.fori_loop(0, chunks * (1 + STEPS), finish, 0)
    pltpu.make_async_copy(stat_recv, stat_recv, stat_sem.at[1]).wait()

    def find_top(d, best):
        return jnp.maximum(best, stat_recv[d, 0:1, :])

    best = lax.fori_loop(0, devs, find_top, jnp.full((1, 128), low, jnp.float32))

    def add_up(d, carry):
        total, base = carry
        return (
            total + stat_recv[d, 1:2, :] * jnp.exp(stat_recv[d, 0:1, :] - best),
            base + stat_recv[d, 2:3, :],
        )

    zero_row = jnp.zeros((1, 128), jnp.float32)
    total, base = lax.fori_loop(0, devs, add_up, (zero_row, zero_row))

    lane8 = lax.broadcasted_iota(jnp.int32, (8, 128), 1)
    is_level = lane8 < LEV
    level_weight = jnp.where(
        is_level, 1.0 + 2.0 * lane8.astype(jnp.float32) / (LEV - 1), 0.0
    )
    to_grid = target_ref[1]
    normaliser = target_ref[2]
    fix_scale = math.sqrt(NT * NLON) / 2.0
    best = jnp.broadcast_to(best, (8, 128))
    total = jnp.broadcast_to(total, (8, 128))
    base = jnp.broadcast_to(base, (8, 128))
    carried = jnp.zeros((8, 128), jnp.float32)
    shift = carried
    fixes = carried
    for n in range(STEPS):
        back = (128 - LEV * n) % 128
        best_n, total_n, base_n = [
            pltpu.roll(x, back, 1) if back else x for x in (best, total, base)
        ]
        column = jnp.sum(mix_ref[n] * carried[0:1], axis=1, keepdims=True)
        moved_by = jnp.broadcast_to(
            jnp.sum(jnp.where(wide_lane == diag, column, 0.0), axis=0, keepdims=True), (8, 128)
        )
        moved = (base_n + moved_by).astype(jnp.bfloat16).astype(jnp.float32) - base_n.astype(
            jnp.bfloat16
        ).astype(jnp.float32)
        shift = jnp.where(is_level, moved * to_grid, 0.0)
        mass_n = jnp.sum(
            jnp.where(
                is_level, jnp.exp(jnp.where(is_level, best_n + shift, 0.0)) * total_n, 0.0
            )
            * level_weight,
            axis=1,
            keepdims=True,
        )
        fix = jnp.log(target_ref[0] / (mass_n / normaliser))
        fixes = jnp.where(lane8 == n, fix, fixes)
        carried = jnp.where(is_level, moved_by + fix * fix_scale, 0.0)
    fix_ref[...] = fixes
    own = jnp.sum(jnp.where(lane == own_lane, shift[0:1], 0.0), axis=1, keepdims=True)
    shift_ref[...] = jnp.broadcast_to(own, (lev_dev, 128))

    pltpu.make_async_copy(
        stat_recv.at[pl.ds(0, devs - 1)], stat_recv.at[pl.ds(0, devs - 1)], stat_sem.at[0]
    ).wait()
    grid_out.wait()


def finish_kernel(shift_ref, grid_ref, out_ref):
    first = pl.program_id(0) * out_ref.shape[0]
    turned = grid_ref[...].T
    for n in range(out_ref.shape[0]):
        out_ref[n, 0] = (
            turned[n * 32 : (n + 1) * 32] + shift_ref[pl.ds(first + n, 1), 0:1]
        ).astype(jnp.bfloat16)


def table_factors(wavenumber, quarter, points, axis):
    phase = (wavenumber * points + quarter) % NLON
    angle = phase.astype(jnp.float32) * (2.0 * math.pi / NLON)
    return jnp.cos(angle), jnp.sin(angle)


def body(
    increment, background, legendre, coupling, damping, target_mass, numerators, pair_low, lat_map
):
    band_count = lax.axis_size("band")
    lev_count = lax.axis_size("lev")
    devs = band_count * lev_count
    lev_dev, lat_dev = increment.shape[:2]
    pair_dev = legendre.shape[0]
    points = lev_dev * lat_dev
    cols = devs * 4 * GROUP
    fits = (
        lat_dev % 32 == 0
        and pair_dev % GROUP == 0
        and lev_dev == 8
        and points % 256 == 0
        and LEV * STEPS == 128
    )
    if not fits:
        return body_general(
            increment,
            background,
            legendre,
            coupling,
            damping,
            target_mass,
            numerators,
            pair_low,
            lat_map,
        )
    chunks = pair_dev // GROUP
    band_id = lax.axis_index("band")
    lev_id = lax.axis_index("lev")

    low = pair_low.reshape(devs, chunks, GROUP).transpose(1, 0, 2).reshape(-1)
    column = jnp.arange(4 * low.shape[0], dtype=jnp.int32)
    wave = jnp.repeat(low, 4)
    wave = jnp.where(column // 2 % 2 == 0, wave, NT - wave)
    quarter = column % 2 * (NLON // 4)
    coarse = jnp.arange(NLON // 128, dtype=jnp.int32) * 128
    fine = jnp.arange(128, dtype=jnp.int32)
    norm = math.sqrt(2.0 / NLON)
    cos_a, sin_a = table_factors(wave[:, None], quarter[:, None], coarse[None, :], 1)
    cos_b, sin_b = table_factors(wave[:, None], 0, fine[None, :], 1)
    cos_a, sin_a = cos_a * norm, sin_a * norm
    cos_at, sin_at = table_factors(wave[None, :], quarter[None, :], coarse[:, None], 0)
    cos_bt, sin_bt = table_factors(wave[None, :], 0, fine[:, None], 0)
    cos_at, sin_at = cos_at * norm, sin_at * norm

    local_lats = lax.dynamic_slice_in_dim(lat_map, band_id * lat_dev, lat_dev)
    row_weight = lat_weights(local_lats).reshape(lat_dev // 32, 1, 32)
    row_weight = jnp.broadcast_to(row_weight, (lat_dev // 32, lev_dev, 32)).reshape(1, points)
    own_pairs = lax.dynamic_slice_in_dim(
        pair_low, (band_id * lev_count + lev_id) * pair_dev, pair_dev
    )
    degree, in_second = degrees(own_pairs)
    holder = jnp.broadcast_to((own_pairs == 0).astype(jnp.float32)[:, None], degree.shape)
    shape_term = degree * (degree + 1.0) / (NT * (NT + 1.0))
    consts = jnp.stack(
        [in_second.astype(jnp.float32), 1.0 / (1.0 + (degree / NT) ** 4)]
        + [1.0 / (1.0 + damping[n] * shape_term) for n in range(STEPS)]
        + [holder, holder],
        axis=1,
    )
    eye = jnp.eye(LEV, dtype=jnp.float32)
    mix = jnp.pad(0.7 * eye + 0.4 * coupling, ((0, 0), (0, 0), (0, 128 - LEV)))
    all_levels = 1.0 + 2.0 * jnp.arange(LEV, dtype=jnp.float32) / (LEV - 1)
    normaliser = (
        jnp.sum(all_levels) * jnp.sum(lat_weights(jnp.arange(NLAT, dtype=jnp.int32))) * NLON
    )
    table_entry = jnp.full((), norm, jnp.bfloat16).astype(jnp.float32)
    scalars = jnp.stack([target_mass[0], math.sqrt(2.0 / NT) * table_entry, normaliser])
    weights = numerators.astype(jnp.float32) / DEN

    vmem = pl.BlockSpec(memory_space=pltpu.VMEM)
    smem = pl.BlockSpec(memory_space=pltpu.SMEM)
    hbm = pl.BlockSpec(memory_space=pl.ANY)
    total = chunks * (1 + STEPS)
    dma = pltpu.SemaphoreType.DMA
    grid_t, fixes, shift = pl.pallas_call(
        lambda *refs: exchange_kernel(
            (band_count, lev_count, lev_dev, lat_dev, chunks), *refs
        ),
        out_shape=(
            jax.ShapeDtypeStruct((NLON, points), jnp.float32),
            jax.ShapeDtypeStruct((8, 128), jnp.float32),
            jax.ShapeDtypeStruct((lev_dev, 128), jnp.float32),
        ),
        in_specs=[smem, smem, hbm, hbm, hbm] + [vmem] * 12,
        out_specs=(hbm, vmem, vmem),
        scratch_shapes=[
            pltpu.VMEM((points, NLON), jnp.bfloat16),
            pltpu.VMEM((cols, NLON), jnp.bfloat16),
            pltpu.VMEM((NLON, chunks * cols), jnp.bfloat16),
            pltpu.VMEM((NLAT, NLAT), jnp.bfloat16),
            pltpu.VMEM((2, NLAT, NT + 2), jnp.bfloat16),
            pltpu.VMEM((GROUP, NLAT, NT + 2), jnp.bfloat16),
            pltpu.VMEM((2, 2 * LEV, NT + 2), jnp.float32),
            pltpu.VMEM((GROUP, 2 * LEV, NT + 2), jnp.float32),
            pltpu.VMEM((GROUP, 2 * LEV, NT + 2), jnp.float32),
            pltpu.VMEM((NLAT // 128, LEV * 4 * GROUP, 128), jnp.float32),
            pltpu.VMEM((NLON, points), jnp.float32),
            pltpu.VMEM((total, cols, points), jnp.bfloat16),
            pltpu.VMEM((total, cols, points), jnp.bfloat16),
            pltpu.VMEM((STEPS, LEV, 128), jnp.float32),
            pltpu.VMEM((4, 128), jnp.float32),
            pltpu.VMEM((devs, 4, 128), jnp.float32),
            dma,
            dma((2,)),
            dma((2,)),
            dma((total,)),
            dma((total,)),
            dma((2,)),
            dma,
        ],
        compiler_params=pltpu.CompilerParams(
            collective_id=0, has_side_effects=True, vmem_limit_bytes=67043328
        ),
    )(
        weights,
        scalars,
        increment,
        legendre,
        background.reshape(pair_dev, 2 * LEV, NT + 2),
        cos_a,
        sin_a,
        cos_b,
        sin_b,
        cos_at,
        sin_at,
        cos_bt,
        sin_bt,
        row_weight,
        lat_map[:, None],
        consts,
        mix,
    )

    halves = lev_dev // 4
    splits = lat_dev // 32
    analysis = pl.pallas_call(
        finish_kernel,
        grid=(halves, splits),
        in_specs=[
            pl.BlockSpec((lev_dev, 128), lambda h, j: (0, 0)),
            pl.BlockSpec((NLON, 128), lambda h, j: (0, j * halves + h)),
        ],
        out_specs=pl.BlockSpec((4, 1, 32, NLON), lambda h, j: (h, j, 0, 0)),
        out_shape=jax.ShapeDtypeStruct((lev_dev, splits, 32, NLON), jnp.bfloat16),
    )(shift, grid_t)
    return (analysis.reshape(lev_dev, lat_dev, NLON), fixes[0, :STEPS])


def solution(mesh):
    return jax.shard_map(
        body,
        mesh=mesh,
        in_specs=(
            P("lev", "band", None),
            P(("band", "lev"), None, None, None),
            P(("band", "lev"), None, None),
            P(),
            P(),
            P(),
            P(),
            P(),
            P(),
        ),
        out_specs=(P("lev", "band", None), P()),
        check_vma=False,
    )
```

```python
import math

import jax
import numpy as np
import jax.numpy as jnp
from jax import lax
from jax.experimental import pallas as pl
from jax.experimental.pallas import tpu as pltpu
from jax.sharding import PartitionSpec as P

NT = 767
NLAT = 768
NLON = 1536
LEV = 32
STEPS = 4
DEN = 64
NPAIR = 384
AXES = ("band", "lev")


def wave_table(pair_low):
    column = jnp.arange(4 * pair_low.shape[0], dtype=jnp.int32)
    low = jnp.repeat(pair_low, 4)
    wavenumber = jnp.where(column // 2 % 2 == 0, low, NT - low)[:, None]
    quarter = (column % 2 * (NLON // 4))[:, None]
    fine = math.gcd(128, NLON)
    unit = 2.0 * math.pi / NLON
    coarse_pts = jnp.arange(NLON // fine, dtype=jnp.int32)[None, :] * fine
    coarse = ((wavenumber * coarse_pts + quarter) % NLON).astype(jnp.float32) * unit
    rest = (wavenumber * jnp.arange(fine, dtype=jnp.int32)[None, :] % NLON).astype(
        jnp.float32
    ) * unit
    norm = math.sqrt(2.0 / NLON)
    cos_a, sin_a, cos_b, sin_b = lax.optimization_barrier(
        (jnp.cos(coarse) * norm, jnp.sin(coarse) * norm, jnp.cos(rest), jnp.sin(rest))
    )
    blocks = [
        cos_a[:, i : i + 1] * cos_b - sin_a[:, i : i + 1] * sin_b for i in range(NLON // fine)
    ]
    return jnp.concatenate(blocks, axis=1).astype(jnp.bfloat16)


def lat_weights(lat_rows):
    return jnp.cos(math.pi * ((lat_rows.astype(jnp.float32) + 0.5) / NLAT - 0.5))


def degrees(low_wave):
    columns = jnp.arange(NT + 2, dtype=jnp.int32)
    in_second = columns[None, :] >= NT + 1 - low_wave[:, None]
    degree = jnp.where(in_second, columns[None, :] - 1, low_wave[:, None] + columns[None, :])
    return (degree.astype(jnp.float32), in_second)


def body_general(
    increment, background, legendre, coupling, damping, target_mass, numerators, pair_low, lat_map
):
    band_count = lax.axis_size("band")
    lev_count = lax.axis_size("lev")
    device_count = band_count * lev_count
    band_id = lax.axis_index("band")
    lev_id = lax.axis_index("lev")
    lev_dev = increment.shape[0]
    lat_dev = increment.shape[1]
    pair_dev = legendre.shape[0]
    points = lev_dev * lat_dev
    fourier_tab = wave_table(pair_low)
    local_lats = lax.dynamic_slice_in_dim(lat_map, band_id * lat_dev, lat_dev)
    row_weight = lat_weights(local_lats)
    all_levels = 1.0 + 2.0 * jnp.arange(LEV, dtype=jnp.float32) / (LEV - 1)
    normaliser = (
        jnp.sum(all_levels) * jnp.sum(lat_weights(jnp.arange(NLAT, dtype=jnp.int32))) * NLON
    )
    fix_scale = math.sqrt(NT * NLON) / 2.0
    own_pairs = lax.dynamic_slice_in_dim(
        pair_low, (band_id * lev_count + lev_id) * pair_dev, pair_dev
    )
    degree, in_second = degrees(own_pairs)
    holder = (own_pairs == 0).astype(jnp.float32)

    fourier = jnp.einsum(
        "ck,xk->cx",
        fourier_tab,
        increment.reshape(points, NLON),
        preferred_element_type=jnp.float32,
    )
    fourier = (fourier * jnp.tile(row_weight, lev_dev)[None, :]).astype(jnp.bfloat16)
    received = lax.all_to_all(
        fourier.reshape(device_count, pair_dev * 4, points), AXES, split_axis=0, concat_axis=0
    )

    pick = (lat_map[:, None] == jnp.arange(NLAT, dtype=jnp.int32)[None, :]).astype(jnp.bfloat16)
    stored = jnp.einsum(
        "jn,pnc->pjc", pick, legendre, preferred_element_type=jnp.float32
    ).astype(jnp.bfloat16)

    received = received.reshape(band_count, lev_count, pair_dev * 4, lev_dev, lat_dev)
    waves_in = received.transpose(2, 1, 3, 0, 4).reshape(pair_dev, 4 * LEV, NLAT)
    coeffs = jnp.einsum("prj,pjc->prc", waves_in, stored, preferred_element_type=jnp.float32)
    coeffs = coeffs.reshape(pair_dev, 2, 2, LEV, NT + 2) * math.sqrt(2.0 / NLAT)
    second_cols = in_second[:, None, None, :]
    smoothing = 1.0 / (1.0 + (degree / NT) ** 4)
    incr_spec = jnp.where(second_cols, coeffs[:, 1], coeffs[:, 0]) * smoothing[:, None, None, :]
    shape_term = degree * (degree + 1.0) / (NT * (NT + 1.0))

    spectral = background
    means = []
    arrived = []
    for step_idx in range(STEPS):
        coupled = 0.7 * spectral + 0.4 * jnp.einsum(
            "lm,prmc->prlc", coupling[step_idx], spectral, precision=lax.Precision.HIGHEST
        )
        weight_now = numerators[step_idx].astype(jnp.float32) / DEN
        spectral = (
            coupled / (1.0 + damping[step_idx] * shape_term)[:, None, None, :]
            + weight_now * incr_spec
        )
        means.append(jnp.sum(spectral[:, 0, :, 0] * holder[:, None], axis=0))
        spec_bf = spectral.astype(jnp.bfloat16)
        zeros_bf = jnp.zeros_like(spec_bf)
        split_rows = jnp.stack(
            [jnp.where(second_cols, zeros_bf, spec_bf), jnp.where(second_cols, spec_bf, zeros_bf)],
            axis=1,
        )
        waves_f = jnp.einsum(
            "prc,pjc->prj",
            split_rows.reshape(pair_dev, 4 * LEV, NT + 2),
            stored,
            preferred_element_type=jnp.float32,
        )
        waves_bf = (waves_f * math.sqrt(2.0 / NT)).astype(jnp.bfloat16)
        outgoing = waves_bf.reshape(pair_dev * 4, lev_count, lev_dev, band_count, lat_dev)
        outgoing = outgoing.transpose(3, 1, 0, 2, 4).reshape(device_count, pair_dev * 4, points)
        spectral, outgoing = lax.optimization_barrier((spectral, outgoing))
        arrived.append(lax.all_to_all(outgoing, AXES, split_axis=0, concat_axis=0))

    tops, sums = [], []
    for step_idx in range(STEPS):
        grid_now = jnp.einsum(
            "cx,ck->xk",
            arrived[step_idx].reshape(NPAIR * 4, points),
            fourier_tab,
            preferred_element_type=jnp.float32,
        ).reshape(lev_dev, lat_dev, NLON)
        top = jnp.max(grid_now, axis=(1, 2))
        tops.append(top)
        sums.append(
            jnp.sum(
                jnp.sum(jnp.exp(grid_now - top[:, None, None]), axis=2) * row_weight[None, :],
                axis=1,
            )
        )

    packed = jnp.concatenate(
        [jnp.stack(tops).reshape(-1), jnp.stack(sums).reshape(-1), jnp.stack(means).reshape(-1)]
    )
    gathered = lax.all_to_all(
        jnp.broadcast_to(packed[None, :], (device_count, packed.shape[0])),
        AXES,
        split_axis=0,
        concat_axis=0,
    )
    count = STEPS * lev_dev
    all_tops = gathered[:, :count].reshape(band_count, lev_count, STEPS, lev_dev)
    all_sums = gathered[:, count : 2 * count].reshape(band_count, lev_count, STEPS, lev_dev)
    all_tops = all_tops.transpose(2, 0, 1, 3).reshape(STEPS, band_count, LEV)
    all_sums = all_sums.transpose(2, 0, 1, 3).reshape(STEPS, band_count, LEV)
    all_means = jnp.sum(gathered[:, 2 * count :], axis=0).reshape(STEPS, LEV)

    table_entry = jnp.full((), math.sqrt(2.0 / NLON), jnp.bfloat16).astype(jnp.float32)
    to_grid = math.sqrt(2.0 / NT) * table_entry
    carried = jnp.zeros((LEV,), jnp.float32)
    shift = jnp.zeros((LEV,), jnp.float32)
    fix_list = []
    for step_idx in range(STEPS):
        carried = 0.7 * carried + 0.4 * jnp.sum(coupling[step_idx] * carried[None, :], axis=1)
        base = all_means[step_idx]
        moved = (base + carried).astype(jnp.bfloat16).astype(jnp.float32) - base.astype(
            jnp.bfloat16
        ).astype(jnp.float32)
        shift = moved * to_grid
        total = jnp.sum(
            jnp.exp(all_tops[step_idx] + shift[None, :]) * all_sums[step_idx] * all_levels[None, :]
        )
        mass_fix = jnp.log(target_mass[0] / (total / normaliser))
        fix_list.append(mass_fix)
        carried = carried + mass_fix * fix_scale
    own_shift = lax.dynamic_slice_in_dim(shift, lev_id * lev_dev, lev_dev)
    analysis = (grid_now + own_shift[:, None, None]).astype(jnp.bfloat16)
    return (analysis, jnp.stack(fix_list))


GROUP = 4
MESH = pl.DeviceIdType.MESH
LAST = (((1,), (1,)), ((), ()))


def sine(x):
    y = x * x
    out = -1.0 / math.factorial(11)
    for n in (9, 7, 5, 3, 1):
        out = out * y + (1.0 if n % 4 == 1 else -1.0) / math.factorial(n)
    return out * x


def table_values(phase):
    turns = jnp.floor((phase + 0.5) * (1.0 / NLON))
    rest = jnp.abs(phase - turns * NLON - NLON / 2) - NLON / 4
    return (sine(rest * (2.0 * math.pi / NLON)) * math.sqrt(2.0 / NLON)).astype(jnp.bfloat16)


def flat_dot(a, b):
    return jnp.dot(a, b, preferred_element_type=jnp.float32)


def exchange_kernel(
    sizes,
    numer_ref,
    damp_ref,
    target_ref,
    inc_ref,
    leg_ref,
    back_ref,
    pair_ref,
    lat_ref,
    coupling_ref,
    grid_ref,
    fix_ref,
    shift_ref,
    consts_ref,
    mix_ref,
    points_in,
    table,
    table_t,
    pick,
    leg_buf,
    stored,
    back_buf,
    incr,
    spec,
    turn,
    acc,
    send,
    recv,
    means,
    stat_send,
    stat_recv,
    load_sem,
    leg_sem,
    back_sem,
    send_sem,
    recv_sem,
    stat_sem,
    out_sem,
):
    bands, levs, lev_dev, lat_dev, chunks = sizes
    devs = bands * levs
    band_id = lax.axis_index("band")
    lev_id = lax.axis_index("lev")
    me = band_id * levs + lev_id
    piece = 32
    splits = lat_dev // piece
    rows = 4 * GROUP
    cols = devs * rows
    points = lev_dev * lat_dev
    slots = chunks * GROUP
    per_tile = 128 // piece
    halves = lev_dev // per_tile

    barrier = pltpu.get_barrier_semaphore()

    def peer(o):
        return (
            lax.rem(band_id + lax.rem(o, bands), bands),
            lax.rem(lev_id + o // bands, levs),
        )

    def greet(o, _):
        pl.semaphore_signal(barrier, inc=1, device_id=peer(o), device_id_type=MESH)
        return 0

    lax.fori_loop(1, devs, greet, 0)

    def load_piece(i, j):
        return pltpu.make_async_copy(
            inc_ref.at[i, pl.ds(j * piece, piece), :],
            points_in.at[pl.ds((j * lev_dev + i) * piece, piece), :],
            load_sem,
        )

    for j in range(splits):
        for i in range(lev_dev):
            load_piece(i, j).start()

    def leg_copy(slot):
        return pltpu.make_async_copy(
            leg_ref.at[slot], leg_buf.at[lax.rem(slot, 2)], leg_sem.at[lax.rem(slot, 2)]
        )

    def back_copy(slot):
        return pltpu.make_async_copy(
            back_ref.at[slot], back_buf.at[lax.rem(slot, 2)], back_sem.at[lax.rem(slot, 2)]
        )

    for slot in range(2):
        leg_copy(slot).start()
        back_copy(slot).start()

    def message(t, o):
        db, dz = peer(o)
        return pltpu.make_async_remote_copy(
            src_ref=send.at[t, pl.ds((db * levs + dz) * rows, rows), :],
            dst_ref=recv.at[t, pl.ds(me * rows, rows), :],
            send_sem=send_sem.at[t],
            recv_sem=recv_sem.at[t],
            device_id=(db, dz),
            device_id_type=MESH,
        )

    def send_all(t):
        def one(o, _):
            message(t, o).start()
            return 0

        lax.fori_loop(1, devs, one, 0)
        pltpu.make_async_copy(
            send.at[t, pl.ds(me * rows, rows), :],
            recv.at[t, pl.ds(me * rows, rows), :],
            recv_sem.at[t],
        ).start()

    def wait_recv(t):
        pltpu.make_async_copy(recv.at[t], recv.at[t], recv_sem.at[t]).wait()

    lane_part = lax.broadcasted_iota(jnp.int32, (rows, 128), 1) // piece

    def gather_pieces(parts):
        out = parts[0]
        for n in range(1, per_tile):
            out = jnp.where(lane_part == n, parts[n], out)
        return out

    def rolled(x, amount):
        amount = amount * piece % 128
        return pltpu.roll(x, amount, 1) if amount else x

    lat_now = (lat_ref[...].astype(jnp.float32) + 0.5) / NLAT - 0.5
    lat_now = jnp.broadcast_to(sine((0.5 - jnp.abs(lat_now)) * math.pi), (rows, NLAT))
    weight_tiles = []
    for j in range(splits):
        tile = jnp.zeros((rows, 128), jnp.float32)
        for b in range(bands):
            t, n = (b * splits + j) // per_tile, (b * splits + j) % per_tile
            source = lat_now[:, t * 128 : (t + 1) * 128]
            part = gather_pieces([rolled(source, il - n) for il in range(per_tile)])
            tile = jnp.where(band_id == b, part, tile)
        weight_tiles += [tile] * halves
    row_weight = jnp.concatenate(weight_tiles, axis=1)[0:1]
    pairs = pair_ref[...].astype(jnp.float32)
    pair_count = pairs.shape[1]
    pair_dev = chunks * GROUP

    def fourier(ch, _):
        def fill(rb, _):
            col = rb * 128 + lax.broadcasted_iota(jnp.int32, (128, 1), 0)
            place = (col >> 4) * pair_dev + ch * GROUP + ((col & 15) >> 2)
            spot = lax.broadcasted_iota(jnp.int32, (128, pair_count), 1) == place
            wave = jnp.sum(jnp.where(spot, pairs, 0.0), axis=1, keepdims=True)
            wave = jnp.where((col & 2) == 0, wave, NT - wave)
            wave = jnp.broadcast_to(wave, (128, 128))
            quarter = ((col & 1) * (NLON // 4)).astype(jnp.float32)
            lanes = lax.broadcasted_iota(jnp.int32, (1, 128), 1).astype(jnp.float32)
            out = pl.multiple_of(rb * 128, 128)
            for kc in range(NLON // 128):
                table[pl.ds(out, 128), kc * 128 : (kc + 1) * 128] = table_values(
                    wave * (lanes + kc * 128.0) + quarter
                )
            return 0

        lax.fori_loop(0, cols // 128, fill, 0)

        @pl.when(ch == 0)
        def _():
            pltpu.make_async_copy(points_in, points_in, load_sem).wait()

        got = lax.dot_general(
            table[...], points_in[...], LAST, preferred_element_type=jnp.float32
        )
        send[ch] = (got * row_weight).astype(jnp.bfloat16)

        @pl.when(ch == 0)
        def _():
            pl.semaphore_wait(barrier, devs - 1)

        send_all(ch)
        return 0

    lax.fori_loop(0, chunks, fourier, 0)

    same = lax.broadcasted_iota(jnp.int32, (pair_count, pair_count), 0) == (
        lax.broadcasted_iota(jnp.int32, (pair_count, pair_count), 1)
    )
    pair_column = jnp.sum(jnp.where(same, pairs, 0.0), axis=1, keepdims=True)
    wave_rows, quarter_rows = [], []
    for n in range(chunks * cols // 128):
        lane = n * 128 + lax.broadcasted_iota(jnp.int32, (1, 128), 1)
        ch = n * 128 // cols
        place = ((lane - ch * cols) >> 4) * pair_dev + ch * GROUP + ((lane & 15) >> 2)
        spot = lax.broadcasted_iota(jnp.int32, (pair_count, 128), 0) == place
        wave = jnp.sum(jnp.where(spot, pair_column, 0.0), axis=0, keepdims=True)
        wave_rows.append(jnp.where((lane & 2) == 0, wave, NT - wave))
        quarter_rows.append(((lane & 1) * (NLON // 4)).astype(jnp.float32))

    def fill_t(kc, _):
        k_column = (kc * 128 + lax.broadcasted_iota(jnp.int32, (128, 128), 0)).astype(jnp.float32)
        for n in range(len(wave_rows)):
            table_t[
                pl.ds(pl.multiple_of(kc * 128, 128), 128), n * 128 : (n + 1) * 128
            ] = table_values(wave_rows[n] * k_column + quarter_rows[n])
        return 0

    lax.fori_loop(0, NLON // 128, fill_t, 0)
    pick[...] = (
        (lax.broadcasted_iota(jnp.int32, (NLAT, NLAT), 0) == lat_ref[...])
        .astype(jnp.float32)
        .astype(jnp.bfloat16)
    )
    means[...] = jnp.zeros_like(means)
    square = [lax.broadcasted_iota(jnp.int32, (LEV, LEV), n) for n in range(2)]
    for n in range(STEPS):
        mix_ref[n] = jnp.where(square[0] == square[1], 0.7, 0.0) + 0.4 * coupling_ref[n]

    def chunk_body(ch, _):
        def prepare(s, _):
            slot = ch * GROUP + s
            leg_copy(slot).wait()
            stored[s] = flat_dot(leg_buf[lax.rem(slot, 2)], pick[...]).astype(jnp.bfloat16)
            spot = lax.broadcasted_iota(jnp.int32, (1, pair_count), 1) == me * pair_dev + slot
            low_wave = jnp.sum(jnp.where(spot, pairs, 0.0), axis=1, keepdims=True)
            column = lax.broadcasted_iota(jnp.int32, (1, NT + 2), 1).astype(jnp.float32)
            second = column >= NT + 1 - low_wave
            degree = jnp.where(second, column - 1.0, low_wave + column)
            ratio = degree / NT
            ratio = ratio * ratio
            shape_term = degree * (degree + 1.0) / (NT * (NT + 1.0))
            consts_ref[s, 0:1, :] = second.astype(jnp.float32)
            consts_ref[s, 1:2, :] = 1.0 / (1.0 + ratio * ratio)
            for n in range(STEPS):
                consts_ref[s, 2 + n : 3 + n, :] = 1.0 / (1.0 + damp_ref[n] * shape_term)
            consts_ref[s, 6:7, :] = jnp.broadcast_to(
                (low_wave == 0.0).astype(jnp.float32), (1, NT + 2)
            )

            @pl.when(slot + 2 < slots)
            def _():
                leg_copy(slot + 2).start()

            return 0

        lax.fori_loop(0, GROUP, prepare, 0)
        wait_recv(ch)

        def arrive(z, _):
            for half in range(halves):
                for t in range(NLAT // 128):
                    tiles = []
                    for n in range(per_tile):
                        g = t * per_tile + n
                        b, j = g // splits, g % splits
                        lane0 = (j * halves + half) * 128
                        tiles.append(
                            recv[
                                ch,
                                pl.ds(pl.multiple_of((b * levs + z) * rows, rows), rows),
                                lane0 : lane0 + 128,
                            ].astype(jnp.float32)
                        )
                    for il in range(per_tile):
                        level = z * lev_dev + half * per_tile + il
                        turn[t, pl.ds(pl.multiple_of(level * rows, rows), rows), :] = gather_pieces([rolled(tiles[n], n - il) for n in range(per_tile)])
            return 0

        lax.fori_loop(0, levs, arrive, 0)

        def direct(s, _):
            slot = ch * GROUP + s
            back_copy(slot).wait()
            waves_in = jnp.concatenate(
                [
                    jnp.concatenate(
                        [
                            turn[t, pl.ds(s * 4 + qr, LEV, stride=rows), :]
                            for t in range(NLAT // 128)
                        ],
                        axis=1,
                    )
                    for qr in range(4)
                ],
                axis=0,
            ).astype(jnp.bfloat16)
            coeffs = lax.dot_general(
                waves_in, stored[s], LAST, preferred_element_type=jnp.float32
            ) * math.sqrt(2.0 / NLAT)
            second = consts_ref[s, 0:1, :] > 0.5
            incr[s] = (
                jnp.where(second, coeffs[2 * LEV :], coeffs[: 2 * LEV]) * consts_ref[s, 1:2, :]
            )
            spec[s] = back_buf[lax.rem(slot, 2)]

            @pl.when(slot + 2 < slots)
            def _():
                back_copy(slot + 2).start()

            return 0

        lax.fori_loop(0, GROUP, direct, 0)

        def step(k, _):
            def inverse(s, _):
                second = consts_ref[s, 0:1, :] > 0.5
                inv = consts_ref[s, pl.ds(2 + k, 1), :]
                mix = mix_ref[k]
                weight = numer_ref[k].astype(jnp.float32) / DEN
                now = [
                    jnp.dot(
                        mix,
                        spec[s, r * LEV : (r + 1) * LEV, :],
                        precision=lax.Precision.HIGHEST,
                        preferred_element_type=jnp.float32,
                    )
                    * inv
                    + weight * incr[s, r * LEV : (r + 1) * LEV, :]
                    for r in range(2)
                ]
                for r in range(2):
                    spec[s, r * LEV : (r + 1) * LEV, :] = now[r]
                means[k] += now[0][:, :128] * consts_ref[s, 6:7, :128]
                both = jnp.concatenate(now, axis=0)
                split = jnp.concatenate(
                    [jnp.where(second, 0.0, both), jnp.where(second, both, 0.0)], axis=0
                ).astype(jnp.bfloat16)
                waves = flat_dot(split, stored[s]) * math.sqrt(2.0 / NT)
                for qr in range(4):
                    for t in range(NLAT // 128):
                        turn[t, pl.ds(s * 4 + qr, LEV, stride=rows), :] = waves[
                            qr * LEV : (qr + 1) * LEV, t * 128 : (t + 1) * 128
                        ]
                return 0

            lax.fori_loop(0, GROUP, inverse, 0)
            t_out = chunks + ch * STEPS + k

            def depart(z, _):
                for half in range(halves):
                    for t in range(NLAT // 128):
                        tiles = []
                        for il in range(per_tile):
                            level = z * lev_dev + half * per_tile + il
                            tiles.append(
                                turn[t, pl.ds(pl.multiple_of(level * rows, rows), rows), :]
                            )
                        for n in range(per_tile):
                            g = t * per_tile + n
                            b, j = g // splits, g % splits
                            lane0 = (j * halves + half) * 128
                            send[
                                t_out,
                                pl.ds(pl.multiple_of((b * levs + z) * rows, rows), rows),
                                lane0 : lane0 + 128,
                            ] = gather_pieces(
                                [rolled(tiles[il], il - n) for il in range(per_tile)]
                            ).astype(jnp.bfloat16)
                return 0

            lax.fori_loop(0, levs, depart, 0)
            send_all(t_out)
            return 0

        lax.fori_loop(0, STEPS, step, 0)
        return 0

    lax.fori_loop(0, chunks, chunk_body, 0)

    wide = 256
    sub = lax.broadcasted_iota(jnp.int32, (lev_dev, points), 0)
    in_level = lax.broadcasted_iota(jnp.int32, (lev_dev, points), 1) // piece % lev_dev == sub
    lane = lax.broadcasted_iota(jnp.int32, (lev_dev, 128), 1)
    own_lane = lev_id * lev_dev + lax.broadcasted_iota(jnp.int32, (lev_dev, 128), 0)
    low = -1e30

    def grid_part(k, lo, hi, add):
        def part(nb, _):
            at = pl.ds(pl.multiple_of(nb * wide, wide), wide)
            total = None
            for ch in range(lo, hi):
                one = flat_dot(
                    table_t[:, ch * cols : (ch + 1) * cols], recv[chunks + ch * STEPS + k, :, at]
                )
                total = one if total is None else total + one
            acc[:, at] = acc[:, at] + total if add else total
            return 0

        lax.fori_loop(0, points // wide, part, 0)

    def mass(k, tops_row, sums_row):
        tops, sums = [], []
        for nb in range(points // wide):
            tile = acc[:, nb * wide : (nb + 1) * wide]
            top = jnp.max(tile, axis=0, keepdims=True)
            tops.append(top)
            sums.append(jnp.sum(jnp.exp(tile - top), axis=0, keepdims=True))
        top = jnp.concatenate(tops, axis=1)
        total = jnp.concatenate(sums, axis=1) * row_weight
        level_top = jnp.max(jnp.where(in_level, top, low), axis=1, keepdims=True)
        level_sum = jnp.sum(
            jnp.where(in_level, total * jnp.exp(jnp.minimum(top - level_top, 0.0)), 0.0),
            axis=1,
            keepdims=True,
        )
        here = lane == own_lane + LEV * k
        tops_row = jnp.where(
            jnp.max(here.astype(jnp.float32), axis=0, keepdims=True) > 0.5,
            jnp.sum(jnp.where(here, level_top, 0.0), axis=0, keepdims=True),
            tops_row,
        )
        sums_row = sums_row + jnp.sum(jnp.where(here, level_sum, 0.0), axis=0, keepdims=True)
        return tops_row, sums_row

    def early(k, carry):
        def take(ch, _):
            wait_recv(chunks + ch * STEPS + k)
            return 0

        lax.fori_loop(0, chunks, take, 0)
        grid_part(k, 0, chunks, False)
        return mass(k, *carry)

    rows_now = (jnp.full((1, 128), low, jnp.float32), jnp.zeros((1, 128), jnp.float32))
    rows_now = lax.fori_loop(0, STEPS - 1, early, rows_now)
    k = STEPS - 1
    if chunks > 1:
        for ch in range(chunks - 1):
            wait_recv(chunks + ch * STEPS + k)
        grid_part(k, 0, chunks - 1, False)
    wait_recv(chunks + (chunks - 1) * STEPS + k)
    grid_part(k, chunks - 1, chunks, chunks > 1)
    grid_out = pltpu.make_async_copy(acc, grid_ref, out_sem)
    grid_out.start()
    tops_row, sums_row = mass(k, *rows_now)

    wide_lane = lax.broadcasted_iota(jnp.int32, (LEV, 128), 1)
    diag = lax.broadcasted_iota(jnp.int32, (LEV, 128), 0)
    means_row = jnp.zeros((1, 128), jnp.float32)
    for n in range(STEPS):
        column = jnp.sum(jnp.where(wide_lane == 0, means[n], 0.0), axis=1, keepdims=True)
        means_row = means_row + jnp.sum(
            jnp.where(wide_lane == diag + LEV * n, column, 0.0), axis=0, keepdims=True
        )
    stat_send[0:1, :] = tops_row
    stat_send[1:2, :] = sums_row
    stat_send[2:3, :] = means_row
    stat_send[3:4, :] = jnp.zeros((1, 128), jnp.float32)

    def stat_one(o, _):
        db, dz = peer(o)
        pltpu.make_async_remote_copy(
            src_ref=stat_send,
            dst_ref=stat_recv.at[me],
            send_sem=stat_sem.at[0],
            recv_sem=stat_sem.at[1],
            device_id=(db, dz),
            device_id_type=MESH,
        ).start()
        return 0

    lax.fori_loop(1, devs, stat_one, 0)
    pltpu.make_async_copy(stat_send, stat_recv.at[me], stat_sem.at[1]).start()

    def finish(t, _):
        left = send.at[t, pl.ds(0, (devs - 1) * rows), :]
        pltpu.make_async_copy(left, left, send_sem.at[t]).wait()
        return 0

    lax.fori_loop(0, chunks * (1 + STEPS), finish, 0)
    pltpu.make_async_copy(stat_recv, stat_recv, stat_sem.at[1]).wait()

    def find_top(d, best):
        return jnp.maximum(best, stat_recv[d, 0:1, :])

    best = lax.fori_loop(0, devs, find_top, jnp.full((1, 128), low, jnp.float32))

    def add_up(d, carry):
        total, base = carry
        return (
            total + stat_recv[d, 1:2, :] * jnp.exp(stat_recv[d, 0:1, :] - best),
            base + stat_recv[d, 2:3, :],
        )

    zero_row = jnp.zeros((1, 128), jnp.float32)
    total, base = lax.fori_loop(0, devs, add_up, (zero_row, zero_row))

    lane8 = lax.broadcasted_iota(jnp.int32, (8, 128), 1)
    is_level = lane8 < LEV
    level_weight = jnp.where(
        is_level, 1.0 + 2.0 * lane8.astype(jnp.float32) / (LEV - 1), 0.0
    )
    to_grid = math.sqrt(2.0 / NT) * float(np.float32(math.sqrt(2.0 / NLON)).astype(jnp.bfloat16))
    lat_sum = sum(math.cos(math.pi * ((n + 0.5) / NLAT - 0.5)) for n in range(NLAT))
    normaliser = sum(1.0 + 2.0 * n / (LEV - 1) for n in range(LEV)) * lat_sum * NLON
    fix_scale = math.sqrt(NT * NLON) / 2.0
    best = jnp.broadcast_to(best, (8, 128))
    total = jnp.broadcast_to(total, (8, 128))
    base = jnp.broadcast_to(base, (8, 128))
    carried = jnp.zeros((8, 128), jnp.float32)
    shift = carried
    for n in range(STEPS):
        back = (128 - LEV * n) % 128
        best_n, total_n, base_n = [
            pltpu.roll(x, back, 1) if back else x for x in (best, total, base)
        ]
        column = jnp.sum(mix_ref[n] * carried[0:1, :LEV], axis=1, keepdims=True)
        moved_by = jnp.broadcast_to(
            jnp.sum(jnp.where(wide_lane == diag, column, 0.0), axis=0, keepdims=True), (8, 128)
        )
        moved = (base_n + moved_by).astype(jnp.bfloat16).astype(jnp.float32) - base_n.astype(
            jnp.bfloat16
        ).astype(jnp.float32)
        shift = jnp.where(is_level, moved * to_grid, 0.0)
        mass_n = jnp.sum(
            jnp.where(
                is_level, jnp.exp(jnp.where(is_level, best_n + shift, 0.0)) * total_n, 0.0
            )
            * level_weight,
            axis=1,
            keepdims=True,
        )
        fix = jnp.log(target_ref[0] / (mass_n / normaliser))
        fix_ref[n] = fix[0, 0]
        carried = jnp.where(is_level, moved_by + fix * fix_scale, 0.0)
    own = jnp.sum(jnp.where(lane == own_lane, shift[0:1], 0.0), axis=1, keepdims=True)
    shift_ref[...] = jnp.broadcast_to(own, (lev_dev, 128))

    pltpu.make_async_copy(
        stat_recv.at[pl.ds(0, devs - 1)], stat_recv.at[pl.ds(0, devs - 1)], stat_sem.at[0]
    ).wait()
    grid_out.wait()


def finish_kernel(fix_ref, shift_ref, grid_ref, out_ref, fix_out):
    for n in range(STEPS):
        fix_out[n] = fix_ref[n]
    first = pl.program_id(0) * out_ref.shape[0]
    turned = grid_ref[...].T
    for n in range(out_ref.shape[0]):
        out_ref[n, 0] = (
            turned[n * 32 : (n + 1) * 32] + shift_ref[pl.ds(first + n, 1), 0:1]
        ).astype(jnp.bfloat16)


def body(
    increment, background, legendre, coupling, damping, target_mass, numerators, pair_low, lat_map
):
    band_count = lax.axis_size("band")
    lev_count = lax.axis_size("lev")
    devs = band_count * lev_count
    lev_dev, lat_dev = increment.shape[:2]
    pair_dev = legendre.shape[0]
    points = lev_dev * lat_dev
    cols = devs * 4 * GROUP
    fits = (
        lat_dev % 32 == 0
        and pair_dev % GROUP == 0
        and lev_dev == 8
        and points % 256 == 0
        and LEV * STEPS == 128
    )
    if not fits:
        return body_general(
            increment,
            background,
            legendre,
            coupling,
            damping,
            target_mass,
            numerators,
            pair_low,
            lat_map,
        )
    chunks = pair_dev // GROUP
    vmem = pl.BlockSpec(memory_space=pltpu.VMEM)
    smem = pl.BlockSpec(memory_space=pltpu.SMEM)
    hbm = pl.BlockSpec(memory_space=pl.ANY)
    total = chunks * (1 + STEPS)
    dma = pltpu.SemaphoreType.DMA
    grid_t, fixes, shift = pl.pallas_call(
        lambda *refs: exchange_kernel(
            (band_count, lev_count, lev_dev, lat_dev, chunks), *refs
        ),
        out_shape=(
            jax.ShapeDtypeStruct((NLON, points), jnp.float32),
            jax.ShapeDtypeStruct((STEPS,), jnp.float32),
            jax.ShapeDtypeStruct((lev_dev, 128), jnp.float32),
        ),
        in_specs=[smem] * 3 + [hbm] * 3 + [vmem] * 3,
        out_specs=(hbm, smem, vmem),
        scratch_shapes=[
            pltpu.VMEM((GROUP, 8, NT + 2), jnp.float32),
            pltpu.VMEM((STEPS, LEV, LEV), jnp.float32),
            pltpu.VMEM((points, NLON), jnp.bfloat16),
            pltpu.VMEM((cols, NLON), jnp.bfloat16),
            pltpu.VMEM((NLON, chunks * cols), jnp.bfloat16),
            pltpu.VMEM((NLAT, NLAT), jnp.bfloat16),
            pltpu.VMEM((2, NT + 2, NLAT), jnp.bfloat16),
            pltpu.VMEM((GROUP, NT + 2, NLAT), jnp.bfloat16),
            pltpu.VMEM((2, 2 * LEV, NT + 2), jnp.float32),
            pltpu.VMEM((GROUP, 2 * LEV, NT + 2), jnp.float32),
            pltpu.VMEM((GROUP, 2 * LEV, NT + 2), jnp.float32),
            pltpu.VMEM((NLAT // 128, LEV * 4 * GROUP, 128), jnp.float32),
            pltpu.VMEM((NLON, points), jnp.float32),
            pltpu.VMEM((total, cols, points), jnp.bfloat16),
            pltpu.VMEM((total, cols, points), jnp.bfloat16),
            pltpu.VMEM((STEPS, LEV, 128), jnp.float32),
            pltpu.VMEM((4, 128), jnp.float32),
            pltpu.VMEM((devs, 4, 128), jnp.float32),
            dma,
            dma((2,)),
            dma((2,)),
            dma((total,)),
            dma((total,)),
            dma((2,)),
            dma,
        ],
        compiler_params=pltpu.CompilerParams(
            collective_id=0, has_side_effects=True, vmem_limit_bytes=67043328
        ),
    )(
        numerators,
        damping,
        target_mass,
        increment,
        legendre.transpose(0, 2, 1),
        background.reshape(pair_dev, 2 * LEV, NT + 2),
        pair_low[None, :],
        lat_map[None, :],
        coupling,
    )

    halves = lev_dev // 4
    splits = lat_dev // 32
    analysis, fixes = pl.pallas_call(
        finish_kernel,
        grid=(halves, splits),
        in_specs=[
            smem,
            pl.BlockSpec((lev_dev, 128), lambda h, j: (0, 0)),
            pl.BlockSpec((NLON, 128), lambda h, j: (0, j * halves + h)),
        ],
        out_specs=(pl.BlockSpec((4, 1, 32, NLON), lambda h, j: (h, j, 0, 0)), smem),
        out_shape=(
            jax.ShapeDtypeStruct((lev_dev, splits, 32, NLON), jnp.bfloat16),
            jax.ShapeDtypeStruct((STEPS,), jnp.float32),
        ),
    )(fixes, shift, grid_t)
    return (analysis.reshape(lev_dev, lat_dev, NLON), fixes)


def solution(mesh):
    return jax.shard_map(
        body,
        mesh=mesh,
        in_specs=(
            P("lev", "band", None),
            P(("band", "lev"), None, None, None),
            P(("band", "lev"), None, None),
            P(),
            P(),
            P(),
            P(),
            P(),
            P(),
        ),
        out_specs=(P("lev", "band", None), P()),
        check_vma=False,
    )
```

```python
import math

import jax
import numpy as np
import jax.numpy as jnp
from jax import lax
from jax.experimental import pallas as pl
from jax.experimental.pallas import tpu as pltpu
from jax.sharding import PartitionSpec as P

NT = 767
NLAT = 768
NLON = 1536
LEV = 32
STEPS = 4
DEN = 64
NPAIR = 384
AXES = ("band", "lev")


def wave_table(pair_low):
    column = jnp.arange(4 * pair_low.shape[0], dtype=jnp.int32)
    low = jnp.repeat(pair_low, 4)
    wavenumber = jnp.where(column // 2 % 2 == 0, low, NT - low)[:, None]
    quarter = (column % 2 * (NLON // 4))[:, None]
    fine = math.gcd(128, NLON)
    unit = 2.0 * math.pi / NLON
    coarse_pts = jnp.arange(NLON // fine, dtype=jnp.int32)[None, :] * fine
    coarse = ((wavenumber * coarse_pts + quarter) % NLON).astype(jnp.float32) * unit
    rest = (wavenumber * jnp.arange(fine, dtype=jnp.int32)[None, :] % NLON).astype(
        jnp.float32
    ) * unit
    norm = math.sqrt(2.0 / NLON)
    cos_a, sin_a, cos_b, sin_b = lax.optimization_barrier(
        (jnp.cos(coarse) * norm, jnp.sin(coarse) * norm, jnp.cos(rest), jnp.sin(rest))
    )
    blocks = [
        cos_a[:, i : i + 1] * cos_b - sin_a[:, i : i + 1] * sin_b for i in range(NLON // fine)
    ]
    return jnp.concatenate(blocks, axis=1).astype(jnp.bfloat16)


def lat_weights(lat_rows):
    return jnp.cos(math.pi * ((lat_rows.astype(jnp.float32) + 0.5) / NLAT - 0.5))


def degrees(low_wave):
    columns = jnp.arange(NT + 2, dtype=jnp.int32)
    in_second = columns[None, :] >= NT + 1 - low_wave[:, None]
    degree = jnp.where(in_second, columns[None, :] - 1, low_wave[:, None] + columns[None, :])
    return (degree.astype(jnp.float32), in_second)


def body_general(
    increment, background, legendre, coupling, damping, target_mass, numerators, pair_low, lat_map
):
    band_count = lax.axis_size("band")
    lev_count = lax.axis_size("lev")
    device_count = band_count * lev_count
    band_id = lax.axis_index("band")
    lev_id = lax.axis_index("lev")
    lev_dev = increment.shape[0]
    lat_dev = increment.shape[1]
    pair_dev = legendre.shape[0]
    points = lev_dev * lat_dev
    fourier_tab = wave_table(pair_low)
    local_lats = lax.dynamic_slice_in_dim(lat_map, band_id * lat_dev, lat_dev)
    row_weight = lat_weights(local_lats)
    all_levels = 1.0 + 2.0 * jnp.arange(LEV, dtype=jnp.float32) / (LEV - 1)
    normaliser = (
        jnp.sum(all_levels) * jnp.sum(lat_weights(jnp.arange(NLAT, dtype=jnp.int32))) * NLON
    )
    fix_scale = math.sqrt(NT * NLON) / 2.0
    own_pairs = lax.dynamic_slice_in_dim(
        pair_low, (band_id * lev_count + lev_id) * pair_dev, pair_dev
    )
    degree, in_second = degrees(own_pairs)
    holder = (own_pairs == 0).astype(jnp.float32)

    fourier = jnp.einsum(
        "ck,xk->cx",
        fourier_tab,
        increment.reshape(points, NLON),
        preferred_element_type=jnp.float32,
    )
    fourier = (fourier * jnp.tile(row_weight, lev_dev)[None, :]).astype(jnp.bfloat16)
    received = lax.all_to_all(
        fourier.reshape(device_count, pair_dev * 4, points), AXES, split_axis=0, concat_axis=0
    )

    pick = (lat_map[:, None] == jnp.arange(NLAT, dtype=jnp.int32)[None, :]).astype(jnp.bfloat16)
    stored = jnp.einsum(
        "jn,pnc->pjc", pick, legendre, preferred_element_type=jnp.float32
    ).astype(jnp.bfloat16)

    received = received.reshape(band_count, lev_count, pair_dev * 4, lev_dev, lat_dev)
    waves_in = received.transpose(2, 1, 3, 0, 4).reshape(pair_dev, 4 * LEV, NLAT)
    coeffs = jnp.einsum("prj,pjc->prc", waves_in, stored, preferred_element_type=jnp.float32)
    coeffs = coeffs.reshape(pair_dev, 2, 2, LEV, NT + 2) * math.sqrt(2.0 / NLAT)
    second_cols = in_second[:, None, None, :]
    smoothing = 1.0 / (1.0 + (degree / NT) ** 4)
    incr_spec = jnp.where(second_cols, coeffs[:, 1], coeffs[:, 0]) * smoothing[:, None, None, :]
    shape_term = degree * (degree + 1.0) / (NT * (NT + 1.0))

    spectral = background
    means = []
    arrived = []
    for step_idx in range(STEPS):
        coupled = 0.7 * spectral + 0.4 * jnp.einsum(
            "lm,prmc->prlc", coupling[step_idx], spectral, precision=lax.Precision.HIGHEST
        )
        weight_now = numerators[step_idx].astype(jnp.float32) / DEN
        spectral = (
            coupled / (1.0 + damping[step_idx] * shape_term)[:, None, None, :]
            + weight_now * incr_spec
        )
        means.append(jnp.sum(spectral[:, 0, :, 0] * holder[:, None], axis=0))
        spec_bf = spectral.astype(jnp.bfloat16)
        zeros_bf = jnp.zeros_like(spec_bf)
        split_rows = jnp.stack(
            [jnp.where(second_cols, zeros_bf, spec_bf), jnp.where(second_cols, spec_bf, zeros_bf)],
            axis=1,
        )
        waves_f = jnp.einsum(
            "prc,pjc->prj",
            split_rows.reshape(pair_dev, 4 * LEV, NT + 2),
            stored,
            preferred_element_type=jnp.float32,
        )
        waves_bf = (waves_f * math.sqrt(2.0 / NT)).astype(jnp.bfloat16)
        outgoing = waves_bf.reshape(pair_dev * 4, lev_count, lev_dev, band_count, lat_dev)
        outgoing = outgoing.transpose(3, 1, 0, 2, 4).reshape(device_count, pair_dev * 4, points)
        spectral, outgoing = lax.optimization_barrier((spectral, outgoing))
        arrived.append(lax.all_to_all(outgoing, AXES, split_axis=0, concat_axis=0))

    tops, sums = [], []
    for step_idx in range(STEPS):
        grid_now = jnp.einsum(
            "cx,ck->xk",
            arrived[step_idx].reshape(NPAIR * 4, points),
            fourier_tab,
            preferred_element_type=jnp.float32,
        ).reshape(lev_dev, lat_dev, NLON)
        top = jnp.max(grid_now, axis=(1, 2))
        tops.append(top)
        sums.append(
            jnp.sum(
                jnp.sum(jnp.exp(grid_now - top[:, None, None]), axis=2) * row_weight[None, :],
                axis=1,
            )
        )

    packed = jnp.concatenate(
        [jnp.stack(tops).reshape(-1), jnp.stack(sums).reshape(-1), jnp.stack(means).reshape(-1)]
    )
    gathered = lax.all_to_all(
        jnp.broadcast_to(packed[None, :], (device_count, packed.shape[0])),
        AXES,
        split_axis=0,
        concat_axis=0,
    )
    count = STEPS * lev_dev
    all_tops = gathered[:, :count].reshape(band_count, lev_count, STEPS, lev_dev)
    all_sums = gathered[:, count : 2 * count].reshape(band_count, lev_count, STEPS, lev_dev)
    all_tops = all_tops.transpose(2, 0, 1, 3).reshape(STEPS, band_count, LEV)
    all_sums = all_sums.transpose(2, 0, 1, 3).reshape(STEPS, band_count, LEV)
    all_means = jnp.sum(gathered[:, 2 * count :], axis=0).reshape(STEPS, LEV)

    table_entry = jnp.full((), math.sqrt(2.0 / NLON), jnp.bfloat16).astype(jnp.float32)
    to_grid = math.sqrt(2.0 / NT) * table_entry
    carried = jnp.zeros((LEV,), jnp.float32)
    shift = jnp.zeros((LEV,), jnp.float32)
    fix_list = []
    for step_idx in range(STEPS):
        carried = 0.7 * carried + 0.4 * jnp.sum(coupling[step_idx] * carried[None, :], axis=1)
        base = all_means[step_idx]
        moved = (base + carried).astype(jnp.bfloat16).astype(jnp.float32) - base.astype(
            jnp.bfloat16
        ).astype(jnp.float32)
        shift = moved * to_grid
        total = jnp.sum(
            jnp.exp(all_tops[step_idx] + shift[None, :]) * all_sums[step_idx] * all_levels[None, :]
        )
        mass_fix = jnp.log(target_mass[0] / (total / normaliser))
        fix_list.append(mass_fix)
        carried = carried + mass_fix * fix_scale
    own_shift = lax.dynamic_slice_in_dim(shift, lev_id * lev_dev, lev_dev)
    analysis = (grid_now + own_shift[:, None, None]).astype(jnp.bfloat16)
    return (analysis, jnp.stack(fix_list))


GROUP = 4
MESH = pl.DeviceIdType.MESH
LAST = (((1,), (1,)), ((), ()))


def sine(x):
    y = x * x
    out = -1.0 / math.factorial(11)
    for n in (9, 7, 5, 3, 1):
        out = out * y + (1.0 if n % 4 == 1 else -1.0) / math.factorial(n)
    return out * x


def table_values(phase):
    turns = jnp.floor((phase + 0.5) * (1.0 / NLON))
    rest = jnp.abs(phase - turns * NLON - NLON / 2) - NLON / 4
    return (sine(rest * (2.0 * math.pi / NLON)) * math.sqrt(2.0 / NLON)).astype(jnp.bfloat16)


def flat_dot(a, b):
    return jnp.dot(a, b, preferred_element_type=jnp.float32)


def exchange_kernel(
    sizes,
    numer_ref,
    damp_ref,
    target_ref,
    inc_ref,
    leg_ref,
    back_ref,
    pair_ref,
    lat_ref,
    coupling_ref,
    out_ref,
    fix_ref,
    consts_ref,
    mix_ref,
    points_in,
    table,
    pick,
    leg_buf,
    stored,
    back_buf,
    incr,
    spec,
    turn,
    acc,
    send,
    recv,
    means,
    weight_rows,
    early_send,
    early_recv,
    late_send,
    late_recv,
    load_sem,
    leg_sem,
    back_sem,
    send_sem,
    recv_sem,
    early_sem,
    late_sem,
    out_sem,
):
    bands, levs, lev_dev, lat_dev, chunks = sizes
    devs = bands * levs
    band_id = lax.axis_index("band")
    lev_id = lax.axis_index("lev")
    me = band_id * levs + lev_id
    piece = 32
    splits = lat_dev // piece
    rows = 4 * GROUP
    cols = devs * rows
    points = lev_dev * lat_dev
    slots = chunks * GROUP
    per_tile = 128 // piece
    halves = lev_dev // per_tile

    barrier = pltpu.get_barrier_semaphore()

    def peer(o):
        return (
            lax.rem(band_id + lax.rem(o, bands), bands),
            lax.rem(lev_id + o // bands, levs),
        )

    def greet(o, _):
        pl.semaphore_signal(barrier, inc=1, device_id=peer(o), device_id_type=MESH)
        return 0

    lax.fori_loop(1, devs, greet, 0)

    def load_piece(i, j):
        return pltpu.make_async_copy(
            inc_ref.at[i, pl.ds(j * piece, piece), :],
            points_in.at[pl.ds((j * lev_dev + i) * piece, piece), :],
            load_sem,
        )

    for j in range(splits):
        for i in range(lev_dev):
            load_piece(i, j).start()

    def leg_copy(slot):
        return pltpu.make_async_copy(
            leg_ref.at[slot], leg_buf.at[lax.rem(slot, 2)], leg_sem.at[lax.rem(slot, 2)]
        )

    def back_copy(slot):
        return pltpu.make_async_copy(
            back_ref.at[slot], back_buf.at[lax.rem(slot, 2)], back_sem.at[lax.rem(slot, 2)]
        )

    for slot in range(2):
        leg_copy(slot).start()
        back_copy(slot).start()

    home = pl.ds((lev_id * bands + band_id) * rows, rows)

    def send_level(t, z):
        def one(o, _):
            band = lax.rem(band_id + o, bands)
            block = send.at[t, pl.ds((z * bands + band) * rows, rows), :]
            own = jnp.logical_and(o == 0, z == lev_id)

            @pl.when(own)
            def _():
                pltpu.make_async_copy(block, recv.at[t, home, :], recv_sem.at[t]).start()

            @pl.when(jnp.logical_not(own))
            def _():
                pltpu.make_async_remote_copy(
                    src_ref=block,
                    dst_ref=recv.at[t, home, :],
                    send_sem=send_sem.at[t],
                    recv_sem=recv_sem.at[t],
                    device_id=(band, z),
                    device_id_type=MESH,
                ).start()

            return 0

        lax.fori_loop(0, bands, one, 0)

    def level_order(n):
        return lax.rem(lev_id + levs // 2 + n, levs)

    def wait_recv(t):
        pltpu.make_async_copy(recv.at[t], recv.at[t], recv_sem.at[t]).wait()

    lane_part = lax.broadcasted_iota(jnp.int32, (rows, 128), 1) // piece

    def gather_pieces(parts):
        out = parts[0]
        for n in range(1, per_tile):
            out = jnp.where(lane_part == n, parts[n], out)
        return out

    def rolled(x, amount):
        amount = amount * piece % 128
        return pltpu.roll(x, amount, 1) if amount else x

    lat_row = lat_ref[...].reshape(1, -1)
    lat_now = (lat_row.astype(jnp.float32) + 0.5) / NLAT - 0.5
    lat_now = jnp.broadcast_to(sine((0.5 - jnp.abs(lat_now)) * math.pi), (rows, NLAT))
    weight_tiles = []
    for j in range(splits):
        tile = jnp.zeros((rows, 128), jnp.float32)
        for b in range(bands):
            t, n = (b * splits + j) // per_tile, (b * splits + j) % per_tile
            source = lat_now[:, t * 128 : (t + 1) * 128]
            part = gather_pieces([rolled(source, il - n) for il in range(per_tile)])
            tile = jnp.where(band_id == b, part, tile)
        weight_tiles += [tile] * halves
    row_weight = jnp.concatenate(weight_tiles, axis=1)[0:1]
    pairs = pair_ref[...].reshape(1, -1).astype(jnp.float32)
    pair_count = pairs.shape[1]
    pair_dev = chunks * GROUP

    block_rows = bands * rows

    def fourier(n, _):
        ch = n // levs
        z = level_order(lax.rem(n, levs))
        col = lax.broadcasted_iota(jnp.int32, (block_rows, 1), 0)
        place = ((col >> 4) * levs + z) * pair_dev + ch * GROUP + ((col & 15) >> 2)
        spot = lax.broadcasted_iota(jnp.int32, (block_rows, pair_count), 1) == place
        wave = jnp.sum(jnp.where(spot, pairs, 0.0), axis=1, keepdims=True)
        wave = jnp.where((col & 2) == 0, wave, NT - wave)
        wave = jnp.broadcast_to(wave, (block_rows, 128))
        quarter = ((col & 1) * (NLON // 4)).astype(jnp.float32)
        lanes = lax.broadcasted_iota(jnp.int32, (1, 128), 1).astype(jnp.float32)
        at = pl.multiple_of(z * block_rows, block_rows)
        spot_rows = pl.ds(pl.multiple_of(ch * cols + at, block_rows), block_rows)
        for kc in range(NLON // 128):
            table[spot_rows, kc * 128 : (kc + 1) * 128] = table_values(
                wave * (lanes + kc * 128.0) + quarter
            )

        @pl.when(n == 0)
        def _():
            pltpu.make_async_copy(points_in, points_in, load_sem).wait()

        got = lax.dot_general(
            table[spot_rows, :], points_in[...], LAST, preferred_element_type=jnp.float32
        )
        send[ch, pl.ds(at, block_rows), :] = (got * row_weight).astype(jnp.bfloat16)

        @pl.when(n == 0)
        def _():
            pl.semaphore_wait(barrier, devs - 1)

        send_level(ch, z)
        return 0

    lax.fori_loop(0, chunks * levs, fourier, 0)

    lane_at = lax.broadcasted_iota(jnp.int32, (piece, 128), 1)
    row_at = lax.broadcasted_iota(jnp.int32, (piece, 128), 0)
    for j in range(splits):
        lane_weight = row_weight[:, j * lev_dev * piece : j * lev_dev * piece + 128]
        weight_rows[j] = jnp.broadcast_to(
            jnp.sum(jnp.where(lane_at == row_at, lane_weight, 0.0), axis=1, keepdims=True),
            (piece, 128),
        )
    pick[...] = (
        (lax.broadcasted_iota(jnp.int32, (NLAT, NLAT), 0) == lat_row)
        .astype(jnp.float32)
        .astype(jnp.bfloat16)
    )
    means[...] = jnp.zeros_like(means)
    square = [lax.broadcasted_iota(jnp.int32, (LEV, LEV), n) for n in range(2)]
    for n in range(STEPS):
        mix_ref[n] = jnp.where(square[0] == square[1], 0.7, 0.0) + 0.4 * coupling_ref[n]

    def chunk_body(ch, _):
        def prepare(s, _):
            slot = ch * GROUP + s
            leg_copy(slot).wait()
            stored[s] = flat_dot(leg_buf[lax.rem(slot, 2)], pick[...]).astype(jnp.bfloat16)
            spot = lax.broadcasted_iota(jnp.int32, (1, pair_count), 1) == me * pair_dev + slot
            low_wave = jnp.sum(jnp.where(spot, pairs, 0.0), axis=1, keepdims=True)
            column = lax.broadcasted_iota(jnp.int32, (1, NT + 2), 1).astype(jnp.float32)
            second = column >= NT + 1 - low_wave
            degree = jnp.where(second, column - 1.0, low_wave + column)
            ratio = degree / NT
            ratio = ratio * ratio
            shape_term = degree * (degree + 1.0) / (NT * (NT + 1.0))
            consts_ref[s, 0:1, :] = second.astype(jnp.float32)
            consts_ref[s, 1:2, :] = 1.0 / (1.0 + ratio * ratio)
            for n in range(STEPS):
                consts_ref[s, 2 + n : 3 + n, :] = 1.0 / (1.0 + damp_ref[n] * shape_term)
            consts_ref[s, 6:7, :] = jnp.broadcast_to(
                (low_wave == 0.0).astype(jnp.float32), (1, NT + 2)
            )

            @pl.when(slot + 2 < slots)
            def _():
                leg_copy(slot + 2).start()

            return 0

        lax.fori_loop(0, GROUP, prepare, 0)
        wait_recv(ch)

        def arrive(z, _):
            for half in range(halves):
                for t in range(NLAT // 128):
                    tiles = []
                    for n in range(per_tile):
                        g = t * per_tile + n
                        b, j = g // splits, g % splits
                        lane0 = (j * halves + half) * 128
                        tiles.append(
                            recv[
                                ch,
                                pl.ds(pl.multiple_of((z * bands + b) * rows, rows), rows),
                                lane0 : lane0 + 128,
                            ].astype(jnp.float32)
                        )
                    for il in range(per_tile):
                        level = z * lev_dev + half * per_tile + il
                        turn[t, pl.ds(pl.multiple_of(level * rows, rows), rows), :] = gather_pieces([rolled(tiles[n], n - il) for n in range(per_tile)])
            return 0

        lax.fori_loop(0, levs, arrive, 0)

        def direct(s, _):
            slot = ch * GROUP + s
            back_copy(slot).wait()
            waves_in = jnp.concatenate(
                [
                    jnp.concatenate(
                        [
                            turn[t, pl.ds(s * 4 + qr, LEV, stride=rows), :]
                            for t in range(NLAT // 128)
                        ],
                        axis=1,
                    )
                    for qr in range(4)
                ],
                axis=0,
            ).astype(jnp.bfloat16)
            coeffs = lax.dot_general(
                waves_in, stored[s], LAST, preferred_element_type=jnp.float32
            ) * math.sqrt(2.0 / NLAT)
            second = consts_ref[s, 0:1, :] > 0.5
            incr[s] = (
                jnp.where(second, coeffs[2 * LEV :], coeffs[: 2 * LEV]) * consts_ref[s, 1:2, :]
            )
            spec[s] = back_buf[lax.rem(slot, 2)]

            @pl.when(slot + 2 < slots)
            def _():
                back_copy(slot + 2).start()

            return 0

        lax.fori_loop(0, GROUP, direct, 0)

        def step(k, _):
            def inverse(s, _):
                second = consts_ref[s, 0:1, :] > 0.5
                inv = consts_ref[s, pl.ds(2 + k, 1), :]
                mix = mix_ref[k]
                weight = numer_ref[k].astype(jnp.float32) / DEN
                now = [
                    jnp.dot(
                        mix,
                        spec[s, r * LEV : (r + 1) * LEV, :],
                        precision=lax.Precision.HIGHEST,
                        preferred_element_type=jnp.float32,
                    )
                    * inv
                    + weight * incr[s, r * LEV : (r + 1) * LEV, :]
                    for r in range(2)
                ]
                for r in range(2):
                    spec[s, r * LEV : (r + 1) * LEV, :] = now[r]
                means[k] += now[0][:, :128] * consts_ref[s, 6:7, :128]
                both = jnp.concatenate(now, axis=0)
                split = jnp.concatenate(
                    [jnp.where(second, 0.0, both), jnp.where(second, both, 0.0)], axis=0
                ).astype(jnp.bfloat16)
                waves = flat_dot(split, stored[s]) * math.sqrt(2.0 / NT)
                for qr in range(4):
                    for t in range(NLAT // 128):
                        turn[t, pl.ds(s * 4 + qr, LEV, stride=rows), :] = waves[
                            qr * LEV : (qr + 1) * LEV, t * 128 : (t + 1) * 128
                        ]
                return 0

            lax.fori_loop(0, GROUP, inverse, 0)
            t_out = chunks + ch * STEPS + k

            def depart(zi, _):
                z = level_order(zi)
                for half in range(halves):
                    for t in range(NLAT // 128):
                        tiles = []
                        for il in range(per_tile):
                            level = z * lev_dev + half * per_tile + il
                            tiles.append(
                                turn[t, pl.ds(pl.multiple_of(level * rows, rows), rows), :]
                            )
                        for n in range(per_tile):
                            g = t * per_tile + n
                            b, j = g // splits, g % splits
                            lane0 = (j * halves + half) * 128
                            send[
                                t_out,
                                pl.ds(pl.multiple_of((z * bands + b) * rows, rows), rows),
                                lane0 : lane0 + 128,
                            ] = gather_pieces(
                                [rolled(tiles[il], il - n) for il in range(per_tile)]
                            ).astype(jnp.bfloat16)
                send_level(t_out, z)
                return 0

            lax.fori_loop(0, levs, depart, 0)
            return 0

        lax.fori_loop(0, STEPS, step, 0)
        return 0

    lax.fori_loop(0, chunks, chunk_body, 0)

    tall = lev_dev * piece
    lane = lax.broadcasted_iota(jnp.int32, (lev_dev, 128), 1)
    level_at = lax.broadcasted_iota(jnp.int32, (lev_dev, 128), 0)
    half_row = 64
    low = -1e30

    def grid_block(k, j, lo, hi):
        at = j * tall if isinstance(j, int) else pl.multiple_of(j * tall, tall)
        total = None
        for ch in range(lo, hi):
            one = flat_dot(
                recv[chunks + ch * STEPS + k, :, pl.ds(at, tall)].T,
                table[ch * cols : (ch + 1) * cols, :],
            )
            total = one if total is None else total + one
        return total

    def folded(tile, op):
        out = tile[:, :128]
        for n in range(1, NLON // 128):
            out = op(out, tile[:, n * 128 : (n + 1) * 128])
        return out

    def mass_block(tile, weights, carry):
        top, total = carry
        levels = [tile[n * piece : (n + 1) * piece] for n in range(lev_dev)]
        block_top = jnp.concatenate(
            [jnp.max(folded(x, jnp.maximum), axis=0, keepdims=True) for x in levels], axis=0
        )
        block_top = jnp.max(block_top, axis=1, keepdims=True)
        new_top = jnp.maximum(top, jnp.broadcast_to(block_top, top.shape))
        sums = []
        for n in range(lev_dev):
            x = jnp.exp(levels[n] - new_top[n : n + 1, 0:1])
            sums.append(jnp.sum(folded(x, jnp.add) * weights, axis=0, keepdims=True))
        block_sum = jnp.sum(jnp.concatenate(sums, axis=0), axis=1, keepdims=True)
        return new_top, total * jnp.exp(top - new_top) + block_sum

    empty = (
        jnp.full((lev_dev, 128), low, jnp.float32),
        jnp.zeros((lev_dev, 128), jnp.float32),
    )

    def packed_row(carry, base):
        top, total = carry
        return jnp.sum(
            jnp.where(lane == level_at + base, top, 0.0)
            + jnp.where(lane == level_at + base + half_row, total, 0.0),
            axis=0,
            keepdims=True,
        )

    last = STEPS - 1
    for ch in range(chunks - 1):
        wait_recv(chunks + ch * STEPS + last)
    if chunks > 1:

        def part(j, _):
            acc[pl.ds(pl.multiple_of(j * tall, tall), tall), :] = grid_block(
                last, j, 0, chunks - 1
            )
            return 0

        lax.fori_loop(0, splits, part, 0)

    def early(k, row):
        def take(ch, _):
            wait_recv(chunks + ch * STEPS + k)
            return 0

        lax.fori_loop(0, chunks, take, 0)

        def part(j, carry):
            return mass_block(grid_block(k, j, 0, chunks), weight_rows[j], carry)

        return row + packed_row(lax.fori_loop(0, splits, part, empty), k * lev_dev)

    zero_row = jnp.zeros((1, 128), jnp.float32)
    early_send[0:1, :] = lax.fori_loop(0, last, early, zero_row)
    wide_lane = lax.broadcasted_iota(jnp.int32, (LEV, 128), 1)
    diag = lax.broadcasted_iota(jnp.int32, (LEV, 128), 0)
    means_row = zero_row
    for n in range(STEPS):
        column = jnp.sum(jnp.where(wide_lane == 0, means[n], 0.0), axis=1, keepdims=True)
        means_row = means_row + jnp.sum(
            jnp.where(wide_lane == diag + LEV * n, column, 0.0), axis=0, keepdims=True
        )
    early_send[1:2, :] = means_row
    place_here = lev_id * bands + band_id

    def share(source, target, sems):
        def one(o, _):
            db, dz = peer(o)
            pltpu.make_async_remote_copy(
                src_ref=source,
                dst_ref=target.at[place_here],
                send_sem=sems.at[0],
                recv_sem=sems.at[1],
                device_id=(db, dz),
                device_id_type=MESH,
            ).start()
            return 0

        lax.fori_loop(1, devs, one, 0)
        pltpu.make_async_copy(source, target.at[place_here], sems.at[1]).start()

    def shared(target, sems):
        pltpu.make_async_copy(target, target, sems.at[1]).wait()

    def sent(target, sems):
        rest = target.at[pl.ds(0, devs - 1)]
        pltpu.make_async_copy(rest, rest, sems.at[0]).wait()

    share(early_send, early_recv, early_sem)
    wait_recv(chunks + (chunks - 1) * STEPS + last)
    carry = empty
    for j in range(splits):
        tile = grid_block(last, j, chunks - 1, chunks)
        if chunks > 1:
            tile = tile + acc[j * tall : (j + 1) * tall, :]
        acc[j * tall : (j + 1) * tall, :] = tile
        carry = mass_block(tile, weight_rows[j], carry)
    late_send[0:1, :] = packed_row(carry, 0)
    share(late_send, late_recv, late_sem)

    row_lane = lax.broadcasted_iota(jnp.int32, (8, 128), 1)
    to_grid = math.sqrt(2.0 / NT) * float(np.float32(math.sqrt(2.0 / NLON)).astype(jnp.bfloat16))
    lat_sum = sum(math.cos(math.pi * ((n + 0.5) / NLAT - 0.5)) for n in range(NLAT))
    normaliser = sum(1.0 + 2.0 * n / (LEV - 1) for n in range(LEV)) * lat_sum * NLON
    fix_scale = math.sqrt(NT * NLON) / 2.0

    def gathered(target):
        out = []
        for z in range(levs):
            top = target[z * bands, 0:1, :]
            for b in range(1, bands):
                top = jnp.maximum(top, target[z * bands + b, 0:1, :])
            total = zero_row
            for b in range(bands):
                here = target[z * bands + b, 0:1, :]
                total = total + jnp.exp(here - top) * pltpu.roll(
                    jnp.broadcast_to(here, (8, 128)), 128 - half_row, 1
                )[0:1]
            out.append((jnp.broadcast_to(top, (8, 128)), jnp.broadcast_to(total, (8, 128))))
        return out

    def fix_of(parts, base, shift):
        valid = jnp.logical_and(row_lane >= base, row_lane < base + lev_dev)
        total = jnp.zeros((8, 128), jnp.float32)
        for z in range(levs):
            turn_by = (base - z * lev_dev) % 128
            moved = pltpu.roll(shift, turn_by, 1) if turn_by else shift
            level = (row_lane - base + z * lev_dev).astype(jnp.float32)
            top, amount = parts[z]
            total = total + jnp.where(
                valid,
                jnp.exp(jnp.where(valid, top + moved, 0.0))
                * amount
                * (1.0 + 2.0 * level / (LEV - 1)),
                0.0,
            )
        total = jnp.sum(total, axis=1, keepdims=True)
        return jnp.log(target_ref[0] / (total / normaliser))

    shared(early_recv, early_sem)
    parts = gathered(early_recv)
    base_row = zero_row
    for d in range(devs):
        base_row = base_row + early_recv[d, 1:2, :]
    base_row = jnp.broadcast_to(base_row, (8, 128))
    is_level = row_lane < LEV
    carried = jnp.zeros((8, 128), jnp.float32)
    for n in range(STEPS):
        back = (128 - LEV * n) % 128
        base_n = pltpu.roll(base_row, back, 1) if back else base_row
        column = jnp.sum(mix_ref[n] * carried[0:1, :LEV], axis=1, keepdims=True)
        moved_by = jnp.broadcast_to(
            jnp.sum(jnp.where(wide_lane == diag, column, 0.0), axis=0, keepdims=True), (8, 128)
        )
        moved = (base_n + moved_by).astype(jnp.bfloat16).astype(jnp.float32) - base_n.astype(
            jnp.bfloat16
        ).astype(jnp.float32)
        shift = jnp.where(is_level, moved * to_grid, 0.0)
        if n < last:
            fix = fix_of(parts, n * lev_dev, shift)
            fix_ref[n] = fix[0, 0]
            carried = jnp.where(is_level, moved_by + fix * fix_scale, 0.0)

    own_lane = lev_id * lev_dev + level_at
    own = jnp.sum(jnp.where(lane == own_lane, shift[0:1], 0.0), axis=1, keepdims=True)
    for j in range(splits):
        for n in range(lev_dev):
            here = (j * lev_dev + n) * piece
            points_in[here : here + piece, :] = (
                acc[here : here + piece, :] + own[n : n + 1, 0:1]
            ).astype(jnp.bfloat16)
            pltpu.make_async_copy(
                points_in.at[pl.ds(here, piece), :],
                out_ref.at[n, pl.ds(j * piece, piece), :],
                out_sem,
            ).start()

    shared(late_recv, late_sem)
    fix_ref[last] = fix_of(gathered(late_recv), 0, shift)[0, 0]

    def finish(t, _):
        left = send.at[t, pl.ds(0, (devs - 1) * rows), :]
        pltpu.make_async_copy(left, left, send_sem.at[t]).wait()
        return 0

    lax.fori_loop(0, chunks * (1 + STEPS), finish, 0)
    sent(early_recv, early_sem)
    sent(late_recv, late_sem)
    pltpu.make_async_copy(points_in, points_in, out_sem).wait()


def body(
    increment, background, legendre, coupling, damping, target_mass, numerators, pair_low, lat_map
):
    band_count = lax.axis_size("band")
    lev_count = lax.axis_size("lev")
    devs = band_count * lev_count
    lev_dev, lat_dev = increment.shape[:2]
    pair_dev = legendre.shape[0]
    points = lev_dev * lat_dev
    cols = devs * 4 * GROUP
    fits = (
        lat_dev % 32 == 0
        and pair_dev % GROUP == 0
        and lev_dev == 8
        and band_count * 4 * GROUP == 128
        and lev_count * lev_dev == LEV
        and STEPS * lev_dev <= 64
        and points % 256 == 0
        and LEV * STEPS == 128
    )
    if not fits:
        return body_general(
            increment,
            background,
            legendre,
            coupling,
            damping,
            target_mass,
            numerators,
            pair_low,
            lat_map,
        )
    chunks = pair_dev // GROUP
    vmem = pl.BlockSpec(memory_space=pltpu.VMEM)
    smem = pl.BlockSpec(memory_space=pltpu.SMEM)
    hbm = pl.BlockSpec(memory_space=pl.ANY)
    total = chunks * (1 + STEPS)
    dma = pltpu.SemaphoreType.DMA
    return pl.pallas_call(
        lambda *refs: exchange_kernel(
            (band_count, lev_count, lev_dev, lat_dev, chunks), *refs
        ),
        out_shape=(
            jax.ShapeDtypeStruct((lev_dev, lat_dev, NLON), jnp.bfloat16),
            jax.ShapeDtypeStruct((STEPS,), jnp.float32),
        ),
        in_specs=[smem] * 3 + [hbm] * 3 + [vmem] * 3,
        out_specs=(hbm, smem),
        scratch_shapes=[
            pltpu.VMEM((GROUP, 8, NT + 2), jnp.float32),
            pltpu.VMEM((STEPS, LEV, LEV), jnp.float32),
            pltpu.VMEM((points, NLON), jnp.bfloat16),
            pltpu.VMEM((chunks * cols, NLON), jnp.bfloat16),
            pltpu.VMEM((NLAT, NLAT), jnp.bfloat16),
            pltpu.VMEM((2, NT + 2, NLAT), jnp.bfloat16),
            pltpu.VMEM((GROUP, NT + 2, NLAT), jnp.bfloat16),
            pltpu.VMEM((2, 2 * LEV, NT + 2), jnp.float32),
            pltpu.VMEM((GROUP, 2 * LEV, NT + 2), jnp.float32),
            pltpu.VMEM((GROUP, 2 * LEV, NT + 2), jnp.float32),
            pltpu.VMEM((NLAT // 128, LEV * 4 * GROUP, 128), jnp.float32),
            pltpu.VMEM((points, NLON), jnp.float32),
            pltpu.VMEM((total, cols, points), jnp.bfloat16),
            pltpu.VMEM((total, cols, points), jnp.bfloat16),
            pltpu.VMEM((STEPS, LEV, 128), jnp.float32),
            pltpu.VMEM((lat_dev // 32, 32, 128), jnp.float32),
            pltpu.VMEM((2, 128), jnp.float32),
            pltpu.VMEM((devs, 2, 128), jnp.float32),
            pltpu.VMEM((1, 128), jnp.float32),
            pltpu.VMEM((devs, 1, 128), jnp.float32),
            dma,
            dma((2,)),
            dma((2,)),
            dma((total,)),
            dma((total,)),
            dma((2,)),
            dma((2,)),
            dma,
        ],
        compiler_params=pltpu.CompilerParams(
            collective_id=0, has_side_effects=True, vmem_limit_bytes=67043328
        ),
    )(
        numerators,
        damping,
        target_mass,
        increment,
        legendre.transpose(0, 2, 1),
        background.reshape(pair_dev, 2 * LEV, NT + 2),
        pair_low,
        lat_map,
        coupling,
    )


def solution(mesh):
    return jax.shard_map(
        body,
        mesh=mesh,
        in_specs=(
            P("lev", "band", None),
            P(("band", "lev"), None, None, None),
            P(("band", "lev"), None, None),
            P(),
            P(),
            P(),
            P(),
            P(),
            P(),
        ),
        out_specs=(P("lev", "band", None), P()),
        check_vma=False,
    )
```

```python
import math

import jax
import numpy as np
import jax.numpy as jnp
from jax import lax
from jax.experimental import pallas as pl
from jax.experimental.pallas import tpu as pltpu
from jax.sharding import PartitionSpec as P

NT = 767
NLAT = 768
NLON = 1536
LEV = 32
STEPS = 4
DEN = 64
NPAIR = 384
AXES = ("band", "lev")


def wave_table(pair_low):
    column = jnp.arange(4 * pair_low.shape[0], dtype=jnp.int32)
    low = jnp.repeat(pair_low, 4)
    wavenumber = jnp.where(column // 2 % 2 == 0, low, NT - low)[:, None]
    quarter = (column % 2 * (NLON // 4))[:, None]
    fine = math.gcd(128, NLON)
    unit = 2.0 * math.pi / NLON
    coarse_pts = jnp.arange(NLON // fine, dtype=jnp.int32)[None, :] * fine
    coarse = ((wavenumber * coarse_pts + quarter) % NLON).astype(jnp.float32) * unit
    rest = (wavenumber * jnp.arange(fine, dtype=jnp.int32)[None, :] % NLON).astype(
        jnp.float32
    ) * unit
    norm = math.sqrt(2.0 / NLON)
    cos_a, sin_a, cos_b, sin_b = lax.optimization_barrier(
        (jnp.cos(coarse) * norm, jnp.sin(coarse) * norm, jnp.cos(rest), jnp.sin(rest))
    )
    blocks = [
        cos_a[:, i : i + 1] * cos_b - sin_a[:, i : i + 1] * sin_b for i in range(NLON // fine)
    ]
    return jnp.concatenate(blocks, axis=1).astype(jnp.bfloat16)


def lat_weights(lat_rows):
    return jnp.cos(math.pi * ((lat_rows.astype(jnp.float32) + 0.5) / NLAT - 0.5))


def degrees(low_wave):
    columns = jnp.arange(NT + 2, dtype=jnp.int32)
    in_second = columns[None, :] >= NT + 1 - low_wave[:, None]
    degree = jnp.where(in_second, columns[None, :] - 1, low_wave[:, None] + columns[None, :])
    return (degree.astype(jnp.float32), in_second)


def body_general(
    increment, background, legendre, coupling, damping, target_mass, numerators, pair_low, lat_map
):
    band_count = lax.axis_size("band")
    lev_count = lax.axis_size("lev")
    device_count = band_count * lev_count
    band_id = lax.axis_index("band")
    lev_id = lax.axis_index("lev")
    lev_dev = increment.shape[0]
    lat_dev = increment.shape[1]
    pair_dev = legendre.shape[0]
    points = lev_dev * lat_dev
    fourier_tab = wave_table(pair_low)
    local_lats = lax.dynamic_slice_in_dim(lat_map, band_id * lat_dev, lat_dev)
    row_weight = lat_weights(local_lats)
    all_levels = 1.0 + 2.0 * jnp.arange(LEV, dtype=jnp.float32) / (LEV - 1)
    normaliser = (
        jnp.sum(all_levels) * jnp.sum(lat_weights(jnp.arange(NLAT, dtype=jnp.int32))) * NLON
    )
    fix_scale = math.sqrt(NT * NLON) / 2.0
    own_pairs = lax.dynamic_slice_in_dim(
        pair_low, (band_id * lev_count + lev_id) * pair_dev, pair_dev
    )
    degree, in_second = degrees(own_pairs)
    holder = (own_pairs == 0).astype(jnp.float32)

    fourier = jnp.einsum(
        "ck,xk->cx",
        fourier_tab,
        increment.reshape(points, NLON),
        preferred_element_type=jnp.float32,
    )
    fourier = (fourier * jnp.tile(row_weight, lev_dev)[None, :]).astype(jnp.bfloat16)
    received = lax.all_to_all(
        fourier.reshape(device_count, pair_dev * 4, points), AXES, split_axis=0, concat_axis=0
    )

    pick = (lat_map[:, None] == jnp.arange(NLAT, dtype=jnp.int32)[None, :]).astype(jnp.bfloat16)
    stored = jnp.einsum(
        "jn,pnc->pjc", pick, legendre, preferred_element_type=jnp.float32
    ).astype(jnp.bfloat16)

    received = received.reshape(band_count, lev_count, pair_dev * 4, lev_dev, lat_dev)
    waves_in = received.transpose(2, 1, 3, 0, 4).reshape(pair_dev, 4 * LEV, NLAT)
    coeffs = jnp.einsum("prj,pjc->prc", waves_in, stored, preferred_element_type=jnp.float32)
    coeffs = coeffs.reshape(pair_dev, 2, 2, LEV, NT + 2) * math.sqrt(2.0 / NLAT)
    second_cols = in_second[:, None, None, :]
    smoothing = 1.0 / (1.0 + (degree / NT) ** 4)
    incr_spec = jnp.where(second_cols, coeffs[:, 1], coeffs[:, 0]) * smoothing[:, None, None, :]
    shape_term = degree * (degree + 1.0) / (NT * (NT + 1.0))

    spectral = background
    means = []
    arrived = []
    for step_idx in range(STEPS):
        coupled = 0.7 * spectral + 0.4 * jnp.einsum(
            "lm,prmc->prlc", coupling[step_idx], spectral, precision=lax.Precision.HIGHEST
        )
        weight_now = numerators[step_idx].astype(jnp.float32) / DEN
        spectral = (
            coupled / (1.0 + damping[step_idx] * shape_term)[:, None, None, :]
            + weight_now * incr_spec
        )
        means.append(jnp.sum(spectral[:, 0, :, 0] * holder[:, None], axis=0))
        spec_bf = spectral.astype(jnp.bfloat16)
        zeros_bf = jnp.zeros_like(spec_bf)
        split_rows = jnp.stack(
            [jnp.where(second_cols, zeros_bf, spec_bf), jnp.where(second_cols, spec_bf, zeros_bf)],
            axis=1,
        )
        waves_f = jnp.einsum(
            "prc,pjc->prj",
            split_rows.reshape(pair_dev, 4 * LEV, NT + 2),
            stored,
            preferred_element_type=jnp.float32,
        )
        waves_bf = (waves_f * math.sqrt(2.0 / NT)).astype(jnp.bfloat16)
        outgoing = waves_bf.reshape(pair_dev * 4, lev_count, lev_dev, band_count, lat_dev)
        outgoing = outgoing.transpose(3, 1, 0, 2, 4).reshape(device_count, pair_dev * 4, points)
        spectral, outgoing = lax.optimization_barrier((spectral, outgoing))
        arrived.append(lax.all_to_all(outgoing, AXES, split_axis=0, concat_axis=0))

    tops, sums = [], []
    for step_idx in range(STEPS):
        grid_now = jnp.einsum(
            "cx,ck->xk",
            arrived[step_idx].reshape(NPAIR * 4, points),
            fourier_tab,
            preferred_element_type=jnp.float32,
        ).reshape(lev_dev, lat_dev, NLON)
        top = jnp.max(grid_now, axis=(1, 2))
        tops.append(top)
        sums.append(
            jnp.sum(
                jnp.sum(jnp.exp(grid_now - top[:, None, None]), axis=2) * row_weight[None, :],
                axis=1,
            )
        )

    packed = jnp.concatenate(
        [jnp.stack(tops).reshape(-1), jnp.stack(sums).reshape(-1), jnp.stack(means).reshape(-1)]
    )
    gathered = lax.all_to_all(
        jnp.broadcast_to(packed[None, :], (device_count, packed.shape[0])),
        AXES,
        split_axis=0,
        concat_axis=0,
    )
    count = STEPS * lev_dev
    all_tops = gathered[:, :count].reshape(band_count, lev_count, STEPS, lev_dev)
    all_sums = gathered[:, count : 2 * count].reshape(band_count, lev_count, STEPS, lev_dev)
    all_tops = all_tops.transpose(2, 0, 1, 3).reshape(STEPS, band_count, LEV)
    all_sums = all_sums.transpose(2, 0, 1, 3).reshape(STEPS, band_count, LEV)
    all_means = jnp.sum(gathered[:, 2 * count :], axis=0).reshape(STEPS, LEV)

    table_entry = jnp.full((), math.sqrt(2.0 / NLON), jnp.bfloat16).astype(jnp.float32)
    to_grid = math.sqrt(2.0 / NT) * table_entry
    carried = jnp.zeros((LEV,), jnp.float32)
    shift = jnp.zeros((LEV,), jnp.float32)
    fix_list = []
    for step_idx in range(STEPS):
        carried = 0.7 * carried + 0.4 * jnp.sum(coupling[step_idx] * carried[None, :], axis=1)
        base = all_means[step_idx]
        moved = (base + carried).astype(jnp.bfloat16).astype(jnp.float32) - base.astype(
            jnp.bfloat16
        ).astype(jnp.float32)
        shift = moved * to_grid
        total = jnp.sum(
            jnp.exp(all_tops[step_idx] + shift[None, :]) * all_sums[step_idx] * all_levels[None, :]
        )
        mass_fix = jnp.log(target_mass[0] / (total / normaliser))
        fix_list.append(mass_fix)
        carried = carried + mass_fix * fix_scale
    own_shift = lax.dynamic_slice_in_dim(shift, lev_id * lev_dev, lev_dev)
    analysis = (grid_now + own_shift[:, None, None]).astype(jnp.bfloat16)
    return (analysis, jnp.stack(fix_list))


GROUP = 4
MESH = pl.DeviceIdType.MESH
LAST = (((1,), (1,)), ((), ()))


def sine(x):
    y = x * x
    out = -1.0 / math.factorial(11)
    for n in (9, 7, 5, 3, 1):
        out = out * y + (1.0 if n % 4 == 1 else -1.0) / math.factorial(n)
    return out * x


def table_values(phase):
    turns = jnp.floor((phase + 0.5) * (1.0 / NLON))
    rest = jnp.abs(phase - turns * NLON - NLON / 2) - NLON / 4
    return (sine(rest * (2.0 * math.pi / NLON)) * math.sqrt(2.0 / NLON)).astype(jnp.bfloat16)


def flat_dot(a, b):
    return jnp.dot(a, b, preferred_element_type=jnp.float32)


def exchange_kernel(
    sizes,
    numer_ref,
    damp_ref,
    target_ref,
    inc_ref,
    leg_ref,
    back_ref,
    pair_ref,
    lat_ref,
    coupling_ref,
    out_ref,
    fix_ref,
    consts_ref,
    mix_ref,
    points_in,
    table,
    pick,
    leg_buf,
    stored,
    back_buf,
    incr,
    spec,
    turn,
    acc,
    send,
    recv,
    means,
    weight_rows,
    early_send,
    early_recv,
    late_send,
    late_recv,
    load_sem,
    leg_sem,
    back_sem,
    send_sem,
    recv_sem,
    piece_sem,
    early_sem,
    late_sem,
):
    bands, levs, lev_dev, lat_dev, chunks = sizes
    devs = bands * levs
    band_id = lax.axis_index("band")
    lev_id = lax.axis_index("lev")
    me = band_id * levs + lev_id
    piece = 32
    splits = lat_dev // piece
    rows = 4 * GROUP
    cols = devs * rows
    points = lev_dev * lat_dev
    slots = chunks * GROUP
    per_tile = 128 // piece
    halves = lev_dev // per_tile

    barrier = pltpu.get_barrier_semaphore()

    def peer(o):
        return (
            lax.rem(band_id + lax.rem(o, bands), bands),
            lax.rem(lev_id + o // bands, levs),
        )

    def greet(o, _):
        pl.semaphore_signal(barrier, inc=1, device_id=peer(o), device_id_type=MESH)
        return 0

    lax.fori_loop(1, devs, greet, 0)

    def load_piece(i, j):
        return pltpu.make_async_copy(
            inc_ref.at[i, pl.ds(j * piece, piece), :],
            points_in.at[pl.ds((j * lev_dev + i) * piece, piece), :],
            load_sem,
        )

    for j in range(splits):
        for i in range(lev_dev):
            load_piece(i, j).start()

    def leg_copy(slot):
        return pltpu.make_async_copy(
            leg_ref.at[slot], leg_buf.at[lax.rem(slot, 2)], leg_sem.at[lax.rem(slot, 2)]
        )

    def back_copy(slot):
        return pltpu.make_async_copy(
            back_ref.at[slot], back_buf.at[lax.rem(slot, 2)], back_sem.at[lax.rem(slot, 2)]
        )

    for slot in range(2):
        leg_copy(slot).start()
        back_copy(slot).start()

    home = pl.ds((lev_id * bands + band_id) * rows, rows)

    def send_level(t, z):
        def one(o, _):
            band = lax.rem(band_id + o, bands)
            block = send.at[t, pl.ds((z * bands + band) * rows, rows), :]
            own = jnp.logical_and(o == 0, z == lev_id)

            @pl.when(own)
            def _():
                pltpu.make_async_copy(block, recv.at[t, home, :], recv_sem.at[t]).start()

            @pl.when(jnp.logical_not(own))
            def _():
                pltpu.make_async_remote_copy(
                    src_ref=block,
                    dst_ref=recv.at[t, home, :],
                    send_sem=send_sem.at[t],
                    recv_sem=recv_sem.at[t],
                    device_id=(band, z),
                    device_id_type=MESH,
                ).start()

            return 0

        lax.fori_loop(0, bands, one, 0)

    final = chunks * (1 + STEPS) - 1
    tall = lev_dev * piece

    def send_pieces():
        def one(n, _):
            j = n // devs
            o = lax.rem(n, bands)
            z = level_order(lax.rem(n // bands, levs))
            band = lax.rem(band_id + o, bands)
            lanes = pl.ds(pl.multiple_of(j * tall, tall), tall)
            block = send.at[final, pl.ds((z * bands + band) * rows, rows), lanes]
            own = jnp.logical_and(o == 0, z == lev_id)

            @pl.when(own)
            def _():
                pltpu.make_async_copy(
                    block, recv.at[final, home, lanes], piece_sem.at[j]
                ).start()

            @pl.when(jnp.logical_not(own))
            def _():
                pltpu.make_async_remote_copy(
                    src_ref=block,
                    dst_ref=recv.at[final, home, lanes],
                    send_sem=send_sem.at[final],
                    recv_sem=piece_sem.at[j],
                    device_id=(band, z),
                    device_id_type=MESH,
                ).start()

            return 0

        lax.fori_loop(0, splits * devs, one, 0)

    def level_order(n):
        return lax.rem(lev_id + levs // 2 + n, levs)

    def wait_recv(t):
        pltpu.make_async_copy(recv.at[t], recv.at[t], recv_sem.at[t]).wait()

    lane_part = lax.broadcasted_iota(jnp.int32, (rows, 128), 1) // piece

    def gather_pieces(parts):
        out = parts[0]
        for n in range(1, per_tile):
            out = jnp.where(lane_part == n, parts[n], out)
        return out

    def rolled(x, amount):
        amount = amount * piece % 128
        return pltpu.roll(x, amount, 1) if amount else x

    lat_row = lat_ref[...].reshape(1, -1)
    lat_now = (lat_row.astype(jnp.float32) + 0.5) / NLAT - 0.5
    lat_now = jnp.broadcast_to(sine((0.5 - jnp.abs(lat_now)) * math.pi), (rows, NLAT))
    weight_tiles = []
    for j in range(splits):
        tile = jnp.zeros((rows, 128), jnp.float32)
        for b in range(bands):
            t, n = (b * splits + j) // per_tile, (b * splits + j) % per_tile
            source = lat_now[:, t * 128 : (t + 1) * 128]
            part = gather_pieces([rolled(source, il - n) for il in range(per_tile)])
            tile = jnp.where(band_id == b, part, tile)
        weight_tiles += [tile] * halves
    row_weight = jnp.concatenate(weight_tiles, axis=1)[0:1]
    pairs = pair_ref[...].reshape(1, -1).astype(jnp.float32)
    pair_count = pairs.shape[1]
    pair_dev = chunks * GROUP

    block_rows = bands * rows

    def fourier(n, _):
        ch = n // levs
        z = level_order(lax.rem(n, levs))
        col = lax.broadcasted_iota(jnp.int32, (block_rows, 1), 0)
        place = ((col >> 4) * levs + z) * pair_dev + ch * GROUP + ((col & 15) >> 2)
        spot = lax.broadcasted_iota(jnp.int32, (block_rows, pair_count), 1) == place
        wave = jnp.sum(jnp.where(spot, pairs, 0.0), axis=1, keepdims=True)
        wave = jnp.where((col & 2) == 0, wave, NT - wave)
        wave = jnp.broadcast_to(wave, (block_rows, 128))
        quarter = ((col & 1) * (NLON // 4)).astype(jnp.float32)
        lanes = lax.broadcasted_iota(jnp.int32, (1, 128), 1).astype(jnp.float32)
        at = pl.multiple_of(z * block_rows, block_rows)
        spot_rows = pl.ds(pl.multiple_of(ch * cols + at, block_rows), block_rows)
        for kc in range(NLON // 128):
            table[spot_rows, kc * 128 : (kc + 1) * 128] = table_values(
                wave * (lanes + kc * 128.0) + quarter
            )

        @pl.when(n == 0)
        def _():
            pltpu.make_async_copy(points_in, points_in, load_sem).wait()

        got = lax.dot_general(
            table[spot_rows, :], points_in[...], LAST, preferred_element_type=jnp.float32
        )
        send[ch, pl.ds(at, block_rows), :] = (got * row_weight).astype(jnp.bfloat16)

        @pl.when(n == 0)
        def _():
            pl.semaphore_wait(barrier, devs - 1)

        send_level(ch, z)
        return 0

    lax.fori_loop(0, chunks * levs, fourier, 0)

    lane_at = lax.broadcasted_iota(jnp.int32, (piece, 128), 1)
    row_at = lax.broadcasted_iota(jnp.int32, (piece, 128), 0)
    for j in range(splits):
        lane_weight = row_weight[:, j * lev_dev * piece : j * lev_dev * piece + 128]
        weight_rows[j] = jnp.broadcast_to(
            jnp.sum(jnp.where(lane_at == row_at, lane_weight, 0.0), axis=1, keepdims=True),
            (piece, 128),
        )
    pick[...] = (
        (lax.broadcasted_iota(jnp.int32, (NLAT, NLAT), 0) == lat_row)
        .astype(jnp.float32)
        .astype(jnp.bfloat16)
    )
    means[...] = jnp.zeros_like(means)
    square = [lax.broadcasted_iota(jnp.int32, (LEV, LEV), n) for n in range(2)]
    for n in range(STEPS):
        mix_ref[n] = jnp.where(square[0] == square[1], 0.7, 0.0) + 0.4 * coupling_ref[n]

    def chunk_body(ch, _):
        def prepare(s, _):
            slot = ch * GROUP + s
            leg_copy(slot).wait()
            stored[s] = flat_dot(leg_buf[lax.rem(slot, 2)], pick[...]).astype(jnp.bfloat16)
            spot = lax.broadcasted_iota(jnp.int32, (1, pair_count), 1) == me * pair_dev + slot
            low_wave = jnp.sum(jnp.where(spot, pairs, 0.0), axis=1, keepdims=True)
            column = lax.broadcasted_iota(jnp.int32, (1, NT + 2), 1).astype(jnp.float32)
            second = column >= NT + 1 - low_wave
            degree = jnp.where(second, column - 1.0, low_wave + column)
            ratio = degree / NT
            ratio = ratio * ratio
            shape_term = degree * (degree + 1.0) / (NT * (NT + 1.0))
            consts_ref[s, 0:1, :] = second.astype(jnp.float32)
            consts_ref[s, 1:2, :] = 1.0 / (1.0 + ratio * ratio)
            for n in range(STEPS):
                consts_ref[s, 2 + n : 3 + n, :] = 1.0 / (1.0 + damp_ref[n] * shape_term)
            consts_ref[s, 6:7, :] = jnp.broadcast_to(
                (low_wave == 0.0).astype(jnp.float32), (1, NT + 2)
            )

            @pl.when(slot + 2 < slots)
            def _():
                leg_copy(slot + 2).start()

            return 0

        lax.fori_loop(0, GROUP, prepare, 0)
        wait_recv(ch)

        def arrive(z, _):
            for half in range(halves):
                for t in range(NLAT // 128):
                    tiles = []
                    for n in range(per_tile):
                        g = t * per_tile + n
                        b, j = g // splits, g % splits
                        lane0 = (j * halves + half) * 128
                        tiles.append(
                            recv[
                                ch,
                                pl.ds(pl.multiple_of((z * bands + b) * rows, rows), rows),
                                lane0 : lane0 + 128,
                            ].astype(jnp.float32)
                        )
                    for il in range(per_tile):
                        level = z * lev_dev + half * per_tile + il
                        turn[t, pl.ds(pl.multiple_of(level * rows, rows), rows), :] = gather_pieces([rolled(tiles[n], n - il) for n in range(per_tile)])
            return 0

        lax.fori_loop(0, levs, arrive, 0)

        def direct(s, _):
            slot = ch * GROUP + s
            back_copy(slot).wait()
            waves_in = jnp.concatenate(
                [
                    jnp.concatenate(
                        [
                            turn[t, pl.ds(s * 4 + qr, LEV, stride=rows), :]
                            for t in range(NLAT // 128)
                        ],
                        axis=1,
                    )
                    for qr in range(4)
                ],
                axis=0,
            ).astype(jnp.bfloat16)
            coeffs = lax.dot_general(
                waves_in, stored[s], LAST, preferred_element_type=jnp.float32
            ) * math.sqrt(2.0 / NLAT)
            second = consts_ref[s, 0:1, :] > 0.5
            incr[s] = (
                jnp.where(second, coeffs[2 * LEV :], coeffs[: 2 * LEV]) * consts_ref[s, 1:2, :]
            )
            spec[s] = back_buf[lax.rem(slot, 2)]

            @pl.when(slot + 2 < slots)
            def _():
                back_copy(slot + 2).start()

            return 0

        lax.fori_loop(0, GROUP, direct, 0)

        def step(k, _):
            def inverse(s, _):
                second = consts_ref[s, 0:1, :] > 0.5
                inv = consts_ref[s, pl.ds(2 + k, 1), :]
                mix = mix_ref[k]
                weight = numer_ref[k].astype(jnp.float32) / DEN
                now = [
                    jnp.dot(
                        mix,
                        spec[s, r * LEV : (r + 1) * LEV, :],
                        precision=lax.Precision.HIGHEST,
                        preferred_element_type=jnp.float32,
                    )
                    * inv
                    + weight * incr[s, r * LEV : (r + 1) * LEV, :]
                    for r in range(2)
                ]
                for r in range(2):
                    spec[s, r * LEV : (r + 1) * LEV, :] = now[r]
                means[k] += now[0][:, :128] * consts_ref[s, 6:7, :128]
                both = jnp.concatenate(now, axis=0)
                split = jnp.concatenate(
                    [jnp.where(second, 0.0, both), jnp.where(second, both, 0.0)], axis=0
                ).astype(jnp.bfloat16)
                waves = flat_dot(split, stored[s]) * math.sqrt(2.0 / NT)
                for qr in range(4):
                    for t in range(NLAT // 128):
                        turn[t, pl.ds(s * 4 + qr, LEV, stride=rows), :] = waves[
                            qr * LEV : (qr + 1) * LEV, t * 128 : (t + 1) * 128
                        ]
                return 0

            lax.fori_loop(0, GROUP, inverse, 0)
            t_out = chunks + ch * STEPS + k

            def depart(zi, _):
                z = level_order(zi)
                for half in range(halves):
                    for t in range(NLAT // 128):
                        tiles = []
                        for il in range(per_tile):
                            level = z * lev_dev + half * per_tile + il
                            tiles.append(
                                turn[t, pl.ds(pl.multiple_of(level * rows, rows), rows), :]
                            )
                        for n in range(per_tile):
                            g = t * per_tile + n
                            b, j = g // splits, g % splits
                            lane0 = (j * halves + half) * 128
                            send[
                                t_out,
                                pl.ds(pl.multiple_of((z * bands + b) * rows, rows), rows),
                                lane0 : lane0 + 128,
                            ] = gather_pieces(
                                [rolled(tiles[il], il - n) for il in range(per_tile)]
                            ).astype(jnp.bfloat16)

                @pl.when(t_out != final)
                def _():
                    send_level(t_out, z)

                return 0

            lax.fori_loop(0, levs, depart, 0)

            @pl.when(t_out == final)
            def _():
                send_pieces()

            return 0

        lax.fori_loop(0, STEPS, step, 0)
        return 0

    lax.fori_loop(0, chunks, chunk_body, 0)

    lane = lax.broadcasted_iota(jnp.int32, (lev_dev, 128), 1)
    level_at = lax.broadcasted_iota(jnp.int32, (lev_dev, 128), 0)
    half_row = 64
    low = -1e30

    def grid_block(k, j, lo, hi):
        at = j * tall if isinstance(j, int) else pl.multiple_of(j * tall, tall)
        total = None
        for ch in range(lo, hi):
            one = flat_dot(
                recv[chunks + ch * STEPS + k, :, pl.ds(at, tall)].T,
                table[ch * cols : (ch + 1) * cols, :],
            )
            total = one if total is None else total + one
        return total

    def folded(tile, op):
        out = tile[:, :128]
        for n in range(1, NLON // 128):
            out = op(out, tile[:, n * 128 : (n + 1) * 128])
        return out

    def mass_block(tile, weights, carry):
        top, total = carry
        levels = [tile[n * piece : (n + 1) * piece] for n in range(lev_dev)]
        block_top = jnp.concatenate(
            [jnp.max(folded(x, jnp.maximum), axis=0, keepdims=True) for x in levels], axis=0
        )
        block_top = jnp.max(block_top, axis=1, keepdims=True)
        new_top = jnp.maximum(top, jnp.broadcast_to(block_top, top.shape))
        sums = []
        for n in range(lev_dev):
            x = jnp.exp(levels[n] - new_top[n : n + 1, 0:1])
            sums.append(jnp.sum(folded(x, jnp.add) * weights, axis=0, keepdims=True))
        block_sum = jnp.sum(jnp.concatenate(sums, axis=0), axis=1, keepdims=True)
        return new_top, total * jnp.exp(top - new_top) + block_sum

    empty = (
        jnp.full((lev_dev, 128), low, jnp.float32),
        jnp.zeros((lev_dev, 128), jnp.float32),
    )

    def packed_row(carry, base):
        top, total = carry
        return jnp.sum(
            jnp.where(lane == level_at + base, top, 0.0)
            + jnp.where(lane == level_at + base + half_row, total, 0.0),
            axis=0,
            keepdims=True,
        )

    last = STEPS - 1
    for ch in range(chunks - 1):
        wait_recv(chunks + ch * STEPS + last)
    if chunks > 1:

        def part(j, _):
            acc[pl.ds(pl.multiple_of(j * tall, tall), tall), :] = grid_block(
                last, j, 0, chunks - 1
            )
            return 0

        lax.fori_loop(0, splits, part, 0)

    def early(k, row):
        def take(ch, _):
            wait_recv(chunks + ch * STEPS + k)
            return 0

        lax.fori_loop(0, chunks, take, 0)

        def part(j, carry):
            return mass_block(grid_block(k, j, 0, chunks), weight_rows[j], carry)

        return row + packed_row(lax.fori_loop(0, splits, part, empty), k * lev_dev)

    zero_row = jnp.zeros((1, 128), jnp.float32)
    early_send[0:1, :] = lax.fori_loop(0, last, early, zero_row)
    wide_lane = lax.broadcasted_iota(jnp.int32, (LEV, 128), 1)
    diag = lax.broadcasted_iota(jnp.int32, (LEV, 128), 0)
    means_row = zero_row
    for n in range(STEPS):
        column = jnp.sum(jnp.where(wide_lane == 0, means[n], 0.0), axis=1, keepdims=True)
        means_row = means_row + jnp.sum(
            jnp.where(wide_lane == diag + LEV * n, column, 0.0), axis=0, keepdims=True
        )
    early_send[1:2, :] = means_row
    place_here = lev_id * bands + band_id

    def share(source, target, sems):
        def one(o, _):
            db, dz = peer(o)
            pltpu.make_async_remote_copy(
                src_ref=source,
                dst_ref=target.at[place_here],
                send_sem=sems.at[0],
                recv_sem=sems.at[1],
                device_id=(db, dz),
                device_id_type=MESH,
            ).start()
            return 0

        lax.fori_loop(1, devs, one, 0)
        pltpu.make_async_copy(source, target.at[place_here], sems.at[1]).start()

    def shared(target, sems):
        pltpu.make_async_copy(target, target, sems.at[1]).wait()

    def sent(target, sems):
        rest = target.at[pl.ds(0, devs - 1)]
        pltpu.make_async_copy(rest, rest, sems.at[0]).wait()

    share(early_send, early_recv, early_sem)
    carry = empty
    for j in range(splits):
        arrived = recv.at[final, :, pl.ds(j * tall, tall)]
        pltpu.make_async_copy(arrived, arrived, piece_sem.at[j]).wait()
        tile = grid_block(last, j, chunks - 1, chunks)
        if chunks > 1:
            tile = tile + acc[j * tall : (j + 1) * tall, :]
        acc[j * tall : (j + 1) * tall, :] = tile
        carry = mass_block(tile, weight_rows[j], carry)
    late_send[0:1, :] = packed_row(carry, 0)
    share(late_send, late_recv, late_sem)

    row_lane = lax.broadcasted_iota(jnp.int32, (8, 128), 1)
    to_grid = math.sqrt(2.0 / NT) * float(np.float32(math.sqrt(2.0 / NLON)).astype(jnp.bfloat16))
    lat_sum = sum(math.cos(math.pi * ((n + 0.5) / NLAT - 0.5)) for n in range(NLAT))
    normaliser = sum(1.0 + 2.0 * n / (LEV - 1) for n in range(LEV)) * lat_sum * NLON
    fix_scale = math.sqrt(NT * NLON) / 2.0

    def gathered(target):
        out = []
        for z in range(levs):
            top = target[z * bands, 0:1, :]
            for b in range(1, bands):
                top = jnp.maximum(top, target[z * bands + b, 0:1, :])
            total = zero_row
            for b in range(bands):
                here = target[z * bands + b, 0:1, :]
                total = total + jnp.exp(here - top) * pltpu.roll(
                    jnp.broadcast_to(here, (8, 128)), 128 - half_row, 1
                )[0:1]
            out.append((jnp.broadcast_to(top, (8, 128)), jnp.broadcast_to(total, (8, 128))))
        return out

    def fix_of(parts, base, shift):
        valid = jnp.logical_and(row_lane >= base, row_lane < base + lev_dev)
        total = jnp.zeros((8, 128), jnp.float32)
        for z in range(levs):
            turn_by = (base - z * lev_dev) % 128
            moved = pltpu.roll(shift, turn_by, 1) if turn_by else shift
            level = (row_lane - base + z * lev_dev).astype(jnp.float32)
            top, amount = parts[z]
            total = total + jnp.where(
                valid,
                jnp.exp(jnp.where(valid, top + moved, 0.0))
                * amount
                * (1.0 + 2.0 * level / (LEV - 1)),
                0.0,
            )
        total = jnp.sum(total, axis=1, keepdims=True)
        return jnp.log(target_ref[0] / (total / normaliser))

    shared(early_recv, early_sem)
    parts = gathered(early_recv)
    base_row = zero_row
    for d in range(devs):
        base_row = base_row + early_recv[d, 1:2, :]
    base_row = jnp.broadcast_to(base_row, (8, 128))
    is_level = row_lane < LEV
    carried = jnp.zeros((8, 128), jnp.float32)
    for n in range(STEPS):
        back = (128 - LEV * n) % 128
        base_n = pltpu.roll(base_row, back, 1) if back else base_row
        column = jnp.sum(mix_ref[n] * carried[0:1, :LEV], axis=1, keepdims=True)
        moved_by = jnp.broadcast_to(
            jnp.sum(jnp.where(wide_lane == diag, column, 0.0), axis=0, keepdims=True), (8, 128)
        )
        moved = (base_n + moved_by).astype(jnp.bfloat16).astype(jnp.float32) - base_n.astype(
            jnp.bfloat16
        ).astype(jnp.float32)
        shift = jnp.where(is_level, moved * to_grid, 0.0)
        if n < last:
            fix = fix_of(parts, n * lev_dev, shift)
            fix_ref[n] = fix[0, 0]
            carried = jnp.where(is_level, moved_by + fix * fix_scale, 0.0)

    own_lane = lev_id * lev_dev + level_at
    own = jnp.sum(jnp.where(lane == own_lane, shift[0:1], 0.0), axis=1, keepdims=True)
    for j in range(splits):
        for n in range(lev_dev):
            here = (j * lev_dev + n) * piece
            out_ref[n, j * piece : (j + 1) * piece, :] = (
                acc[here : here + piece, :] + own[n : n + 1, 0:1]
            ).astype(jnp.bfloat16)

    shared(late_recv, late_sem)
    fix_ref[last] = fix_of(gathered(late_recv), 0, shift)[0, 0]

    def finish(t, _):
        left = send.at[t, pl.ds(0, (devs - 1) * rows), :]
        pltpu.make_async_copy(left, left, send_sem.at[t]).wait()
        return 0

    lax.fori_loop(0, chunks * (1 + STEPS), finish, 0)
    sent(early_recv, early_sem)
    sent(late_recv, late_sem)


def body(
    increment, background, legendre, coupling, damping, target_mass, numerators, pair_low, lat_map
):
    band_count = lax.axis_size("band")
    lev_count = lax.axis_size("lev")
    devs = band_count * lev_count
    lev_dev, lat_dev = increment.shape[:2]
    pair_dev = legendre.shape[0]
    points = lev_dev * lat_dev
    cols = devs * 4 * GROUP
    fits = (
        lat_dev % 32 == 0
        and pair_dev % GROUP == 0
        and lev_dev == 8
        and band_count * 4 * GROUP == 128
        and lev_count * lev_dev == LEV
        and STEPS * lev_dev <= 64
        and points % 256 == 0
        and LEV * STEPS == 128
    )
    if not fits:
        return body_general(
            increment,
            background,
            legendre,
            coupling,
            damping,
            target_mass,
            numerators,
            pair_low,
            lat_map,
        )
    chunks = pair_dev // GROUP
    vmem = pl.BlockSpec(memory_space=pltpu.VMEM)
    smem = pl.BlockSpec(memory_space=pltpu.SMEM)
    hbm = pl.BlockSpec(memory_space=pl.ANY)
    total = chunks * (1 + STEPS)
    dma = pltpu.SemaphoreType.DMA
    return pl.pallas_call(
        lambda *refs: exchange_kernel(
            (band_count, lev_count, lev_dev, lat_dev, chunks), *refs
        ),
        out_shape=(
            pltpu.VMEM((lev_dev, lat_dev, NLON), jnp.bfloat16),
            jax.ShapeDtypeStruct((STEPS,), jnp.float32),
        ),
        in_specs=[smem] * 3 + [hbm] * 3 + [vmem] * 3,
        out_specs=(vmem, smem),
        scratch_shapes=[
            pltpu.VMEM((GROUP, 8, NT + 2), jnp.float32),
            pltpu.VMEM((STEPS, LEV, LEV), jnp.float32),
            pltpu.VMEM((points, NLON), jnp.bfloat16),
            pltpu.VMEM((chunks * cols, NLON), jnp.bfloat16),
            pltpu.VMEM((NLAT, NLAT), jnp.bfloat16),
            pltpu.VMEM((2, NT + 2, NLAT), jnp.bfloat16),
            pltpu.VMEM((GROUP, NT + 2, NLAT), jnp.bfloat16),
            pltpu.VMEM((2, 2 * LEV, NT + 2), jnp.float32),
            pltpu.VMEM((GROUP, 2 * LEV, NT + 2), jnp.float32),
            pltpu.VMEM((GROUP, 2 * LEV, NT + 2), jnp.float32),
            pltpu.VMEM((NLAT // 128, LEV * 4 * GROUP, 128), jnp.float32),
            pltpu.VMEM((points, NLON), jnp.float32),
            pltpu.VMEM((total, cols, points), jnp.bfloat16),
            pltpu.VMEM((total, cols, points), jnp.bfloat16),
            pltpu.VMEM((STEPS, LEV, 128), jnp.float32),
            pltpu.VMEM((lat_dev // 32, 32, 128), jnp.float32),
            pltpu.VMEM((2, 128), jnp.float32),
            pltpu.VMEM((devs, 2, 128), jnp.float32),
            pltpu.VMEM((1, 128), jnp.float32),
            pltpu.VMEM((devs, 1, 128), jnp.float32),
            dma,
            dma((2,)),
            dma((2,)),
            dma((total,)),
            dma((total,)),
            dma((lat_dev // 32,)),
            dma((2,)),
            dma((2,)),
        ],
        compiler_params=pltpu.CompilerParams(
            collective_id=0, has_side_effects=True, vmem_limit_bytes=62000000
        ),
    )(
        numerators,
        damping,
        target_mass,
        increment,
        legendre.transpose(0, 2, 1),
        background.reshape(pair_dev, 2 * LEV, NT + 2),
        pair_low,
        lat_map,
        coupling,
    )


def solution(mesh):
    return jax.shard_map(
        body,
        mesh=mesh,
        in_specs=(
            P("lev", "band", None),
            P(("band", "lev"), None, None, None),
            P(("band", "lev"), None, None),
            P(),
            P(),
            P(),
            P(),
            P(),
            P(),
        ),
        out_specs=(P("lev", "band", None), P()),
        check_vma=False,
    )
```

```python
import math

import jax
import numpy as np
import jax.numpy as jnp
from jax import lax
from jax.experimental import pallas as pl
from jax.experimental.pallas import tpu as pltpu
from jax.sharding import PartitionSpec as P

NT = 767
NLAT = 768
NLON = 1536
LEV = 32
STEPS = 4
DEN = 64
NPAIR = 384
AXES = ("band", "lev")


def wave_table(pair_low):
    column = jnp.arange(4 * pair_low.shape[0], dtype=jnp.int32)
    low = jnp.repeat(pair_low, 4)
    wavenumber = jnp.where(column // 2 % 2 == 0, low, NT - low)[:, None]
    quarter = (column % 2 * (NLON // 4))[:, None]
    fine = math.gcd(128, NLON)
    unit = 2.0 * math.pi / NLON
    coarse_pts = jnp.arange(NLON // fine, dtype=jnp.int32)[None, :] * fine
    coarse = ((wavenumber * coarse_pts + quarter) % NLON).astype(jnp.float32) * unit
    rest = (wavenumber * jnp.arange(fine, dtype=jnp.int32)[None, :] % NLON).astype(
        jnp.float32
    ) * unit
    norm = math.sqrt(2.0 / NLON)
    cos_a, sin_a, cos_b, sin_b = lax.optimization_barrier(
        (jnp.cos(coarse) * norm, jnp.sin(coarse) * norm, jnp.cos(rest), jnp.sin(rest))
    )
    blocks = [
        cos_a[:, i : i + 1] * cos_b - sin_a[:, i : i + 1] * sin_b for i in range(NLON // fine)
    ]
    return jnp.concatenate(blocks, axis=1).astype(jnp.bfloat16)


def lat_weights(lat_rows):
    return jnp.cos(math.pi * ((lat_rows.astype(jnp.float32) + 0.5) / NLAT - 0.5))


def degrees(low_wave):
    columns = jnp.arange(NT + 2, dtype=jnp.int32)
    in_second = columns[None, :] >= NT + 1 - low_wave[:, None]
    degree = jnp.where(in_second, columns[None, :] - 1, low_wave[:, None] + columns[None, :])
    return (degree.astype(jnp.float32), in_second)


def body_general(
    increment, background, legendre, coupling, damping, target_mass, numerators, pair_low, lat_map
):
    band_count = lax.axis_size("band")
    lev_count = lax.axis_size("lev")
    device_count = band_count * lev_count
    band_id = lax.axis_index("band")
    lev_id = lax.axis_index("lev")
    lev_dev = increment.shape[0]
    lat_dev = increment.shape[1]
    pair_dev = legendre.shape[0]
    points = lev_dev * lat_dev
    fourier_tab = wave_table(pair_low)
    local_lats = lax.dynamic_slice_in_dim(lat_map, band_id * lat_dev, lat_dev)
    row_weight = lat_weights(local_lats)
    all_levels = 1.0 + 2.0 * jnp.arange(LEV, dtype=jnp.float32) / (LEV - 1)
    normaliser = (
        jnp.sum(all_levels) * jnp.sum(lat_weights(jnp.arange(NLAT, dtype=jnp.int32))) * NLON
    )
    fix_scale = math.sqrt(NT * NLON) / 2.0
    own_pairs = lax.dynamic_slice_in_dim(
        pair_low, (band_id * lev_count + lev_id) * pair_dev, pair_dev
    )
    degree, in_second = degrees(own_pairs)
    holder = (own_pairs == 0).astype(jnp.float32)

    fourier = jnp.einsum(
        "ck,xk->cx",
        fourier_tab,
        increment.reshape(points, NLON),
        preferred_element_type=jnp.float32,
    )
    fourier = (fourier * jnp.tile(row_weight, lev_dev)[None, :]).astype(jnp.bfloat16)
    received = lax.all_to_all(
        fourier.reshape(device_count, pair_dev * 4, points), AXES, split_axis=0, concat_axis=0
    )

    pick = (lat_map[:, None] == jnp.arange(NLAT, dtype=jnp.int32)[None, :]).astype(jnp.bfloat16)
    stored = jnp.einsum(
        "jn,pnc->pjc", pick, legendre, preferred_element_type=jnp.float32
    ).astype(jnp.bfloat16)

    received = received.reshape(band_count, lev_count, pair_dev * 4, lev_dev, lat_dev)
    waves_in = received.transpose(2, 1, 3, 0, 4).reshape(pair_dev, 4 * LEV, NLAT)
    coeffs = jnp.einsum("prj,pjc->prc", waves_in, stored, preferred_element_type=jnp.float32)
    coeffs = coeffs.reshape(pair_dev, 2, 2, LEV, NT + 2) * math.sqrt(2.0 / NLAT)
    second_cols = in_second[:, None, None, :]
    smoothing = 1.0 / (1.0 + (degree / NT) ** 4)
    incr_spec = jnp.where(second_cols, coeffs[:, 1], coeffs[:, 0]) * smoothing[:, None, None, :]
    shape_term = degree * (degree + 1.0) / (NT * (NT + 1.0))

    spectral = background
    means = []
    arrived = []
    for step_idx in range(STEPS):
        coupled = 0.7 * spectral + 0.4 * jnp.einsum(
            "lm,prmc->prlc", coupling[step_idx], spectral, precision=lax.Precision.HIGHEST
        )
        weight_now = numerators[step_idx].astype(jnp.float32) / DEN
        spectral = (
            coupled / (1.0 + damping[step_idx] * shape_term)[:, None, None, :]
            + weight_now * incr_spec
        )
        means.append(jnp.sum(spectral[:, 0, :, 0] * holder[:, None], axis=0))
        spec_bf = spectral.astype(jnp.bfloat16)
        zeros_bf = jnp.zeros_like(spec_bf)
        split_rows = jnp.stack(
            [jnp.where(second_cols, zeros_bf, spec_bf), jnp.where(second_cols, spec_bf, zeros_bf)],
            axis=1,
        )
        waves_f = jnp.einsum(
            "prc,pjc->prj",
            split_rows.reshape(pair_dev, 4 * LEV, NT + 2),
            stored,
            preferred_element_type=jnp.float32,
        )
        waves_bf = (waves_f * math.sqrt(2.0 / NT)).astype(jnp.bfloat16)
        outgoing = waves_bf.reshape(pair_dev * 4, lev_count, lev_dev, band_count, lat_dev)
        outgoing = outgoing.transpose(3, 1, 0, 2, 4).reshape(device_count, pair_dev * 4, points)
        spectral, outgoing = lax.optimization_barrier((spectral, outgoing))
        arrived.append(lax.all_to_all(outgoing, AXES, split_axis=0, concat_axis=0))

    tops, sums = [], []
    for step_idx in range(STEPS):
        grid_now = jnp.einsum(
            "cx,ck->xk",
            arrived[step_idx].reshape(NPAIR * 4, points),
            fourier_tab,
            preferred_element_type=jnp.float32,
        ).reshape(lev_dev, lat_dev, NLON)
        top = jnp.max(grid_now, axis=(1, 2))
        tops.append(top)
        sums.append(
            jnp.sum(
                jnp.sum(jnp.exp(grid_now - top[:, None, None]), axis=2) * row_weight[None, :],
                axis=1,
            )
        )

    packed = jnp.concatenate(
        [jnp.stack(tops).reshape(-1), jnp.stack(sums).reshape(-1), jnp.stack(means).reshape(-1)]
    )
    gathered = lax.all_to_all(
        jnp.broadcast_to(packed[None, :], (device_count, packed.shape[0])),
        AXES,
        split_axis=0,
        concat_axis=0,
    )
    count = STEPS * lev_dev
    all_tops = gathered[:, :count].reshape(band_count, lev_count, STEPS, lev_dev)
    all_sums = gathered[:, count : 2 * count].reshape(band_count, lev_count, STEPS, lev_dev)
    all_tops = all_tops.transpose(2, 0, 1, 3).reshape(STEPS, band_count, LEV)
    all_sums = all_sums.transpose(2, 0, 1, 3).reshape(STEPS, band_count, LEV)
    all_means = jnp.sum(gathered[:, 2 * count :], axis=0).reshape(STEPS, LEV)

    table_entry = jnp.full((), math.sqrt(2.0 / NLON), jnp.bfloat16).astype(jnp.float32)
    to_grid = math.sqrt(2.0 / NT) * table_entry
    carried = jnp.zeros((LEV,), jnp.float32)
    shift = jnp.zeros((LEV,), jnp.float32)
    fix_list = []
    for step_idx in range(STEPS):
        carried = 0.7 * carried + 0.4 * jnp.sum(coupling[step_idx] * carried[None, :], axis=1)
        base = all_means[step_idx]
        moved = (base + carried).astype(jnp.bfloat16).astype(jnp.float32) - base.astype(
            jnp.bfloat16
        ).astype(jnp.float32)
        shift = moved * to_grid
        total = jnp.sum(
            jnp.exp(all_tops[step_idx] + shift[None, :]) * all_sums[step_idx] * all_levels[None, :]
        )
        mass_fix = jnp.log(target_mass[0] / (total / normaliser))
        fix_list.append(mass_fix)
        carried = carried + mass_fix * fix_scale
    own_shift = lax.dynamic_slice_in_dim(shift, lev_id * lev_dev, lev_dev)
    analysis = (grid_now + own_shift[:, None, None]).astype(jnp.bfloat16)
    return (analysis, jnp.stack(fix_list))


GROUP = 4
MESH = pl.DeviceIdType.MESH
LAST = (((1,), (1,)), ((), ()))


def sine(x):
    y = x * x
    out = -1.0 / math.factorial(11)
    for n in (9, 7, 5, 3, 1):
        out = out * y + (1.0 if n % 4 == 1 else -1.0) / math.factorial(n)
    return out * x


def table_values(phase):
    turns = jnp.floor((phase + 0.5) * (1.0 / NLON))
    rest = jnp.abs(phase - turns * NLON - NLON / 2) - NLON / 4
    return (sine(rest * (2.0 * math.pi / NLON)) * math.sqrt(2.0 / NLON)).astype(jnp.bfloat16)


def flat_dot(a, b):
    return jnp.dot(a, b, preferred_element_type=jnp.float32)


def exchange_kernel(
    sizes,
    numer_in,
    damp_in,
    target_in,
    inc_ref,
    leg_ref,
    back_ref,
    pair_in,
    lat_in,
    coupling_in,
    out_ref,
    fix_ref,
    numer_ref,
    damp_ref,
    target_ref,
    pair_ref,
    lat_ref,
    coupling_ref,
    small_sem,
    consts_ref,
    mix_ref,
    points_in,
    table,
    pick,
    leg_buf,
    stored,
    back_buf,
    incr,
    spec,
    turn,
    acc,
    send,
    recv,
    means,
    weight_rows,
    early_send,
    early_recv,
    late_send,
    late_recv,
    load_sem,
    leg_sem,
    back_sem,
    send_sem,
    recv_sem,
    piece_sem,
    early_sem,
    late_sem,
):
    bands, levs, lev_dev, lat_dev, chunks = sizes
    devs = bands * levs
    band_id = lax.axis_index("band")
    lev_id = lax.axis_index("lev")
    me = band_id * levs + lev_id
    piece = 32
    splits = lat_dev // piece
    rows = 4 * GROUP
    cols = devs * rows
    points = lev_dev * lat_dev
    slots = chunks * GROUP
    per_tile = 128 // piece
    halves = lev_dev // per_tile

    barrier = pltpu.get_barrier_semaphore()

    def peer(o):
        return (
            lax.rem(band_id + lax.rem(o, bands), bands),
            lax.rem(lev_id + o // bands, levs),
        )

    def greet(o, _):
        pl.semaphore_signal(barrier, inc=1, device_id=peer(o), device_id_type=MESH)
        return 0

    lax.fori_loop(1, devs, greet, 0)

    small = [
        pltpu.make_async_copy(source, target, small_sem.at[n])
        for n, (source, target) in enumerate(
            [
                (pair_in, pair_ref),
                (lat_in, lat_ref),
                (coupling_in, coupling_ref),
                (numer_in, numer_ref),
                (damp_in, damp_ref),
                (target_in, target_ref),
            ]
        )
    ]
    for copy in small:
        copy.start()

    def load_piece(i, j):
        return pltpu.make_async_copy(
            inc_ref.at[i, pl.ds(j * piece, piece), :],
            points_in.at[pl.ds((j * lev_dev + i) * piece, piece), :],
            load_sem,
        )

    for j in range(splits):
        for i in range(lev_dev):
            load_piece(i, j).start()

    def leg_copy(slot):
        return pltpu.make_async_copy(
            leg_ref.at[slot], leg_buf.at[lax.rem(slot, 2)], leg_sem.at[lax.rem(slot, 2)]
        )

    def back_copy(slot):
        return pltpu.make_async_copy(
            back_ref.at[slot], back_buf.at[lax.rem(slot, 2)], back_sem.at[lax.rem(slot, 2)]
        )

    for slot in range(2):
        leg_copy(slot).start()
        back_copy(slot).start()

    home = pl.ds((lev_id * bands + band_id) * rows, rows)

    def send_level(t, z):
        def one(o, _):
            band = lax.rem(band_id + o, bands)
            block = send.at[t, pl.ds((z * bands + band) * rows, rows), :]
            own = jnp.logical_and(o == 0, z == lev_id)

            @pl.when(own)
            def _():
                pltpu.make_async_copy(block, recv.at[t, home, :], recv_sem.at[t]).start()

            @pl.when(jnp.logical_not(own))
            def _():
                pltpu.make_async_remote_copy(
                    src_ref=block,
                    dst_ref=recv.at[t, home, :],
                    send_sem=send_sem.at[t],
                    recv_sem=recv_sem.at[t],
                    device_id=(band, z),
                    device_id_type=MESH,
                ).start()

            return 0

        lax.fori_loop(0, bands, one, 0)

    final = chunks * (1 + STEPS) - 1
    tall = lev_dev * piece

    def send_pieces():
        def one(n, _):
            j = n // devs
            o = lax.rem(n, bands)
            z = level_order(lax.rem(n // bands, levs))
            band = lax.rem(band_id + o, bands)
            lanes = pl.ds(pl.multiple_of(j * 128, 128), 128)
            block = send.at[final, pl.ds((z * bands + band) * rows, rows), lanes]
            own = jnp.logical_and(o == 0, z == lev_id)

            @pl.when(own)
            def _():
                pltpu.make_async_copy(
                    block, recv.at[final, home, lanes], piece_sem.at[j]
                ).start()

            @pl.when(jnp.logical_not(own))
            def _():
                pltpu.make_async_remote_copy(
                    src_ref=block,
                    dst_ref=recv.at[final, home, lanes],
                    send_sem=send_sem.at[final],
                    recv_sem=piece_sem.at[j],
                    device_id=(band, z),
                    device_id_type=MESH,
                ).start()

            return 0

        lax.fori_loop(0, splits * halves * devs, one, 0)

    def level_order(n):
        return lax.rem(lev_id + levs // 2 + n, levs)

    def wait_recv(t):
        pltpu.make_async_copy(recv.at[t], recv.at[t], recv_sem.at[t]).wait()

    lane_part = lax.broadcasted_iota(jnp.int32, (rows, 128), 1) // piece

    def gather_pieces(parts):
        out = parts[0]
        for n in range(1, per_tile):
            out = jnp.where(lane_part == n, parts[n], out)
        return out

    def rolled(x, amount):
        amount = amount * piece % 128
        return pltpu.roll(x, amount, 1) if amount else x

    small[0].wait()
    small[1].wait()
    lat_row = lat_ref[...].reshape(1, -1)
    lat_now = (lat_row.astype(jnp.float32) + 0.5) / NLAT - 0.5
    lat_now = jnp.broadcast_to(sine((0.5 - jnp.abs(lat_now)) * math.pi), (rows, NLAT))
    weight_tiles = []
    for j in range(splits):
        tile = jnp.zeros((rows, 128), jnp.float32)
        for b in range(bands):
            t, n = (b * splits + j) // per_tile, (b * splits + j) % per_tile
            source = lat_now[:, t * 128 : (t + 1) * 128]
            part = gather_pieces([rolled(source, il - n) for il in range(per_tile)])
            tile = jnp.where(band_id == b, part, tile)
        weight_tiles += [tile] * halves
    row_weight = jnp.concatenate(weight_tiles, axis=1)[0:1]
    pairs = pair_ref[...].reshape(1, -1).astype(jnp.float32)
    pair_count = pairs.shape[1]
    pair_dev = chunks * GROUP

    block_rows = bands * rows

    def fourier(n, _):
        ch = n // levs
        z = level_order(lax.rem(n, levs))
        col = lax.broadcasted_iota(jnp.int32, (block_rows, 1), 0)
        place = ((col >> 4) * levs + z) * pair_dev + ch * GROUP + ((col & 15) >> 2)
        spot = lax.broadcasted_iota(jnp.int32, (block_rows, pair_count), 1) == place
        wave = jnp.sum(jnp.where(spot, pairs, 0.0), axis=1, keepdims=True)
        wave = jnp.where((col & 2) == 0, wave, NT - wave)
        wave = jnp.broadcast_to(wave, (block_rows, 128))
        quarter = ((col & 1) * (NLON // 4)).astype(jnp.float32)
        lanes = lax.broadcasted_iota(jnp.int32, (1, 128), 1).astype(jnp.float32)
        at = pl.multiple_of(z * block_rows, block_rows)
        spot_rows = pl.ds(pl.multiple_of(ch * cols + at, block_rows), block_rows)
        for kc in range(NLON // 128):
            table[spot_rows, kc * 128 : (kc + 1) * 128] = table_values(
                wave * (lanes + kc * 128.0) + quarter
            )

        @pl.when(n == 0)
        def _():
            pltpu.make_async_copy(points_in, points_in, load_sem).wait()

        got = lax.dot_general(
            table[spot_rows, :], points_in[...], LAST, preferred_element_type=jnp.float32
        )
        send[ch, pl.ds(at, block_rows), :] = (got * row_weight).astype(jnp.bfloat16)

        @pl.when(n == 0)
        def _():
            pl.semaphore_wait(barrier, devs - 1)

        send_level(ch, z)
        return 0

    lax.fori_loop(0, chunks * levs, fourier, 0)

    lane_at = lax.broadcasted_iota(jnp.int32, (piece, 128), 1)
    row_at = lax.broadcasted_iota(jnp.int32, (piece, 128), 0)
    for j in range(splits):
        lane_weight = row_weight[:, j * lev_dev * piece : j * lev_dev * piece + 128]
        weight_rows[j] = jnp.broadcast_to(
            jnp.sum(jnp.where(lane_at == row_at, lane_weight, 0.0), axis=1, keepdims=True),
            (piece, 128),
        )
    pick[...] = (
        (lax.broadcasted_iota(jnp.int32, (NLAT, NLAT), 0) == lat_row)
        .astype(jnp.float32)
        .astype(jnp.bfloat16)
    )
    means[...] = jnp.zeros_like(means)
    for copy in small[2:]:
        copy.wait()
    square = [lax.broadcasted_iota(jnp.int32, (LEV, LEV), n) for n in range(2)]
    for n in range(STEPS):
        mix_ref[n] = jnp.where(square[0] == square[1], 0.7, 0.0) + 0.4 * coupling_ref[n]

    def chunk_body(ch, _):
        def prepare(s, _):
            slot = ch * GROUP + s
            leg_copy(slot).wait()
            stored[s] = flat_dot(leg_buf[lax.rem(slot, 2)], pick[...]).astype(jnp.bfloat16)
            spot = lax.broadcasted_iota(jnp.int32, (1, pair_count), 1) == me * pair_dev + slot
            low_wave = jnp.sum(jnp.where(spot, pairs, 0.0), axis=1, keepdims=True)
            column = lax.broadcasted_iota(jnp.int32, (1, NT + 2), 1).astype(jnp.float32)
            second = column >= NT + 1 - low_wave
            degree = jnp.where(second, column - 1.0, low_wave + column)
            ratio = degree / NT
            ratio = ratio * ratio
            shape_term = degree * (degree + 1.0) / (NT * (NT + 1.0))
            consts_ref[s, 0:1, :] = second.astype(jnp.float32)
            consts_ref[s, 1:2, :] = 1.0 / (1.0 + ratio * ratio)
            for n in range(STEPS):
                consts_ref[s, 2 + n : 3 + n, :] = 1.0 / (1.0 + damp_ref[n] * shape_term)
            consts_ref[s, 6:7, :] = jnp.broadcast_to(
                (low_wave == 0.0).astype(jnp.float32), (1, NT + 2)
            )

            @pl.when(slot + 2 < slots)
            def _():
                leg_copy(slot + 2).start()

            return 0

        lax.fori_loop(0, GROUP, prepare, 0)
        wait_recv(ch)

        def arrive(z, _):
            for half in range(halves):
                for t in range(NLAT // 128):
                    tiles = []
                    for n in range(per_tile):
                        g = t * per_tile + n
                        b, j = g // splits, g % splits
                        lane0 = (j * halves + half) * 128
                        tiles.append(
                            recv[
                                ch,
                                pl.ds(pl.multiple_of((z * bands + b) * rows, rows), rows),
                                lane0 : lane0 + 128,
                            ].astype(jnp.float32)
                        )
                    for il in range(per_tile):
                        level = z * lev_dev + half * per_tile + il
                        turn[t, pl.ds(pl.multiple_of(level * rows, rows), rows), :] = gather_pieces([rolled(tiles[n], n - il) for n in range(per_tile)])
            return 0

        lax.fori_loop(0, levs, arrive, 0)

        def direct(s, _):
            slot = ch * GROUP + s
            back_copy(slot).wait()
            waves_in = jnp.concatenate(
                [
                    jnp.concatenate(
                        [
                            turn[t, pl.ds(s * 4 + qr, LEV, stride=rows), :]
                            for t in range(NLAT // 128)
                        ],
                        axis=1,
                    )
                    for qr in range(4)
                ],
                axis=0,
            ).astype(jnp.bfloat16)
            coeffs = lax.dot_general(
                waves_in, stored[s], LAST, preferred_element_type=jnp.float32
            ) * math.sqrt(2.0 / NLAT)
            second = consts_ref[s, 0:1, :] > 0.5
            incr[s] = (
                jnp.where(second, coeffs[2 * LEV :], coeffs[: 2 * LEV]) * consts_ref[s, 1:2, :]
            )
            spec[s] = back_buf[lax.rem(slot, 2)]

            @pl.when(slot + 2 < slots)
            def _():
                back_copy(slot + 2).start()

            return 0

        lax.fori_loop(0, GROUP, direct, 0)

        def step(k, _):
            def inverse(s, _):
                second = consts_ref[s, 0:1, :] > 0.5
                inv = consts_ref[s, pl.ds(2 + k, 1), :]
                mix = mix_ref[k]
                weight = numer_ref[k].astype(jnp.float32) / DEN
                now = [
                    jnp.dot(
                        mix,
                        spec[s, r * LEV : (r + 1) * LEV, :],
                        precision=lax.Precision.HIGHEST,
                        preferred_element_type=jnp.float32,
                    )
                    * inv
                    + weight * incr[s, r * LEV : (r + 1) * LEV, :]
                    for r in range(2)
                ]
                for r in range(2):
                    spec[s, r * LEV : (r + 1) * LEV, :] = now[r]
                means[k] += now[0][:, :128] * consts_ref[s, 6:7, :128]
                both = jnp.concatenate(now, axis=0)
                split = jnp.concatenate(
                    [jnp.where(second, 0.0, both), jnp.where(second, both, 0.0)], axis=0
                ).astype(jnp.bfloat16)
                waves = flat_dot(split, stored[s]) * math.sqrt(2.0 / NT)
                for qr in range(4):
                    for t in range(NLAT // 128):
                        turn[t, pl.ds(s * 4 + qr, LEV, stride=rows), :] = waves[
                            qr * LEV : (qr + 1) * LEV, t * 128 : (t + 1) * 128
                        ]
                return 0

            lax.fori_loop(0, GROUP, inverse, 0)
            t_out = chunks + ch * STEPS + k

            def depart(zi, _):
                z = level_order(zi)
                for half in range(halves):
                    for t in range(NLAT // 128):
                        tiles = []
                        for il in range(per_tile):
                            level = z * lev_dev + half * per_tile + il
                            tiles.append(
                                turn[t, pl.ds(pl.multiple_of(level * rows, rows), rows), :]
                            )
                        for n in range(per_tile):
                            g = t * per_tile + n
                            b, j = g // splits, g % splits
                            lane0 = (j * halves + half) * 128
                            send[
                                t_out,
                                pl.ds(pl.multiple_of((z * bands + b) * rows, rows), rows),
                                lane0 : lane0 + 128,
                            ] = gather_pieces(
                                [rolled(tiles[il], il - n) for il in range(per_tile)]
                            ).astype(jnp.bfloat16)

                @pl.when(k != STEPS - 1)
                def _():
                    send_level(t_out, z)

                return 0

            lax.fori_loop(0, levs, depart, 0)
            return 0

        lax.fori_loop(0, STEPS, step, 0)
        return 0

    lax.fori_loop(0, chunks, chunk_body, 0)

    def send_last(n, _):
        send_level(chunks + n // levs * STEPS + STEPS - 1, level_order(lax.rem(n, levs)))
        return 0

    lax.fori_loop(0, (chunks - 1) * levs, send_last, 0)

    lane = lax.broadcasted_iota(jnp.int32, (lev_dev, 128), 1)
    level_at = lax.broadcasted_iota(jnp.int32, (lev_dev, 128), 0)
    half_row = 64
    low = -1e30

    def grid_block(k, j, lo, hi, size=None):
        size = size or tall
        at = j * size if isinstance(j, int) else pl.multiple_of(j * size, size)
        total = None
        for ch in range(lo, hi):
            one = flat_dot(
                recv[chunks + ch * STEPS + k, :, pl.ds(at, size)].T,
                table[ch * cols : (ch + 1) * cols, :],
            )
            total = one if total is None else total + one
        return total

    def folded(tile, op):
        out = tile[:, :128]
        for n in range(1, NLON // 128):
            out = op(out, tile[:, n * 128 : (n + 1) * 128])
        return out

    def mass_block(tile, weights, carry):
        top, total = carry
        count = tile.shape[0] // piece
        levels = [tile[n * piece : (n + 1) * piece] for n in range(count)]
        block_top = jnp.concatenate(
            [jnp.max(folded(x, jnp.maximum), axis=0, keepdims=True) for x in levels], axis=0
        )
        block_top = jnp.max(block_top, axis=1, keepdims=True)
        new_top = jnp.maximum(top, jnp.broadcast_to(block_top, top.shape))
        sums = []
        for n in range(count):
            x = jnp.exp(levels[n] - new_top[n : n + 1, 0:1])
            sums.append(jnp.sum(folded(x, jnp.add) * weights, axis=0, keepdims=True))
        block_sum = jnp.sum(jnp.concatenate(sums, axis=0), axis=1, keepdims=True)
        return new_top, total * jnp.exp(top - new_top) + block_sum

    empty = (
        jnp.full((lev_dev, 128), low, jnp.float32),
        jnp.zeros((lev_dev, 128), jnp.float32),
    )

    def packed_row(carry, base):
        top, total = carry
        return jnp.sum(
            jnp.where(lane == level_at + base, top, 0.0)
            + jnp.where(lane == level_at + base + half_row, total, 0.0),
            axis=0,
            keepdims=True,
        )

    last = STEPS - 1
    def early(k, row):
        def take(ch, _):
            wait_recv(chunks + ch * STEPS + k)
            return 0

        lax.fori_loop(0, chunks, take, 0)

        def part(j, carry):
            return mass_block(grid_block(k, j, 0, chunks), weight_rows[j], carry)

        return row + packed_row(lax.fori_loop(0, splits, part, empty), k * lev_dev)

    zero_row = jnp.zeros((1, 128), jnp.float32)
    early_send[0:1, :] = lax.fori_loop(0, last, early, zero_row)
    wide_lane = lax.broadcasted_iota(jnp.int32, (LEV, 128), 1)
    diag = lax.broadcasted_iota(jnp.int32, (LEV, 128), 0)
    means_row = zero_row
    for n in range(STEPS):
        column = jnp.sum(jnp.where(wide_lane == 0, means[n], 0.0), axis=1, keepdims=True)
        means_row = means_row + jnp.sum(
            jnp.where(wide_lane == diag + LEV * n, column, 0.0), axis=0, keepdims=True
        )
    early_send[1:2, :] = means_row
    place_here = lev_id * bands + band_id

    def share(source, target, sems):
        def one(o, _):
            db, dz = peer(o)
            pltpu.make_async_remote_copy(
                src_ref=source,
                dst_ref=target.at[place_here],
                send_sem=sems.at[0],
                recv_sem=sems.at[1],
                device_id=(db, dz),
                device_id_type=MESH,
            ).start()
            return 0

        lax.fori_loop(1, devs, one, 0)
        pltpu.make_async_copy(source, target.at[place_here], sems.at[1]).start()

    def shared(target, sems):
        pltpu.make_async_copy(target, target, sems.at[1]).wait()

    def sent(target, sems):
        rest = target.at[pl.ds(0, devs - 1)]
        pltpu.make_async_copy(rest, rest, sems.at[0]).wait()

    share(early_send, early_recv, early_sem)
    send_pieces()
    for ch in range(chunks - 1):
        wait_recv(chunks + ch * STEPS + last)
    if chunks > 1:

        def part(j, _):
            acc[pl.ds(pl.multiple_of(j * tall, tall), tall), :] = grid_block(
                last, j, 0, chunks - 1
            )
            return 0

        lax.fori_loop(0, splits, part, 0)

    row_lane = lax.broadcasted_iota(jnp.int32, (8, 128), 1)
    to_grid = math.sqrt(2.0 / NT) * float(np.float32(math.sqrt(2.0 / NLON)).astype(jnp.bfloat16))
    lat_sum = sum(math.cos(math.pi * ((n + 0.5) / NLAT - 0.5)) for n in range(NLAT))
    normaliser = sum(1.0 + 2.0 * n / (LEV - 1) for n in range(LEV)) * lat_sum * NLON
    fix_scale = math.sqrt(NT * NLON) / 2.0

    def gathered(target):
        out = []
        for z in range(levs):
            here = target[z * bands : (z + 1) * bands, 0, :]
            top = jnp.max(here, axis=0, keepdims=True)
            total = jnp.sum(
                jnp.exp(here - top) * pltpu.roll(here, 128 - half_row, 1), axis=0, keepdims=True
            )
            out.append((jnp.broadcast_to(top, (8, 128)), jnp.broadcast_to(total, (8, 128))))
        return out

    def fix_of(parts, base, shift):
        valid = jnp.logical_and(row_lane >= base, row_lane < base + lev_dev)
        total = jnp.zeros((8, 128), jnp.float32)
        for z in range(levs):
            turn_by = (base - z * lev_dev) % 128
            moved = pltpu.roll(shift, turn_by, 1) if turn_by else shift
            level = (row_lane - base + z * lev_dev).astype(jnp.float32)
            top, amount = parts[z]
            total = total + jnp.where(
                valid,
                jnp.exp(jnp.where(valid, top + moved, 0.0))
                * amount
                * (1.0 + 2.0 * level / (LEV - 1)),
                0.0,
            )
        total = jnp.sum(total, axis=1, keepdims=True)
        return jnp.log(target_ref[0] / (total / normaliser))

    shared(early_recv, early_sem)
    parts = gathered(early_recv)
    base_row = zero_row
    for z in range(levs):
        base_row = base_row + jnp.sum(
            early_recv[z * bands : (z + 1) * bands, 1, :], axis=0, keepdims=True
        )
    base_row = jnp.broadcast_to(base_row, (8, 128))
    is_level = row_lane < LEV
    carried = jnp.zeros((8, 128), jnp.float32)
    for n in range(STEPS):
        back = (128 - LEV * n) % 128
        base_n = pltpu.roll(base_row, back, 1) if back else base_row
        column = jnp.sum(mix_ref[n] * carried[0:1, :LEV], axis=1, keepdims=True)
        moved_by = jnp.broadcast_to(
            jnp.sum(jnp.where(wide_lane == diag, column, 0.0), axis=0, keepdims=True), (8, 128)
        )
        moved = (base_n + moved_by).astype(jnp.bfloat16).astype(jnp.float32) - base_n.astype(
            jnp.bfloat16
        ).astype(jnp.float32)
        shift = jnp.where(is_level, moved * to_grid, 0.0)
        if n < last:
            fix = fix_of(parts, n * lev_dev, shift)
            fix_ref[n] = fix[0, 0]
            carried = jnp.where(is_level, moved_by + fix * fix_scale, 0.0)

    own_lane = lev_id * lev_dev + level_at
    own = jnp.sum(jnp.where(lane == own_lane, shift[0:1], 0.0), axis=1, keepdims=True)
    carries = [tuple(x[:per_tile] for x in empty)] * halves
    for n in range(splits * halves):
        here = slice(n * 128, (n + 1) * 128)
        arrived = recv.at[final, :, here]
        pltpu.make_async_copy(arrived, arrived, piece_sem.at[n]).wait()
        tile = grid_block(last, n, chunks - 1, chunks, 128)
        if chunks > 1:
            tile = tile + acc[here, :]
        for m in range(per_tile):
            level = n % halves * per_tile + m
            out_ref[level, n // halves * piece : (n // halves + 1) * piece, :] = (
                tile[m * piece : (m + 1) * piece] + own[level : level + 1, 0:1]
            ).astype(jnp.bfloat16)
        carries[n % halves] = mass_block(tile, weight_rows[n // halves], carries[n % halves])
    carry = tuple(jnp.concatenate([c[n] for c in carries], axis=0) for n in range(2))
    late_send[0:1, :] = packed_row(carry, 0)
    share(late_send, late_recv, late_sem)

    shared(late_recv, late_sem)
    fix_ref[last] = fix_of(gathered(late_recv), 0, shift)[0, 0]

    def finish(t, _):
        left = send.at[t, pl.ds(0, (devs - 1) * rows), :]
        pltpu.make_async_copy(left, left, send_sem.at[t]).wait()
        return 0

    lax.fori_loop(0, chunks * (1 + STEPS), finish, 0)
    sent(early_recv, early_sem)
    sent(late_recv, late_sem)


def body(
    increment, background, legendre, coupling, damping, target_mass, numerators, pair_low, lat_map
):
    band_count = lax.axis_size("band")
    lev_count = lax.axis_size("lev")
    devs = band_count * lev_count
    lev_dev, lat_dev = increment.shape[:2]
    pair_dev = legendre.shape[0]
    points = lev_dev * lat_dev
    cols = devs * 4 * GROUP
    fits = (
        lat_dev % 32 == 0
        and pair_dev % GROUP == 0
        and lev_dev == 8
        and band_count * 4 * GROUP == 128
        and lev_count * lev_dev == LEV
        and STEPS * lev_dev <= 64
        and points % 256 == 0
        and LEV * STEPS == 128
    )
    if not fits:
        return body_general(
            increment,
            background,
            legendre,
            coupling,
            damping,
            target_mass,
            numerators,
            pair_low,
            lat_map,
        )
    chunks = pair_dev // GROUP
    vmem = pl.BlockSpec(memory_space=pltpu.VMEM)
    smem = pl.BlockSpec(memory_space=pltpu.SMEM)
    hbm = pl.BlockSpec(memory_space=pl.ANY)
    total = chunks * (1 + STEPS)
    dma = pltpu.SemaphoreType.DMA
    return pl.pallas_call(
        lambda *refs: exchange_kernel(
            (band_count, lev_count, lev_dev, lat_dev, chunks), *refs
        ),
        out_shape=(
            pltpu.VMEM((lev_dev, lat_dev, NLON), jnp.bfloat16),
            jax.ShapeDtypeStruct((STEPS,), jnp.float32),
        ),
        in_specs=[hbm] * 9,
        out_specs=(vmem, smem),
        scratch_shapes=[
            pltpu.SMEM((STEPS,), jnp.int32),
            pltpu.SMEM((STEPS,), jnp.float32),
            pltpu.SMEM((1,), jnp.float32),
            pltpu.VMEM(pair_low.shape, jnp.int32),
            pltpu.VMEM(lat_map.shape, jnp.int32),
            pltpu.VMEM(coupling.shape, jnp.float32),
            pltpu.SemaphoreType.DMA((6,)),
            pltpu.VMEM((GROUP, 8, NT + 2), jnp.float32),
            pltpu.VMEM((STEPS, LEV, LEV), jnp.float32),
            pltpu.VMEM((points, NLON), jnp.bfloat16),
            pltpu.VMEM((chunks * cols, NLON), jnp.bfloat16),
            pltpu.VMEM((NLAT, NLAT), jnp.bfloat16),
            pltpu.VMEM((2, NT + 2, NLAT), jnp.bfloat16),
            pltpu.VMEM((GROUP, NT + 2, NLAT), jnp.bfloat16),
            pltpu.VMEM((2, 2 * LEV, NT + 2), jnp.float32),
            pltpu.VMEM((GROUP, 2 * LEV, NT + 2), jnp.float32),
            pltpu.VMEM((GROUP, 2 * LEV, NT + 2), jnp.float32),
            pltpu.VMEM((NLAT // 128, LEV * 4 * GROUP, 128), jnp.float32),
            pltpu.VMEM((points, NLON), jnp.float32),
            pltpu.VMEM((total, cols, points), jnp.bfloat16),
            pltpu.VMEM((total, cols, points), jnp.bfloat16),
            pltpu.VMEM((STEPS, LEV, 128), jnp.float32),
            pltpu.VMEM((lat_dev // 32, 32, 128), jnp.float32),
            pltpu.VMEM((2, 128), jnp.float32),
            pltpu.VMEM((devs, 2, 128), jnp.float32),
            pltpu.VMEM((1, 128), jnp.float32),
            pltpu.VMEM((devs, 1, 128), jnp.float32),
            dma,
            dma((2,)),
            dma((2,)),
            dma((total,)),
            dma((total,)),
            dma((points // 128,)),
            dma((2,)),
            dma((2,)),
        ],
        compiler_params=pltpu.CompilerParams(
            collective_id=0, has_side_effects=True, vmem_limit_bytes=62000000
        ),
    )(
        numerators,
        damping,
        target_mass,
        increment,
        legendre.transpose(0, 2, 1),
        background.reshape(pair_dev, 2 * LEV, NT + 2),
        pair_low,
        lat_map,
        coupling,
    )


def solution(mesh):
    return jax.shard_map(
        body,
        mesh=mesh,
        in_specs=(
            P("lev", "band", None),
            P(("band", "lev"), None, None, None),
            P(("band", "lev"), None, None),
            P(),
            P(),
            P(),
            P(),
            P(),
            P(),
        ),
        out_specs=(P("lev", "band", None), P()),
        check_vma=False,
    )
```

```python
import math

import jax
import numpy as np
import jax.numpy as jnp
from jax import lax
from jax.experimental import pallas as pl
from jax.experimental.pallas import tpu as pltpu
from jax.sharding import PartitionSpec as P

NT = 767
NLAT = 768
NLON = 1536
LEV = 32
STEPS = 4
DEN = 64
NPAIR = 384
AXES = ("band", "lev")


def wave_table(pair_low):
    column = jnp.arange(4 * pair_low.shape[0], dtype=jnp.int32)
    low = jnp.repeat(pair_low, 4)
    wavenumber = jnp.where(column // 2 % 2 == 0, low, NT - low)[:, None]
    quarter = (column % 2 * (NLON // 4))[:, None]
    fine = math.gcd(128, NLON)
    unit = 2.0 * math.pi / NLON
    coarse_pts = jnp.arange(NLON // fine, dtype=jnp.int32)[None, :] * fine
    coarse = ((wavenumber * coarse_pts + quarter) % NLON).astype(jnp.float32) * unit
    rest = (wavenumber * jnp.arange(fine, dtype=jnp.int32)[None, :] % NLON).astype(
        jnp.float32
    ) * unit
    norm = math.sqrt(2.0 / NLON)
    cos_a, sin_a, cos_b, sin_b = lax.optimization_barrier(
        (jnp.cos(coarse) * norm, jnp.sin(coarse) * norm, jnp.cos(rest), jnp.sin(rest))
    )
    blocks = [
        cos_a[:, i : i + 1] * cos_b - sin_a[:, i : i + 1] * sin_b for i in range(NLON // fine)
    ]
    return jnp.concatenate(blocks, axis=1).astype(jnp.bfloat16)


def lat_weights(lat_rows):
    return jnp.cos(math.pi * ((lat_rows.astype(jnp.float32) + 0.5) / NLAT - 0.5))


def degrees(low_wave):
    columns = jnp.arange(NT + 2, dtype=jnp.int32)
    in_second = columns[None, :] >= NT + 1 - low_wave[:, None]
    degree = jnp.where(in_second, columns[None, :] - 1, low_wave[:, None] + columns[None, :])
    return (degree.astype(jnp.float32), in_second)


def body_general(
    increment, background, legendre, coupling, damping, target_mass, numerators, pair_low, lat_map
):
    band_count = lax.axis_size("band")
    lev_count = lax.axis_size("lev")
    device_count = band_count * lev_count
    band_id = lax.axis_index("band")
    lev_id = lax.axis_index("lev")
    lev_dev = increment.shape[0]
    lat_dev = increment.shape[1]
    pair_dev = legendre.shape[0]
    points = lev_dev * lat_dev
    fourier_tab = wave_table(pair_low)
    local_lats = lax.dynamic_slice_in_dim(lat_map, band_id * lat_dev, lat_dev)
    row_weight = lat_weights(local_lats)
    all_levels = 1.0 + 2.0 * jnp.arange(LEV, dtype=jnp.float32) / (LEV - 1)
    normaliser = (
        jnp.sum(all_levels) * jnp.sum(lat_weights(jnp.arange(NLAT, dtype=jnp.int32))) * NLON
    )
    fix_scale = math.sqrt(NT * NLON) / 2.0
    own_pairs = lax.dynamic_slice_in_dim(
        pair_low, (band_id * lev_count + lev_id) * pair_dev, pair_dev
    )
    degree, in_second = degrees(own_pairs)
    holder = (own_pairs == 0).astype(jnp.float32)

    fourier = jnp.einsum(
        "ck,xk->cx",
        fourier_tab,
        increment.reshape(points, NLON),
        preferred_element_type=jnp.float32,
    )
    fourier = (fourier * jnp.tile(row_weight, lev_dev)[None, :]).astype(jnp.bfloat16)
    received = lax.all_to_all(
        fourier.reshape(device_count, pair_dev * 4, points), AXES, split_axis=0, concat_axis=0
    )

    pick = (lat_map[:, None] == jnp.arange(NLAT, dtype=jnp.int32)[None, :]).astype(jnp.bfloat16)
    stored = jnp.einsum(
        "jn,pnc->pjc", pick, legendre, preferred_element_type=jnp.float32
    ).astype(jnp.bfloat16)

    received = received.reshape(band_count, lev_count, pair_dev * 4, lev_dev, lat_dev)
    waves_in = received.transpose(2, 1, 3, 0, 4).reshape(pair_dev, 4 * LEV, NLAT)
    coeffs = jnp.einsum("prj,pjc->prc", waves_in, stored, preferred_element_type=jnp.float32)
    coeffs = coeffs.reshape(pair_dev, 2, 2, LEV, NT + 2) * math.sqrt(2.0 / NLAT)
    second_cols = in_second[:, None, None, :]
    smoothing = 1.0 / (1.0 + (degree / NT) ** 4)
    incr_spec = jnp.where(second_cols, coeffs[:, 1], coeffs[:, 0]) * smoothing[:, None, None, :]
    shape_term = degree * (degree + 1.0) / (NT * (NT + 1.0))

    spectral = background
    means = []
    arrived = []
    for step_idx in range(STEPS):
        coupled = 0.7 * spectral + 0.4 * jnp.einsum(
            "lm,prmc->prlc", coupling[step_idx], spectral, precision=lax.Precision.HIGHEST
        )
        weight_now = numerators[step_idx].astype(jnp.float32) / DEN
        spectral = (
            coupled / (1.0 + damping[step_idx] * shape_term)[:, None, None, :]
            + weight_now * incr_spec
        )
        means.append(jnp.sum(spectral[:, 0, :, 0] * holder[:, None], axis=0))
        spec_bf = spectral.astype(jnp.bfloat16)
        zeros_bf = jnp.zeros_like(spec_bf)
        split_rows = jnp.stack(
            [jnp.where(second_cols, zeros_bf, spec_bf), jnp.where(second_cols, spec_bf, zeros_bf)],
            axis=1,
        )
        waves_f = jnp.einsum(
            "prc,pjc->prj",
            split_rows.reshape(pair_dev, 4 * LEV, NT + 2),
            stored,
            preferred_element_type=jnp.float32,
        )
        waves_bf = (waves_f * math.sqrt(2.0 / NT)).astype(jnp.bfloat16)
        outgoing = waves_bf.reshape(pair_dev * 4, lev_count, lev_dev, band_count, lat_dev)
        outgoing = outgoing.transpose(3, 1, 0, 2, 4).reshape(device_count, pair_dev * 4, points)
        spectral, outgoing = lax.optimization_barrier((spectral, outgoing))
        arrived.append(lax.all_to_all(outgoing, AXES, split_axis=0, concat_axis=0))

    tops, sums = [], []
    for step_idx in range(STEPS):
        grid_now = jnp.einsum(
            "cx,ck->xk",
            arrived[step_idx].reshape(NPAIR * 4, points),
            fourier_tab,
            preferred_element_type=jnp.float32,
        ).reshape(lev_dev, lat_dev, NLON)
        top = jnp.max(grid_now, axis=(1, 2))
        tops.append(top)
        sums.append(
            jnp.sum(
                jnp.sum(jnp.exp(grid_now - top[:, None, None]), axis=2) * row_weight[None, :],
                axis=1,
            )
        )

    packed = jnp.concatenate(
        [jnp.stack(tops).reshape(-1), jnp.stack(sums).reshape(-1), jnp.stack(means).reshape(-1)]
    )
    gathered = lax.all_to_all(
        jnp.broadcast_to(packed[None, :], (device_count, packed.shape[0])),
        AXES,
        split_axis=0,
        concat_axis=0,
    )
    count = STEPS * lev_dev
    all_tops = gathered[:, :count].reshape(band_count, lev_count, STEPS, lev_dev)
    all_sums = gathered[:, count : 2 * count].reshape(band_count, lev_count, STEPS, lev_dev)
    all_tops = all_tops.transpose(2, 0, 1, 3).reshape(STEPS, band_count, LEV)
    all_sums = all_sums.transpose(2, 0, 1, 3).reshape(STEPS, band_count, LEV)
    all_means = jnp.sum(gathered[:, 2 * count :], axis=0).reshape(STEPS, LEV)

    table_entry = jnp.full((), math.sqrt(2.0 / NLON), jnp.bfloat16).astype(jnp.float32)
    to_grid = math.sqrt(2.0 / NT) * table_entry
    carried = jnp.zeros((LEV,), jnp.float32)
    shift = jnp.zeros((LEV,), jnp.float32)
    fix_list = []
    for step_idx in range(STEPS):
        carried = 0.7 * carried + 0.4 * jnp.sum(coupling[step_idx] * carried[None, :], axis=1)
        base = all_means[step_idx]
        moved = (base + carried).astype(jnp.bfloat16).astype(jnp.float32) - base.astype(
            jnp.bfloat16
        ).astype(jnp.float32)
        shift = moved * to_grid
        total = jnp.sum(
            jnp.exp(all_tops[step_idx] + shift[None, :]) * all_sums[step_idx] * all_levels[None, :]
        )
        mass_fix = jnp.log(target_mass[0] / (total / normaliser))
        fix_list.append(mass_fix)
        carried = carried + mass_fix * fix_scale
    own_shift = lax.dynamic_slice_in_dim(shift, lev_id * lev_dev, lev_dev)
    analysis = (grid_now + own_shift[:, None, None]).astype(jnp.bfloat16)
    return (analysis, jnp.stack(fix_list))


GROUP = 4
MESH = pl.DeviceIdType.MESH
LAST = (((1,), (1,)), ((), ()))


def sine(x):
    y = x * x
    out = -1.0 / math.factorial(11)
    for n in (9, 7, 5, 3, 1):
        out = out * y + (1.0 if n % 4 == 1 else -1.0) / math.factorial(n)
    return out * x


def table_values(phase):
    turns = jnp.floor((phase + 0.5) * (1.0 / NLON))
    rest = jnp.abs(phase - turns * NLON - NLON / 2) - NLON / 4
    return (sine(rest * (2.0 * math.pi / NLON)) * math.sqrt(2.0 / NLON)).astype(jnp.bfloat16)


def flat_dot(a, b):
    return jnp.dot(a, b, preferred_element_type=jnp.float32)


def exchange_kernel(
    sizes,
    numer_in,
    damp_in,
    target_in,
    inc_ref,
    leg_ref,
    back_ref,
    pair_in,
    lat_in,
    coupling_in,
    out_ref,
    fix_ref,
    numer_ref,
    damp_ref,
    target_ref,
    pair_ref,
    lat_ref,
    coupling_ref,
    small_sem,
    consts_ref,
    mix_ref,
    points_in,
    table,
    pick,
    leg_buf,
    stored,
    back_buf,
    incr,
    spec,
    turn,
    acc,
    send,
    recv,
    means,
    weight_rows,
    early_send,
    early_recv,
    late_send,
    late_recv,
    load_sem,
    leg_sem,
    back_sem,
    send_sem,
    recv_sem,
    piece_sem,
    early_sem,
    late_sem,
):
    bands, levs, lev_dev, lat_dev, chunks = sizes
    devs = bands * levs
    band_id = lax.axis_index("band")
    lev_id = lax.axis_index("lev")
    me = band_id * levs + lev_id
    piece = 32
    splits = lat_dev // piece
    rows = 4 * GROUP
    cols = devs * rows
    points = lev_dev * lat_dev
    slots = chunks * GROUP
    per_tile = 128 // piece
    halves = lev_dev // per_tile

    barrier = pltpu.get_barrier_semaphore()

    def peer(o):
        return (
            lax.rem(band_id + lax.rem(o, bands), bands),
            lax.rem(lev_id + o // bands, levs),
        )

    def greet(o, _):
        pl.semaphore_signal(barrier, inc=1, device_id=peer(o), device_id_type=MESH)
        return 0

    lax.fori_loop(1, devs, greet, 0)

    small = [
        pltpu.make_async_copy(source, target, small_sem.at[n])
        for n, (source, target) in enumerate(
            [
                (pair_in, pair_ref),
                (lat_in, lat_ref),
                (coupling_in, coupling_ref),
                (numer_in, numer_ref),
                (damp_in, damp_ref),
                (target_in, target_ref),
            ]
        )
    ]
    for copy in small:
        copy.start()

    def load_piece(i, j):
        return pltpu.make_async_copy(
            inc_ref.at[i, pl.ds(j * piece, piece), :],
            points_in.at[pl.ds((j * lev_dev + i) * piece, piece), :],
            load_sem,
        )

    for j in range(splits):
        for i in range(lev_dev):
            load_piece(i, j).start()

    def leg_copy(slot):
        return pltpu.make_async_copy(
            leg_ref.at[slot], leg_buf.at[lax.rem(slot, 2)], leg_sem.at[lax.rem(slot, 2)]
        )

    def back_copy(slot):
        return pltpu.make_async_copy(
            back_ref.at[slot], back_buf.at[lax.rem(slot, 2)], back_sem.at[lax.rem(slot, 2)]
        )

    for slot in range(2):
        leg_copy(slot).start()
        back_copy(slot).start()

    home = pl.ds((lev_id * bands + band_id) * rows, rows)

    def send_level(t, z):
        def one(o, _):
            band = lax.rem(band_id + o, bands)
            block = send.at[t, pl.ds((z * bands + band) * rows, rows), :]
            own = jnp.logical_and(o == 0, z == lev_id)

            @pl.when(own)
            def _():
                pltpu.make_async_copy(block, recv.at[t, home, :], recv_sem.at[t]).start()

            @pl.when(jnp.logical_not(own))
            def _():
                pltpu.make_async_remote_copy(
                    src_ref=block,
                    dst_ref=recv.at[t, home, :],
                    send_sem=send_sem.at[t],
                    recv_sem=recv_sem.at[t],
                    device_id=(band, z),
                    device_id_type=MESH,
                ).start()

            return 0

        lax.fori_loop(0, bands, one, 0)

    final = chunks * (1 + STEPS) - 1
    tall = lev_dev * piece

    def send_pieces():
        def one(n, _):
            j = n // devs
            o = lax.rem(n, bands)
            z = level_order(lax.rem(n // bands, levs))
            band = lax.rem(band_id + o, bands)
            lanes = pl.ds(pl.multiple_of(j * 128, 128), 128)
            block = send.at[final, pl.ds((z * bands + band) * rows, rows), lanes]
            own = jnp.logical_and(o == 0, z == lev_id)

            @pl.when(own)
            def _():
                pltpu.make_async_copy(
                    block, recv.at[final, home, lanes], piece_sem.at[j]
                ).start()

            @pl.when(jnp.logical_not(own))
            def _():
                pltpu.make_async_remote_copy(
                    src_ref=block,
                    dst_ref=recv.at[final, home, lanes],
                    send_sem=send_sem.at[final],
                    recv_sem=piece_sem.at[j],
                    device_id=(band, z),
                    device_id_type=MESH,
                ).start()

            return 0

        lax.fori_loop(0, splits * halves * devs, one, 0)

    def level_order(n):
        return lax.rem(lev_id + levs // 2 + n, levs)

    def wait_recv(t):
        pltpu.make_async_copy(recv.at[t], recv.at[t], recv_sem.at[t]).wait()

    lane_part = lax.broadcasted_iota(jnp.int32, (rows, 128), 1) // piece

    def gather_pieces(parts):
        out = parts[0]
        for n in range(1, per_tile):
            out = jnp.where(lane_part == n, parts[n], out)
        return out

    def rolled(x, amount):
        amount = amount * piece % 128
        return pltpu.roll(x, amount, 1) if amount else x

    small[0].wait()
    small[1].wait()
    lat_row = lat_ref[...].reshape(1, -1)
    lat_now = (lat_row.astype(jnp.float32) + 0.5) / NLAT - 0.5
    lat_now = jnp.broadcast_to(sine((0.5 - jnp.abs(lat_now)) * math.pi), (rows, NLAT))
    weight_tiles = []
    for j in range(splits):
        tile = jnp.zeros((rows, 128), jnp.float32)
        for b in range(bands):
            t, n = (b * splits + j) // per_tile, (b * splits + j) % per_tile
            source = lat_now[:, t * 128 : (t + 1) * 128]
            part = gather_pieces([rolled(source, il - n) for il in range(per_tile)])
            tile = jnp.where(band_id == b, part, tile)
        weight_tiles += [tile] * halves
    row_weight = jnp.concatenate(weight_tiles, axis=1)[0:1]
    pairs = pair_ref[...].reshape(1, -1).astype(jnp.float32)
    pair_count = pairs.shape[1]
    pair_dev = chunks * GROUP

    block_rows = bands * rows

    def fourier(n, _):
        ch = n // levs
        z = level_order(lax.rem(n, levs))
        col = lax.broadcasted_iota(jnp.int32, (block_rows, 1), 0)
        place = ((col >> 4) * levs + z) * pair_dev + ch * GROUP + ((col & 15) >> 2)
        spot = lax.broadcasted_iota(jnp.int32, (block_rows, pair_count), 1) == place
        wave = jnp.sum(jnp.where(spot, pairs, 0.0), axis=1, keepdims=True)
        wave = jnp.where((col & 2) == 0, wave, NT - wave)
        wave = jnp.broadcast_to(wave, (block_rows, 128))
        quarter = ((col & 1) * (NLON // 4)).astype(jnp.float32)
        lanes = lax.broadcasted_iota(jnp.int32, (1, 128), 1).astype(jnp.float32)
        at = pl.multiple_of(z * block_rows, block_rows)
        spot_rows = pl.ds(pl.multiple_of(ch * cols + at, block_rows), block_rows)
        for kc in range(NLON // 128):
            table[spot_rows, kc * 128 : (kc + 1) * 128] = table_values(
                wave * (lanes + kc * 128.0) + quarter
            )

        @pl.when(n == 0)
        def _():
            pltpu.make_async_copy(points_in, points_in, load_sem).wait()

        got = lax.dot_general(
            table[spot_rows, :], points_in[...], LAST, preferred_element_type=jnp.float32
        )
        send[ch, pl.ds(at, block_rows), :] = (got * row_weight).astype(jnp.bfloat16)

        @pl.when(n == 0)
        def _():
            pl.semaphore_wait(barrier, devs - 1)

        send_level(ch, z)
        return 0

    lax.fori_loop(0, chunks * levs, fourier, 0)

    lane_at = lax.broadcasted_iota(jnp.int32, (piece, 128), 1)
    row_at = lax.broadcasted_iota(jnp.int32, (piece, 128), 0)
    for j in range(splits):
        lane_weight = row_weight[:, j * lev_dev * piece : j * lev_dev * piece + 128]
        weight_rows[j] = jnp.broadcast_to(
            jnp.sum(jnp.where(lane_at == row_at, lane_weight, 0.0), axis=1, keepdims=True),
            (piece, 128),
        )
    pick[...] = (
        (lax.broadcasted_iota(jnp.int32, (NLAT, NLAT), 0) == lat_row)
        .astype(jnp.float32)
        .astype(jnp.bfloat16)
    )
    means[...] = jnp.zeros_like(means)
    for copy in small[2:]:
        copy.wait()
    square = [lax.broadcasted_iota(jnp.int32, (LEV, LEV), n) for n in range(2)]
    for n in range(STEPS):
        mix_ref[n] = jnp.where(square[0] == square[1], 0.7, 0.0) + 0.4 * coupling_ref[n]

    def chunk_body(ch, _):
        def prepare(s, _):
            slot = ch * GROUP + s
            leg_copy(slot).wait()
            stored[s] = flat_dot(leg_buf[lax.rem(slot, 2)], pick[...]).astype(jnp.bfloat16)
            spot = lax.broadcasted_iota(jnp.int32, (1, pair_count), 1) == me * pair_dev + slot
            low_wave = jnp.sum(jnp.where(spot, pairs, 0.0), axis=1, keepdims=True)
            column = lax.broadcasted_iota(jnp.int32, (1, NT + 2), 1).astype(jnp.float32)
            second = column >= NT + 1 - low_wave
            degree = jnp.where(second, column - 1.0, low_wave + column)
            ratio = degree / NT
            ratio = ratio * ratio
            shape_term = degree * (degree + 1.0) / (NT * (NT + 1.0))
            consts_ref[s, 0:1, :] = second.astype(jnp.float32)
            consts_ref[s, 1:2, :] = 1.0 / (1.0 + ratio * ratio)
            for n in range(STEPS):
                consts_ref[s, 2 + n : 3 + n, :] = 1.0 / (1.0 + damp_ref[n] * shape_term)
            consts_ref[s, 6:7, :] = jnp.broadcast_to(
                (low_wave == 0.0).astype(jnp.float32), (1, NT + 2)
            )

            @pl.when(slot + 2 < slots)
            def _():
                leg_copy(slot + 2).start()

            return 0

        lax.fori_loop(0, GROUP, prepare, 0)
        wait_recv(ch)

        def arrive(z, _):
            for half in range(halves):
                for t in range(NLAT // 128):
                    tiles = []
                    for n in range(per_tile):
                        g = t * per_tile + n
                        b, j = g // splits, g % splits
                        lane0 = (j * halves + half) * 128
                        tiles.append(
                            recv[
                                ch,
                                pl.ds(pl.multiple_of((z * bands + b) * rows, rows), rows),
                                lane0 : lane0 + 128,
                            ].astype(jnp.float32)
                        )
                    for il in range(per_tile):
                        level = z * lev_dev + half * per_tile + il
                        turn[t, pl.ds(pl.multiple_of(level * rows, rows), rows), :] = gather_pieces([rolled(tiles[n], n - il) for n in range(per_tile)])
            return 0

        lax.fori_loop(0, levs, arrive, 0)

        def direct(s, _):
            slot = ch * GROUP + s
            back_copy(slot).wait()
            waves_in = jnp.concatenate(
                [
                    jnp.concatenate(
                        [
                            turn[t, pl.ds(s * 4 + qr, LEV, stride=rows), :]
                            for t in range(NLAT // 128)
                        ],
                        axis=1,
                    )
                    for qr in range(4)
                ],
                axis=0,
            ).astype(jnp.bfloat16)
            coeffs = lax.dot_general(
                waves_in, stored[s], LAST, preferred_element_type=jnp.float32
            ) * math.sqrt(2.0 / NLAT)
            second = consts_ref[s, 0:1, :] > 0.5
            incr[s] = (
                jnp.where(second, coeffs[2 * LEV :], coeffs[: 2 * LEV]) * consts_ref[s, 1:2, :]
            )
            spec[s] = back_buf[lax.rem(slot, 2)]

            @pl.when(slot + 2 < slots)
            def _():
                back_copy(slot + 2).start()

            return 0

        lax.fori_loop(0, GROUP, direct, 0)

        def step(k, _):
            def inverse(s, _):
                second = consts_ref[s, 0:1, :] > 0.5
                inv = consts_ref[s, pl.ds(2 + k, 1), :]
                mix = mix_ref[k]
                weight = numer_ref[k].astype(jnp.float32) / DEN
                now = [
                    jnp.dot(
                        mix,
                        spec[s, r * LEV : (r + 1) * LEV, :],
                        precision=lax.Precision.HIGHEST,
                        preferred_element_type=jnp.float32,
                    )
                    * inv
                    + weight * incr[s, r * LEV : (r + 1) * LEV, :]
                    for r in range(2)
                ]
                for r in range(2):
                    spec[s, r * LEV : (r + 1) * LEV, :] = now[r]
                means[k] += now[0][:, :128] * consts_ref[s, 6:7, :128]
                both = jnp.concatenate(now, axis=0)
                split = jnp.concatenate(
                    [jnp.where(second, 0.0, both), jnp.where(second, both, 0.0)], axis=0
                ).astype(jnp.bfloat16)
                waves = flat_dot(split, stored[s]) * math.sqrt(2.0 / NT)
                for qr in range(4):
                    for t in range(NLAT // 128):
                        turn[t, pl.ds(s * 4 + qr, LEV, stride=rows), :] = waves[
                            qr * LEV : (qr + 1) * LEV, t * 128 : (t + 1) * 128
                        ]
                return 0

            lax.fori_loop(0, GROUP, inverse, 0)
            t_out = chunks + ch * STEPS + k

            def depart(zi, _):
                z = level_order(zi)
                for half in range(halves):
                    for t in range(NLAT // 128):
                        tiles = []
                        for il in range(per_tile):
                            level = z * lev_dev + half * per_tile + il
                            tiles.append(
                                turn[t, pl.ds(pl.multiple_of(level * rows, rows), rows), :]
                            )
                        for n in range(per_tile):
                            g = t * per_tile + n
                            b, j = g // splits, g % splits
                            lane0 = (j * halves + half) * 128
                            send[
                                t_out,
                                pl.ds(pl.multiple_of((z * bands + b) * rows, rows), rows),
                                lane0 : lane0 + 128,
                            ] = gather_pieces(
                                [rolled(tiles[il], il - n) for il in range(per_tile)]
                            ).astype(jnp.bfloat16)

                @pl.when(k != STEPS - 1)
                def _():
                    send_level(t_out, z)

                return 0

            lax.fori_loop(0, levs, depart, 0)
            return 0

        lax.fori_loop(0, STEPS, step, 0)
        return 0

    lax.fori_loop(0, chunks, chunk_body, 0)

    def send_last(n, _):
        send_level(chunks + n // levs * STEPS + STEPS - 1, level_order(lax.rem(n, levs)))
        return 0

    lax.fori_loop(0, (chunks - 1) * levs, send_last, 0)

    lane = lax.broadcasted_iota(jnp.int32, (lev_dev, 128), 1)
    level_at = lax.broadcasted_iota(jnp.int32, (lev_dev, 128), 0)
    half_row = 64
    low = -1e30

    def grid_block(k, j, lo, hi, size=None):
        size = size or tall
        at = j * size if isinstance(j, int) else pl.multiple_of(j * size, size)
        total = None
        for ch in range(lo, hi):
            one = flat_dot(
                recv[chunks + ch * STEPS + k, :, pl.ds(at, size)].T,
                table[ch * cols : (ch + 1) * cols, :],
            )
            total = one if total is None else total + one
        return total

    def folded(tile, op):
        out = tile[:, :128]
        for n in range(1, NLON // 128):
            out = op(out, tile[:, n * 128 : (n + 1) * 128])
        return out

    def mass_block(tile, weights, carry):
        top, total = carry
        count = tile.shape[0] // piece
        levels = [tile[n * piece : (n + 1) * piece] for n in range(count)]
        block_top = jnp.concatenate(
            [jnp.max(folded(x, jnp.maximum), axis=0, keepdims=True) for x in levels], axis=0
        )
        block_top = jnp.max(block_top, axis=1, keepdims=True)
        new_top = jnp.maximum(top, jnp.broadcast_to(block_top, top.shape))
        sums = []
        for n in range(count):
            x = jnp.exp(levels[n] - new_top[n : n + 1, 0:1])
            sums.append(jnp.sum(folded(x, jnp.add) * weights, axis=0, keepdims=True))
        block_sum = jnp.sum(jnp.concatenate(sums, axis=0), axis=1, keepdims=True)
        return new_top, total * jnp.exp(top - new_top) + block_sum

    empty = (
        jnp.full((lev_dev, 128), low, jnp.float32),
        jnp.zeros((lev_dev, 128), jnp.float32),
    )

    def packed_row(carry, base):
        top, total = carry
        return jnp.sum(
            jnp.where(lane == level_at + base, top, 0.0)
            + jnp.where(lane == level_at + base + half_row, total, 0.0),
            axis=0,
            keepdims=True,
        )

    last = STEPS - 1
    def early(k, row):
        def take(ch, _):
            wait_recv(chunks + ch * STEPS + k)
            return 0

        lax.fori_loop(0, chunks, take, 0)

        def part(j, carry):
            return mass_block(grid_block(k, j, 0, chunks), weight_rows[j], carry)

        return row + packed_row(lax.fori_loop(0, splits, part, empty), k * lev_dev)

    zero_row = jnp.zeros((1, 128), jnp.float32)
    early_send[0:1, :] = lax.fori_loop(0, last, early, zero_row)
    wide_lane = lax.broadcasted_iota(jnp.int32, (LEV, 128), 1)
    diag = lax.broadcasted_iota(jnp.int32, (LEV, 128), 0)
    means_row = zero_row
    for n in range(STEPS):
        column = jnp.sum(jnp.where(wide_lane == 0, means[n], 0.0), axis=1, keepdims=True)
        means_row = means_row + jnp.sum(
            jnp.where(wide_lane == diag + LEV * n, column, 0.0), axis=0, keepdims=True
        )
    early_send[1:2, :] = means_row
    place_here = lev_id * bands + band_id

    def share(source, target, sems):
        def one(o, _):
            db, dz = peer(o)
            pltpu.make_async_remote_copy(
                src_ref=source,
                dst_ref=target.at[place_here],
                send_sem=sems.at[0],
                recv_sem=sems.at[1],
                device_id=(db, dz),
                device_id_type=MESH,
            ).start()
            return 0

        lax.fori_loop(1, devs, one, 0)
        pltpu.make_async_copy(source, target.at[place_here], sems.at[1]).start()

    def shared(target, sems):
        pltpu.make_async_copy(target, target, sems.at[1]).wait()

    def sent(target, sems):
        rest = target.at[pl.ds(0, devs - 1)]
        pltpu.make_async_copy(rest, rest, sems.at[0]).wait()

    share(early_send, early_recv, early_sem)
    send_pieces()
    for ch in range(chunks - 1):
        wait_recv(chunks + ch * STEPS + last)
    if chunks > 1:

        def part(j, _):
            acc[pl.ds(pl.multiple_of(j * tall, tall), tall), :] = grid_block(
                last, j, 0, chunks - 1
            )
            return 0

        lax.fori_loop(0, splits, part, 0)

    row_lane = lax.broadcasted_iota(jnp.int32, (8, 128), 1)
    to_grid = math.sqrt(2.0 / NT) * float(np.float32(math.sqrt(2.0 / NLON)).astype(jnp.bfloat16))
    lat_sum = sum(math.cos(math.pi * ((n + 0.5) / NLAT - 0.5)) for n in range(NLAT))
    normaliser = sum(1.0 + 2.0 * n / (LEV - 1) for n in range(LEV)) * lat_sum * NLON
    fix_scale = math.sqrt(NT * NLON) / 2.0

    def gathered(target):
        out = []
        for z in range(levs):
            here = target[z * bands : (z + 1) * bands, 0, :]
            top = jnp.max(here, axis=0, keepdims=True)
            total = jnp.sum(
                jnp.exp(here - top) * pltpu.roll(here, 128 - half_row, 1), axis=0, keepdims=True
            )
            out.append((jnp.broadcast_to(top, (8, 128)), jnp.broadcast_to(total, (8, 128))))
        return out

    def fix_of(parts, base, shift):
        valid = jnp.logical_and(row_lane >= base, row_lane < base + lev_dev)
        total = jnp.zeros((8, 128), jnp.float32)
        for z in range(levs):
            turn_by = (base - z * lev_dev) % 128
            moved = pltpu.roll(shift, turn_by, 1) if turn_by else shift
            level = (row_lane - base + z * lev_dev).astype(jnp.float32)
            top, amount = parts[z]
            total = total + jnp.where(
                valid,
                jnp.exp(jnp.where(valid, top + moved, 0.0))
                * amount
                * (1.0 + 2.0 * level / (LEV - 1)),
                0.0,
            )
        total = jnp.sum(total, axis=1, keepdims=True)
        return jnp.log(target_ref[0] / (total / normaliser))

    shared(early_recv, early_sem)
    parts = gathered(early_recv)
    base_row = zero_row
    for z in range(levs):
        base_row = base_row + jnp.sum(
            early_recv[z * bands : (z + 1) * bands, 1, :], axis=0, keepdims=True
        )
    base_row = jnp.broadcast_to(base_row, (8, 128))
    is_level = row_lane < LEV
    carried = jnp.zeros((8, 128), jnp.float32)
    for n in range(STEPS):
        back = (128 - LEV * n) % 128
        base_n = pltpu.roll(base_row, back, 1) if back else base_row
        column = jnp.sum(mix_ref[n] * carried[0:1, :LEV], axis=1, keepdims=True)
        moved_by = jnp.broadcast_to(
            jnp.sum(jnp.where(wide_lane == diag, column, 0.0), axis=0, keepdims=True), (8, 128)
        )
        moved = (base_n + moved_by).astype(jnp.bfloat16).astype(jnp.float32) - base_n.astype(
            jnp.bfloat16
        ).astype(jnp.float32)
        shift = jnp.where(is_level, moved * to_grid, 0.0)
        if n < last:
            fix = fix_of(parts, n * lev_dev, shift)
            fix_ref[n] = fix[0, 0]
            carried = jnp.where(is_level, moved_by + fix * fix_scale, 0.0)

    own_lane = lev_id * lev_dev + level_at
    own = jnp.sum(jnp.where(lane == own_lane, shift[0:1], 0.0), axis=1, keepdims=True)
    carries = [tuple(x[:per_tile] for x in empty)] * halves
    for n in range(splits * halves):
        here = slice(n * 128, (n + 1) * 128)
        arrived = recv.at[final, :, here]
        pltpu.make_async_copy(arrived, arrived, piece_sem.at[n]).wait()
        tile = grid_block(last, n, chunks - 1, chunks, 128)
        if chunks > 1:
            tile = tile + acc[here, :]
        for m in range(per_tile):
            level = n % halves * per_tile + m
            out_ref[level, n // halves * piece : (n // halves + 1) * piece, :] = (
                tile[m * piece : (m + 1) * piece] + own[level : level + 1, 0:1]
            ).astype(jnp.bfloat16)
        carries[n % halves] = mass_block(tile, weight_rows[n // halves], carries[n % halves])
    carry = tuple(jnp.concatenate([c[n] for c in carries], axis=0) for n in range(2))
    late_send[0:1, :] = packed_row(carry, 0)
    share(late_send, late_recv, late_sem)

    def finish(t, _):
        left = send.at[t, pl.ds(0, (devs - 1) * rows), :]
        pltpu.make_async_copy(left, left, send_sem.at[t]).wait()
        return 0

    lax.fori_loop(0, chunks * (1 + STEPS), finish, 0)
    sent(early_recv, early_sem)
    shared(late_recv, late_sem)
    fix_ref[last] = fix_of(gathered(late_recv), 0, shift)[0, 0]

    sent(late_recv, late_sem)


def body(
    increment, background, legendre, coupling, damping, target_mass, numerators, pair_low, lat_map
):
    band_count = lax.axis_size("band")
    lev_count = lax.axis_size("lev")
    devs = band_count * lev_count
    lev_dev, lat_dev = increment.shape[:2]
    pair_dev = legendre.shape[0]
    points = lev_dev * lat_dev
    cols = devs * 4 * GROUP
    fits = (
        lat_dev % 32 == 0
        and pair_dev % GROUP == 0
        and lev_dev == 8
        and band_count * 4 * GROUP == 128
        and lev_count * lev_dev == LEV
        and STEPS * lev_dev <= 64
        and points % 256 == 0
        and LEV * STEPS == 128
    )
    if not fits:
        return body_general(
            increment,
            background,
            legendre,
            coupling,
            damping,
            target_mass,
            numerators,
            pair_low,
            lat_map,
        )
    chunks = pair_dev // GROUP
    vmem = pl.BlockSpec(memory_space=pltpu.VMEM)
    smem = pl.BlockSpec(memory_space=pltpu.SMEM)
    hbm = pl.BlockSpec(memory_space=pl.ANY)
    total = chunks * (1 + STEPS)
    dma = pltpu.SemaphoreType.DMA
    return pl.pallas_call(
        lambda *refs: exchange_kernel(
            (band_count, lev_count, lev_dev, lat_dev, chunks), *refs
        ),
        out_shape=(
            pltpu.VMEM((lev_dev, lat_dev, NLON), jnp.bfloat16),
            jax.ShapeDtypeStruct((STEPS,), jnp.float32),
        ),
        in_specs=[hbm] * 9,
        out_specs=(vmem, smem),
        scratch_shapes=[
            pltpu.SMEM((STEPS,), jnp.int32),
            pltpu.SMEM((STEPS,), jnp.float32),
            pltpu.SMEM((1,), jnp.float32),
            pltpu.VMEM(pair_low.shape, jnp.int32),
            pltpu.VMEM(lat_map.shape, jnp.int32),
            pltpu.VMEM(coupling.shape, jnp.float32),
            pltpu.SemaphoreType.DMA((6,)),
            pltpu.VMEM((GROUP, 8, NT + 2), jnp.float32),
            pltpu.VMEM((STEPS, LEV, LEV), jnp.float32),
            pltpu.VMEM((points, NLON), jnp.bfloat16),
            pltpu.VMEM((chunks * cols, NLON), jnp.bfloat16),
            pltpu.VMEM((NLAT, NLAT), jnp.bfloat16),
            pltpu.VMEM((2, NT + 2, NLAT), jnp.bfloat16),
            pltpu.VMEM((GROUP, NT + 2, NLAT), jnp.bfloat16),
            pltpu.VMEM((2, 2 * LEV, NT + 2), jnp.float32),
            pltpu.VMEM((GROUP, 2 * LEV, NT + 2), jnp.float32),
            pltpu.VMEM((GROUP, 2 * LEV, NT + 2), jnp.float32),
            pltpu.VMEM((NLAT // 128, LEV * 4 * GROUP, 128), jnp.float32),
            pltpu.VMEM((points, NLON), jnp.float32),
            pltpu.VMEM((total, cols, points), jnp.bfloat16),
            pltpu.VMEM((total, cols, points), jnp.bfloat16),
            pltpu.VMEM((STEPS, LEV, 128), jnp.float32),
            pltpu.VMEM((lat_dev // 32, 32, 128), jnp.float32),
            pltpu.VMEM((2, 128), jnp.float32),
            pltpu.VMEM((devs, 2, 128), jnp.float32),
            pltpu.VMEM((1, 128), jnp.float32),
            pltpu.VMEM((devs, 1, 128), jnp.float32),
            dma,
            dma((2,)),
            dma((2,)),
            dma((total,)),
            dma((total,)),
            dma((points // 128,)),
            dma((2,)),
            dma((2,)),
        ],
        compiler_params=pltpu.CompilerParams(
            collective_id=0, has_side_effects=True, vmem_limit_bytes=62000000
        ),
    )(
        numerators,
        damping,
        target_mass,
        increment,
        legendre.transpose(0, 2, 1),
        background.reshape(pair_dev, 2 * LEV, NT + 2),
        pair_low,
        lat_map,
        coupling,
    )


def solution(mesh):
    return jax.shard_map(
        body,
        mesh=mesh,
        in_specs=(
            P("lev", "band", None),
            P(("band", "lev"), None, None, None),
            P(("band", "lev"), None, None),
            P(),
            P(),
            P(),
            P(),
            P(),
            P(),
        ),
        out_specs=(P("lev", "band", None), P()),
        check_vma=False,
    )
```
